32 devices in a mesh: wide: 8 (over y, x, core), narrow: 4 (over z).
Axes of the slice: x: 2, y: 2, z: 4, core: 2. Of those that a mesh axis runs over, the one named last changes fastest.
Arguments:
- tokens: bfloat16 [65536, 768], P(('wide', 'narrow')), may hold values from -6 to 6
- cotangent: bfloat16 [65536, 768], P(('wide', 'narrow')), may hold values from -6 to 6
- lengths: int32 [64, 24], P(('wide', 'narrow')), may hold values from 1 to 128, 1024 in all within a row
- features: float32 [64, 384], replicated, may hold values from -5 to 5
- ln1_gain: bfloat16 [768], P('wide'), may hold values from 0.5 to 1.5
- ln1_bias: bfloat16 [768], P('wide'), may hold values from -1.75 to 1.75
- q_weight: bfloat16 [768, 768], P('wide'), may hold values from -0.21875 to 0.21875
- q_bias: bfloat16 [768], P('wide'), may hold values from -3 to 3
- k_weight: bfloat16 [768, 768], P('wide'), may hold values from -0.21875 to 0.21875
- k_bias: bfloat16 [768], P('wide'), may hold values from -3 to 3
- v_weight: bfloat16 [768, 768], P('wide'), may hold values from -0.21875 to 0.21875
- v_bias: bfloat16 [768], P('wide'), may hold values from -3 to 3
- out_weight: bfloat16 [768, 768], P('wide'), may hold values from -0.875 to 0.875
- out_bias: bfloat16 [768], P('wide'), may hold values from -3 to 3
- ln2_gain: bfloat16 [768], P('wide'), may hold values from 0.5 to 1.5
- ln2_bias: bfloat16 [768], P('wide'), may hold values from -1.75 to 1.75
- up_weight: bfloat16 [768, 3072], P('wide'), may hold values from -0.21875 to 0.21875
- up_bias: bfloat16 [3072], P('wide'), may hold values from -3 to 3
- down_weight: bfloat16 [3072, 768], P('wide'), may hold values from -0.109375 to 0.109375
- down_bias: bfloat16 [768], P('wide'), may hold values from -3 to 3
Outputs:
- output: bfloat16 [65536, 768], P(('wide', 'narrow'))
- input_grad: float32 [65536, 768], P(('wide', 'narrow'))
- ln1_gain_grad: float32 [768], P('wide')
- ln1_bias_grad: float32 [768], P('wide')
- q_weight_grad: float32 [768, 768], P('wide')
- q_bias_grad: float32 [768], P('wide')
- k_weight_grad: float32 [768, 768], P('wide')
- k_bias_grad: float32 [768], P('wide')
- v_weight_grad: float32 [768, 768], P('wide')
- v_bias_grad: float32 [768], P('wide')
- out_weight_grad: float32 [768, 768], P('wide')
- out_bias_grad: float32 [768], P('wide')
- ln2_gain_grad: float32 [768], P('wide')
- ln2_bias_grad: float32 [768], P('wide')
- up_weight_grad: float32 [768, 3072], P('wide')
- up_bias_grad: float32 [3072], P('wide')
- down_weight_grad: float32 [3072, 768], P('wide')
- down_bias_grad: float32 [768], P('wide')
The draws below stay inside these ranges and needn't reach their ends.
Inputs may be any that keep to these rules, and one draw needn't show every extreme that they name: Each row holds the 24 piece lengths of one sequence in order, summing to 1024; the largest is exactly 128.
All inputs are finite; a program needn't handle non-finite values.
Results may differ from the reference program's by a relative error of at most 0.03.
Values may be sent and summed in bfloat16 or wider, within the bound.
A program may use at most 192 MiB of HBM per device.

```python
import math
import jax
import jax.numpy as jnp
import numpy as np
from jax import lax

D = 768
HEADS = 12
HD = 64
FEAT = 32
FF = 3072
SEQ = 1024
SEGS = 24
MOLMAX = 128
SEQS = 64
TOKENS = 65536


def strengthened(drawn, stream_key, source, target, parts, factor):
    owner, partner = [(jnp.arange(drawn.shape[dim]) // (drawn.shape[dim] // parts)).reshape([-1 if axis == dim else 1 for axis in range(drawn.ndim)]) for dim in (source, target)]
    chosen = jax.random.permutation(stream_key, parts)[partner]
    strong = (owner == chosen) | (owner == (partner + parts // 2) % parts)
    return jnp.where(strong, factor * drawn, drawn)


def block_levels(rng, dims, shards, least, largest):
    def one(axis_at, shards_of):
        steps = jax.random.uniform(jax.random.fold_in(jax.random.fold_in(rng, 6), axis_at), (shards_of,), jnp.float32, least / len(shards), largest / len(shards))
        return jnp.repeat(jnp.exp(steps), dims[axis_at] // shards_of).reshape((-1,) + (1,) * (len(dims) - axis_at - 1))

    loudness = one(*shards[0])
    for cut in shards[1:]:
        loudness = loudness * one(*cut)
    return loudness


def profile(amount, total, limit, slope):
    loads = [(1 << 20) // math.isqrt(rank ** slope) + 1 for rank in range(2, amount + 1)]
    spare, given = total - limit - (amount - 1), [1] * (amount - 1)
    while spare > 0:
        candidates = [i for i in range(amount - 1) if given[i] < limit]
        whole, left = sum([loads[i] for i in candidates]), spare
        for i in candidates:
            addition = min(limit - given[i], max(1, left * loads[i] // whole), spare)
            given[i] = given[i] + addition
            spare = spare - addition
    return np.array([limit] + given)


def uneven_parts(rng, count, total, bound, skew):
    if count == 2:
        one = jax.random.randint(rng, (), max(1, total - bound), min(bound, total - 1) + 1)
        return jnp.stack([one, total - one])
    tallies = jnp.asarray(profile(count, total, bound, skew), jnp.int32)
    twos = (count - 1) // 2
    giver, sink = tallies[1:1 + 2 * twos:2], tallies[2:2 + 2 * twos:2]
    margin = jnp.minimum(giver - 1, bound - sink)
    shifted = jax.random.randint(jax.random.fold_in(rng, 1), (twos,), 0, 1 << 20) % (margin + 1)
    tallies = tallies.at[1:1 + 2 * twos:2].set(giver - shifted).at[2:2 + 2 * twos:2].set(sink + shifted)
    return tallies[jax.random.permutation(jax.random.fold_in(rng, 2), count)]


def bell_draw(own_key, shape, scale, most, split=(), kind=jnp.bfloat16):
    loudness = block_levels(own_key, shape, split, -0.22, 0.18) if split else 1.0
    values = jax.random.normal(own_key, shape, jnp.float32) * scale * loudness
    return jnp.minimum(jnp.maximum(values, -most), most).astype(kind)


def noise_with(key, extent, spread, reach, cuts, heavy, kind=jnp.bfloat16):
    array = spread * jax.random.normal(key, extent, jnp.float32)
    if cuts:
        array = array * block_levels(key, extent, cuts, -0.22, 0.18)
    return jnp.clip(strengthened(array, jax.random.fold_in(key, 3), *heavy), -reach, reach).astype(kind)


def setup_inputs(seed: int = 0) -> dict:
    key_list = jax.random.split(jax.random.key(seed), 21)
    tokens = bell_draw(key_list[0], (TOKENS, D), 1.0, 6.0, ((0, 32),))
    cotangent = noise_with(key_list[1], (TOKENS, D), 1.0, 6.0, ((0, 32),), (0, 1, 32, 2.75))
    lengths = jax.vmap(lambda own: uneven_parts(own, SEGS, SEQ, MOLMAX, 1))(jax.random.split(key_list[2], SEQS)).reshape((SEQS, SEGS)).astype(jnp.int32)
    features = bell_draw(key_list[3], (HD, HEADS * FEAT), 1.0, 5.0, (), jnp.float32)
    ln1_gain = jnp.clip(1.0 + 0.1 * jax.random.normal(key_list[4], (D,), jnp.float32), 0.5, 1.5).astype(jnp.bfloat16)
    ln1_bias = bell_draw(key_list[5], (D,), 0.3, 1.75, ((0, 8),))
    q_weight = bell_draw(key_list[6], (D, D), D ** -0.5, 0.21875, ((0, 8),))
    q_bias = bell_draw(key_list[7], (D,), 0.5, 3.0, ((0, 8),))
    k_weight = bell_draw(key_list[8], (D, D), D ** -0.5, 0.21875, ((0, 8),))
    k_bias = bell_draw(key_list[9], (D,), 0.5, 3.0, ((0, 8),))
    v_weight = bell_draw(key_list[10], (D, D), D ** -0.5, 0.21875, ((0, 8),))
    v_bias = bell_draw(key_list[11], (D,), 0.5, 3.0, ((0, 8),))
    out_weight = bell_draw(key_list[12], (D, D), (D // 16) ** -0.5, 0.875, ((0, 8),))
    out_bias = bell_draw(key_list[13], (D,), 0.5, 3.0, ((0, 8),))
    ln2_gain = jnp.clip(1.0 + 0.1 * jax.random.normal(key_list[14], (D,), jnp.float32), 0.5, 1.5).astype(jnp.bfloat16)
    ln2_bias = bell_draw(key_list[15], (D,), 0.3, 1.75, ((0, 8),))
    up_weight = bell_draw(key_list[16], (D, FF), D ** -0.5, 0.21875, ((0, 8),))
    up_bias = bell_draw(key_list[17], (FF,), 0.5, 3.0, ((0, 8),))
    down_weight = bell_draw(key_list[18], (FF, D), FF ** -0.5, 0.109375, ((0, 8),))
    down_bias = bell_draw(key_list[19], (D,), 0.5, 3.0, ((0, 8),))
    return dict(tokens=tokens, cotangent=cotangent, lengths=lengths, features=features, ln1_gain=ln1_gain, ln1_bias=ln1_bias, q_weight=q_weight, q_bias=q_bias, k_weight=k_weight, k_bias=k_bias, v_weight=v_weight, v_bias=v_bias, out_weight=out_weight, out_bias=out_bias, ln2_gain=ln2_gain, ln2_bias=ln2_bias, up_weight=up_weight, up_bias=up_bias, down_weight=down_weight, down_bias=down_bias)


@jax.custom_vjp
def low(v):
    return lax.optimization_barrier(v.astype(jnp.bfloat16)).astype(jnp.float32)

@jax.custom_vjp
def low_back(v):
    return v

def low_keep(v):
    return (low(v), None)

def low_pass(kept, grad):
    return (grad,)

def back_keep(v):
    return (v, None)

def back_low(kept, grad):
    return (low(grad),)
low.defvjp(low_keep, low_pass)
low_back.defvjp(back_keep, back_low)
EPSILON = 1e-05
HIGHEST = lax.Precision.HIGHEST

def pieces(lens_row, seq_len):
    seg_end = jnp.cumsum(lens_row).astype(jnp.int32)
    seg_start = (seg_end - lens_row).astype(jnp.int32)
    places = jnp.arange(seq_len, dtype=jnp.int32)
    segment = lax.optimization_barrier(jnp.sum((places[:, None] >= seg_end[None, :]).astype(jnp.int32), axis=1)).astype(jnp.int32)
    slots = jnp.arange(SEGS, dtype=jnp.int32)
    begins = lax.optimization_barrier(jnp.sum(jnp.where(segment[:, None] == slots[None, :], seg_start[None, :], 0), axis=1)).astype(jnp.int32)
    position = places - begins
    valid = (segment < SEGS - 1).astype(jnp.float32)
    allowed = (places[None, :] <= places[:, None]) & (segment[None, :] == segment[:, None])
    return (position, valid, allowed)

def rotate(heads_field, position):
    half = HD // 2
    rates = jnp.exp(jnp.arange(half, dtype=jnp.float32) * (-2.0 * math.log(10000.0) / HD))
    angles = position.astype(jnp.float32)[:, None] * rates[None, :]
    cosine = jnp.cos(angles)[:, None, :]
    sine = jnp.sin(angles)[:, None, :]
    first = heads_field[..., :half]
    second = heads_field[..., half:]
    return jnp.concatenate([first * cosine - second * sine, second * cosine + first * sine], axis=-1)

def featurize(rotated, features):
    table = features.reshape(HD, HEADS, FEAT)
    scores = jnp.einsum('lhe,ehm->lhm', rotated, table, precision=HIGHEST) * 0.125
    return jax.nn.elu(scores) + 1.0

def normalize(stream, gain, shift):
    average = lax.optimization_barrier(jnp.mean(stream, axis=-1, keepdims=True))
    centered = stream - average
    variance = lax.optimization_barrier(jnp.mean(centered * centered, axis=-1, keepdims=True))
    return centered * lax.rsqrt(variance + EPSILON) * gain + shift

def attend_sequence(operands, features):
    query_pre, key_pre, values, lens_row = operands
    position, valid, allowed = pieces(lens_row, SEQ)
    query_feat = low(featurize(rotate(query_pre.reshape(SEQ, HEADS, HD), position), features))
    key_feat = low(featurize(rotate(key_pre.reshape(SEQ, HEADS, HD), position), features))
    value_heads = values.reshape(SEQ, HEADS, HD)

    def one_head(head_ops):
        head_query, head_key, head_value = head_ops
        scores = jnp.where(allowed, jnp.dot(head_query, head_key.T, precision=HIGHEST), 0.0)
        kept_scores = low_back(scores)
        denominator = lax.optimization_barrier(jnp.sum(kept_scores, axis=1))
        numerator = low_back(jnp.dot(low(kept_scores), head_value, precision=HIGHEST))
        return numerator / denominator[:, None]
    mixed = lax.map(jax.checkpoint(one_head), (jnp.transpose(query_feat, (1, 0, 2)), jnp.transpose(key_feat, (1, 0, 2)), jnp.transpose(value_heads, (1, 0, 2))))
    return jnp.transpose(mixed, (1, 0, 2)).reshape(SEQ, D) * valid[:, None]

def layer(params, stream, lens_group, features):
    gain_first, shift_first, query_mat, query_add, key_mat, key_add, value_mat, value_add, proj_mat, proj_add, gain_second, shift_second, up_mat, up_add, down_mat, down_add = params
    count = lens_group.shape[0]
    hidden_one = low(normalize(stream, gain_first, shift_first))
    query_pre = low_back(jnp.dot(hidden_one, query_mat, precision=HIGHEST) + query_add)
    key_pre = low_back(jnp.dot(hidden_one, key_mat, precision=HIGHEST) + key_add)
    values = low(low_back(jnp.dot(hidden_one, value_mat, precision=HIGHEST) + value_add))

    def per_sequence(operands):
        return attend_sequence(operands, features)
    attended = lax.map(jax.checkpoint(per_sequence), (query_pre.reshape(count, SEQ, D), key_pre.reshape(count, SEQ, D), values.reshape(count, SEQ, D), lens_group))
    attended = low(attended.reshape(count * SEQ, D))
    residual = stream + low_back(jnp.dot(attended, proj_mat, precision=HIGHEST) + proj_add)
    hidden_two = low(normalize(residual, gain_second, shift_second))
    upper = low_back(jnp.dot(hidden_two, up_mat, precision=HIGHEST) + up_add)
    activated = low(jax.nn.gelu(upper, approximate=False))
    return residual + low_back(jnp.dot(activated, down_mat, precision=HIGHEST) + down_add)

def reference(tokens, cotangent, lengths, features, ln1_gain, ln1_bias, q_weight, q_bias, k_weight, k_bias, v_weight, v_bias, out_weight, out_bias, ln2_gain, ln2_bias, up_weight, up_bias, down_weight, down_bias):
    params = tuple((weight.astype(jnp.float32) for weight in (ln1_gain, ln1_bias, q_weight, q_bias, k_weight, k_bias, v_weight, v_bias, out_weight, out_bias, ln2_gain, ln2_bias, up_weight, up_bias, down_weight, down_bias)))
    per_group = math.gcd(SEQS, max(1, 4096 // SEQ))
    groups = SEQS // per_group
    stream = tokens.astype(jnp.float32).reshape(groups, per_group * SEQ, D)
    upstream = cotangent.astype(jnp.float32).reshape(groups, per_group * SEQ, D)
    lens_all = lengths.reshape(groups, per_group, SEGS)

    def one_group(totals, operands):
        block_rows, block_grad, block_lens = operands

        def forward(weights, rows):
            return layer(weights, rows, block_lens, features)
        result, pullback = jax.vjp(forward, params, block_rows)
        weight_grads, row_grads = pullback(block_grad)
        totals = jax.tree.map(jnp.add, totals, weight_grads)
        return (totals, (result.astype(jnp.bfloat16), row_grads))
    zeros = jax.tree.map(jnp.zeros_like, params)
    totals, (outputs, row_grads) = lax.scan(one_group, zeros, (stream, upstream, lens_all))
    return (outputs.reshape(TOKENS, D), row_grads.reshape(TOKENS, D), totals[0], totals[1], totals[2], totals[3], totals[4], totals[5], totals[6], totals[7], totals[8], totals[9], totals[10], totals[11], totals[12], totals[13], totals[14], totals[15])
```

```python
from functools import partial
import math

import jax
import jax.numpy as jnp
from jax import lax
from jax.sharding import PartitionSpec as P

D = 768
HEADS = 12
HD = 64
FEAT = 32
SEGS = 24
BLOCK = 128

EPSILON = 1e-05
HIGHEST = lax.Precision.HIGHEST


def pieces(lens_row, seq_len):
    seg_end = jnp.cumsum(lens_row)
    seg_start = seg_end - lens_row
    places = jnp.arange(seq_len, dtype=jnp.int32)
    segment = jnp.sum((places[:, None] >= seg_end[None, :]).astype(jnp.int32), axis=1)
    slots = jnp.arange(SEGS, dtype=jnp.int32)
    begins = jnp.sum(jnp.where(segment[:, None] == slots[None, :], seg_start[None, :], 0), axis=1)
    position = places - begins
    valid = (segment < SEGS - 1).astype(jnp.float32)
    return (position, valid, segment)


def rotate(heads_field, position):
    half = HD // 2
    rates = jnp.exp(jnp.arange(half, dtype=jnp.float32) * (-2.0 * math.log(10000.0) / HD))
    angles = position.astype(jnp.float32)[:, None] * rates[None, :]
    cosine = jnp.cos(angles)[:, None, :]
    sine = jnp.sin(angles)[:, None, :]
    first = heads_field[..., :half]
    second = heads_field[..., half:]
    return jnp.concatenate(
        [first * cosine - second * sine, second * cosine + first * sine], axis=-1
    )


def featurize(rotated, features):
    table = features.reshape(HD, HEADS, FEAT)
    scores = jnp.einsum("lhe,ehm->lhm", rotated, table, precision=HIGHEST) * 0.125
    return jax.nn.elu(scores) + 1.0


def normalize(stream, gain, shift):
    average = jnp.mean(stream, axis=-1, keepdims=True)
    centered = stream - average
    variance = jnp.mean(centered * centered, axis=-1, keepdims=True)
    return centered * lax.rsqrt(variance + EPSILON) * gain + shift


def contract_rows(left, right):
    return lax.dot_general(
        left, right, (((0,), (0,)), ((), ())), preferred_element_type=jnp.float32
    )


def times_transposed(left, right):
    return lax.dot_general(
        left, right, (((1,), (1,)), ((), ())), preferred_element_type=jnp.float32
    )


def column_sums(matrix):
    return jnp.sum(matrix.astype(jnp.float32), axis=0)


def gather_rows(shard):
    return lax.all_gather(shard, "wide", axis=0, tiled=True)


def reduce_rows(full):
    share = lax.psum_scatter(full.astype(jnp.bfloat16), "wide", scatter_dimension=0, tiled=True)
    return lax.psum(share, "narrow").astype(jnp.float32)


def to_blocks(field, nseq, width):
    seq_len = field.shape[0] // nseq
    nb = seq_len // BLOCK
    return jnp.transpose(field.reshape(nseq, nb, BLOCK, HEADS, width), (0, 3, 1, 2, 4))


def from_blocks(blocks):
    nseq, heads, nb, block, width = blocks.shape
    return jnp.transpose(blocks, (0, 2, 3, 1, 4)).reshape(nseq * nb * block, heads * width)


def window(blocks, fill=0):
    pad = [(0, 0)] * blocks.ndim
    pad[-3] = (1, 0)
    prev = jnp.pad(blocks, pad, constant_values=fill)[..., :-1, :, :]
    return jnp.concatenate([prev, blocks], axis=-2)


def unwindow(win):
    own = win[..., BLOCK:, :]
    nxt = win[..., 1:, :BLOCK, :]
    pad = [(0, 0)] * win.ndim
    pad[-3] = (0, 1)
    return own + jnp.pad(nxt, pad)


def on_device(
    tokens,
    cotangent,
    lengths,
    features,
    ln1_gain,
    ln1_bias,
    q_weight,
    q_bias,
    k_weight,
    k_bias,
    v_weight,
    v_bias,
    out_weight,
    out_bias,
    ln2_gain,
    ln2_bias,
    up_weight,
    up_bias,
    down_weight,
    down_bias,
):
    nseq = lengths.shape[0]
    total = tokens.shape[0]
    seq_len = total // nseq
    nb = seq_len // BLOCK
    wide = D // ln1_gain.shape[0]

    small_shards = (ln1_gain, ln1_bias, q_bias, k_bias, v_bias, out_bias, ln2_gain, ln2_bias, down_bias, up_bias)
    small_sizes = [piece.shape[0] for piece in small_shards]
    small_all = gather_rows(jnp.concatenate(small_shards)[None, :]).astype(jnp.float32)
    smalls = []
    offset = 0
    for size in small_sizes:
        smalls.append(small_all[:, offset:offset + size].reshape(wide * size))
        offset += size
    g1, b1, bq, bk, bv, bo, g2, b2, bd, bu = smalls
    qkv_mat = gather_rows(jnp.concatenate([q_weight, k_weight, v_weight], axis=1))
    proj_mat = gather_rows(out_weight)
    up_mat = gather_rows(up_weight)
    down_mat = gather_rows(down_weight)

    position, valid, segment = jax.vmap(partial(pieces, seq_len=seq_len))(lengths)
    position = position.reshape(total)
    valid_tok = valid.reshape(total)
    seg_blocks = segment.reshape(nseq, nb, BLOCK)
    seg_win = window(seg_blocks[..., None], fill=-1)[..., 0]
    rel_q = jnp.arange(BLOCK, dtype=jnp.int32)[:, None]
    rel_k = jnp.arange(2 * BLOCK, dtype=jnp.int32)[None, :]
    allowed = (rel_k <= rel_q + BLOCK)[None, None] & (
        seg_win[:, :, None, :] == seg_blocks[:, :, :, None]
    )
    allowed = allowed[:, None]
    valid_blk = valid.reshape(nseq, 1, nb, BLOCK, 1)

    stream = tokens.astype(jnp.float32)
    normed_one, norm_one_back = jax.vjp(normalize, stream, g1, b1)
    hidden_one = normed_one.astype(jnp.bfloat16)
    qkv = jnp.dot(hidden_one, qkv_mat, preferred_element_type=jnp.float32)
    query_pre = qkv[:, :D] + bq
    key_pre = qkv[:, D:2 * D] + bk
    values = (qkv[:, 2 * D:] + bv).astype(jnp.bfloat16)

    def features_of(projected):
        return featurize(rotate(projected.reshape(total, HEADS, HD), position), features)

    query_feat, query_back = jax.vjp(features_of, query_pre)
    key_feat, key_back = jax.vjp(features_of, key_pre)
    pq = to_blocks(query_feat.astype(jnp.bfloat16).reshape(total, HEADS * FEAT), nseq, FEAT)
    pk = window(to_blocks(key_feat.astype(jnp.bfloat16).reshape(total, HEADS * FEAT), nseq, FEAT))
    vb = window(to_blocks(values, nseq, HD))

    scores = jnp.einsum("shnqf,shnkf->shnqk", pq, pk, preferred_element_type=jnp.float32)
    scores = jnp.where(allowed, scores, 0.0)
    denominator = jnp.sum(scores, axis=-1, keepdims=True)
    scores_low = scores.astype(jnp.bfloat16)
    numerator = jnp.einsum("shnqk,shnkd->shnqd", scores_low, vb, preferred_element_type=jnp.float32)
    mixed = numerator / denominator * valid_blk
    attended = from_blocks(mixed).astype(jnp.bfloat16)
    residual = stream + (jnp.dot(attended, proj_mat, preferred_element_type=jnp.float32) + bo)
    normed_two, norm_two_back = jax.vjp(normalize, residual, g2, b2)
    hidden_two = normed_two.astype(jnp.bfloat16)
    upper = jnp.dot(hidden_two, up_mat, preferred_element_type=jnp.float32) + bu
    activated, gelu_back = jax.vjp(partial(jax.nn.gelu, approximate=False), upper)
    act_low = activated.astype(jnp.bfloat16)
    result = residual + (jnp.dot(act_low, down_mat, preferred_element_type=jnp.float32) + bd)
    output = result.astype(jnp.bfloat16)

    upward = cotangent
    grad_out = upward.astype(jnp.float32)
    down_grad = contract_rows(act_low, upward)
    down_bias_grad = column_sums(upward)
    grad_act = times_transposed(upward, down_mat)
    grad_upper = gelu_back(grad_act)[0].astype(jnp.bfloat16)
    up_grad = contract_rows(hidden_two, grad_upper)
    up_bias_grad = column_sums(grad_upper)
    grad_hidden_two = times_transposed(grad_upper, up_mat)
    grad_residual_norm, gain_two_grad, shift_two_grad = norm_two_back(grad_hidden_two)
    grad_residual = grad_out + grad_residual_norm
    grad_proj_in = grad_residual.astype(jnp.bfloat16)
    proj_grad = contract_rows(attended, grad_proj_in)
    proj_bias_grad = column_sums(grad_proj_in)
    grad_attended = times_transposed(grad_proj_in, proj_mat)

    head_grad = to_blocks(grad_attended, nseq, HD)
    scaled = head_grad * valid_blk
    grad_num = (scaled / denominator).astype(jnp.bfloat16)
    grad_den = -jnp.sum(scaled * numerator, axis=-1, keepdims=True) / (denominator * denominator)
    grad_scores = jnp.einsum("shnqd,shnkd->shnqk", grad_num, vb, preferred_element_type=jnp.float32)
    grad_scores = (grad_scores + grad_den).astype(jnp.bfloat16)
    grad_scores = jnp.where(allowed, grad_scores, jnp.zeros((), jnp.bfloat16))
    grad_vwin = jnp.einsum("shnqk,shnqd->shnkd", scores_low, grad_num, preferred_element_type=jnp.float32)
    grad_qf = jnp.einsum("shnqk,shnkf->shnqf", grad_scores, pk, preferred_element_type=jnp.float32)
    grad_kwin = jnp.einsum("shnqk,shnqf->shnkf", grad_scores, pq, preferred_element_type=jnp.float32)
    grad_value = from_blocks(unwindow(grad_vwin)).astype(jnp.bfloat16)
    grad_qf = from_blocks(grad_qf).reshape(total, HEADS, FEAT)
    grad_kf = from_blocks(unwindow(grad_kwin)).reshape(total, HEADS, FEAT)
    grad_query = query_back(grad_qf)[0].astype(jnp.bfloat16)
    grad_key = key_back(grad_kf)[0].astype(jnp.bfloat16)
    grad_qkv = jnp.concatenate([grad_query, grad_key, grad_value], axis=1)
    qkv_grad = contract_rows(hidden_one, grad_qkv)
    qkv_bias_grad = column_sums(grad_qkv)
    grad_hidden_one = times_transposed(grad_qkv, qkv_mat)
    grad_stream_norm, gain_one_grad, shift_one_grad = norm_one_back(grad_hidden_one)
    input_grad = grad_residual + grad_stream_norm

    down_share = reduce_rows(down_grad)
    up_share = reduce_rows(up_grad)
    proj_share = reduce_rows(proj_grad)
    qkv_share = reduce_rows(qkv_grad)
    small_grads = (
        gain_one_grad,
        shift_one_grad,
        qkv_bias_grad[:D],
        qkv_bias_grad[D:2 * D],
        qkv_bias_grad[2 * D:],
        proj_bias_grad,
        gain_two_grad,
        shift_two_grad,
        down_bias_grad,
        up_bias_grad,
    )
    packed = jnp.concatenate([piece.reshape(wide, -1) for piece in small_grads], axis=1)
    packed = lax.psum_scatter(packed, "wide", scatter_dimension=0, tiled=True)
    packed = lax.psum(packed, "narrow").reshape(-1)
    small_out = []
    offset = 0
    for size in small_sizes:
        small_out.append(packed[offset:offset + size])
        offset += size
    (
        gain_one_share,
        shift_one_share,
        query_bias_share,
        key_bias_share,
        value_bias_share,
        proj_bias_share,
        gain_two_share,
        shift_two_share,
        down_bias_share,
        up_bias_share,
    ) = small_out
    return (
        output,
        input_grad,
        gain_one_share,
        shift_one_share,
        qkv_share[:, :D],
        query_bias_share,
        qkv_share[:, D:2 * D],
        key_bias_share,
        qkv_share[:, 2 * D:],
        value_bias_share,
        proj_share,
        proj_bias_share,
        gain_two_share,
        shift_two_share,
        up_share,
        up_bias_share,
        down_share,
        down_bias_share,
    )


def solution(mesh):
    in_specs = (
        P(("wide", "narrow"), None),
        P(("wide", "narrow"), None),
        P(("wide", "narrow"), None),
        P(),
        P("wide"),
        P("wide"),
        P("wide", None),
        P("wide"),
        P("wide", None),
        P("wide"),
        P("wide", None),
        P("wide"),
        P("wide", None),
        P("wide"),
        P("wide"),
        P("wide"),
        P("wide", None),
        P("wide"),
        P("wide", None),
        P("wide"),
    )
    out_specs = (
        P(("wide", "narrow"), None),
        P(("wide", "narrow"), None),
        P("wide"),
        P("wide"),
        P("wide", None),
        P("wide"),
        P("wide", None),
        P("wide"),
        P("wide", None),
        P("wide"),
        P("wide", None),
        P("wide"),
        P("wide"),
        P("wide"),
        P("wide", None),
        P("wide"),
        P("wide", None),
        P("wide"),
    )
    return jax.shard_map(
        on_device, mesh=mesh, in_specs=in_specs, out_specs=out_specs, check_vma=False
    )
```

```python
from functools import partial
import math

import jax
import jax.numpy as jnp
from jax import lax
from jax.sharding import PartitionSpec as P

D = 768
HEADS = 12
HD = 64
FEAT = 32
SEGS = 24
BLOCK = 128

EPSILON = 1e-05
HIGHEST = lax.Precision.HIGHEST


def pieces(lens_row, seq_len):
    seg_end = jnp.cumsum(lens_row)
    seg_start = seg_end - lens_row
    places = jnp.arange(seq_len, dtype=jnp.int32)
    segment = jnp.sum((places[:, None] >= seg_end[None, :]).astype(jnp.int32), axis=1)
    slots = jnp.arange(SEGS, dtype=jnp.int32)
    begins = jnp.sum(jnp.where(segment[:, None] == slots[None, :], seg_start[None, :], 0), axis=1)
    position = places - begins
    valid = (segment < SEGS - 1).astype(jnp.float32)
    return (position, valid, segment)


def rotate(heads_field, position):
    half = HD // 2
    rates = jnp.exp(jnp.arange(half, dtype=jnp.float32) * (-2.0 * math.log(10000.0) / HD))
    angles = position.astype(jnp.float32)[:, None] * rates[None, :]
    cosine = jnp.cos(angles)[:, None, :]
    sine = jnp.sin(angles)[:, None, :]
    first = heads_field[..., :half]
    second = heads_field[..., half:]
    return jnp.concatenate(
        [first * cosine - second * sine, second * cosine + first * sine], axis=-1
    )


def featurize(rotated, features):
    table = features.reshape(HD, HEADS, FEAT)
    scores = jnp.einsum("lhe,ehm->lhm", rotated, table, precision=HIGHEST) * 0.125
    return jax.nn.elu(scores) + 1.0


def normalize(stream, gain, shift):
    average = jnp.mean(stream, axis=-1, keepdims=True)
    centered = stream - average
    variance = jnp.mean(centered * centered, axis=-1, keepdims=True)
    return centered * lax.rsqrt(variance + EPSILON) * gain + shift


def contract_rows(left, right):
    return lax.dot_general(
        left, right, (((0,), (0,)), ((), ())), preferred_element_type=jnp.float32
    )


def times_transposed(left, right):
    return lax.dot_general(
        left, right, (((1,), (1,)), ((), ())), preferred_element_type=jnp.float32
    )


def column_sums(matrix):
    return jnp.sum(matrix.astype(jnp.float32), axis=0)


def gather_rows(shard):
    return lax.all_gather(shard, "wide", axis=0, tiled=True)


def narrow_sum(share):
    size = lax.psum(1, "narrow")
    steps = size.bit_length() - 1
    assert 1 << steps == size
    me = lax.axis_index("narrow")
    rows = share.shape[0]
    assert rows % size == 0
    acc = share.astype(jnp.float32)
    for k in range(steps):
        half = acc.shape[0] // 2
        upper = ((me >> k) & 1) == 1
        lo, hi = acc[:half], acc[half:]
        keep = jnp.where(upper, hi, lo)
        send = jnp.where(upper, lo, hi).astype(jnp.bfloat16)
        pairs = [(i, i ^ (1 << k)) for i in range(size)]
        acc = keep + lax.ppermute(send, "narrow", pairs).astype(jnp.float32)
    part = acc.astype(jnp.bfloat16)
    for k in reversed(range(steps)):
        upper = ((me >> k) & 1) == 1
        pairs = [(i, i ^ (1 << k)) for i in range(size)]
        other = lax.ppermute(part, "narrow", pairs)
        part = jnp.where(upper, jnp.concatenate([other, part]), jnp.concatenate([part, other]))
    return part.astype(jnp.float32)


def reduce_rows(full):
    share = lax.psum_scatter(full.astype(jnp.bfloat16), "wide", scatter_dimension=0, tiled=True)
    return narrow_sum(share)


def gelu_parts(upper):
    cdf = 0.5 * (1.0 + lax.erf(upper * math.sqrt(0.5)))
    slope = cdf + upper * jnp.exp(-0.5 * upper * upper) * (1.0 / math.sqrt(2.0 * math.pi))
    return upper * cdf, slope


def to_blocks(field, nseq, width):
    seq_len = field.shape[0] // nseq
    nb = seq_len // BLOCK
    return jnp.transpose(field.reshape(nseq, nb, BLOCK, HEADS, width), (0, 3, 1, 2, 4))


def from_blocks(blocks):
    nseq, heads, nb, block, width = blocks.shape
    return jnp.transpose(blocks, (0, 2, 3, 1, 4)).reshape(nseq * nb * block, heads * width)


def window(blocks, fill=0):
    pad = [(0, 0)] * blocks.ndim
    pad[-3] = (1, 0)
    prev = jnp.pad(blocks, pad, constant_values=fill)[..., :-1, :, :]
    return jnp.concatenate([prev, blocks], axis=-2)


def unwindow(win):
    own = win[..., BLOCK:, :]
    nxt = win[..., 1:, :BLOCK, :]
    pad = [(0, 0)] * win.ndim
    pad[-3] = (0, 1)
    return own + jnp.pad(nxt, pad)


def as_columns(vectors, rows):
    return jnp.concatenate([v.reshape(rows, -1) for v in vectors], axis=1)


def on_device(
    tokens,
    cotangent,
    lengths,
    features,
    ln1_gain,
    ln1_bias,
    q_weight,
    q_bias,
    k_weight,
    k_bias,
    v_weight,
    v_bias,
    out_weight,
    out_bias,
    ln2_gain,
    ln2_bias,
    up_weight,
    up_bias,
    down_weight,
    down_bias,
):
    nseq = lengths.shape[0]
    total = tokens.shape[0]
    seq_len = total // nseq
    nb = seq_len // BLOCK
    shard_rows = ln1_gain.shape[0]
    wide = D // shard_rows

    small_shards = (ln1_gain, ln1_bias, q_bias, k_bias, v_bias, out_bias, ln2_gain, ln2_bias, down_bias, up_bias)
    small_cols = [piece.shape[0] // shard_rows for piece in small_shards]
    query_ext = gather_rows(jnp.concatenate([q_weight, as_columns(small_shards, shard_rows)], axis=1))
    query_mat = query_ext[:, :D]
    smalls = []
    offset = D
    for cols in small_cols:
        smalls.append(query_ext[:, offset:offset + cols].astype(jnp.float32).reshape(-1))
        offset += cols
    g1, b1, bq, bk, bv, bo, g2, b2, bd, bu = smalls
    key_mat = gather_rows(k_weight)
    value_mat = gather_rows(v_weight)
    proj_mat = gather_rows(out_weight)
    up_mat = gather_rows(up_weight)
    down_mat = gather_rows(down_weight)

    position, valid, segment = jax.vmap(partial(pieces, seq_len=seq_len))(lengths)
    position = position.reshape(total)
    seg_blocks = segment.reshape(nseq, nb, BLOCK)
    seg_win = window(seg_blocks[..., None], fill=-1)[..., 0]
    rel_q = jnp.arange(BLOCK, dtype=jnp.int32)[:, None]
    rel_k = jnp.arange(2 * BLOCK, dtype=jnp.int32)[None, :]
    allowed = (rel_k <= rel_q + BLOCK)[None, None] & (
        seg_win[:, :, None, :] == seg_blocks[:, :, :, None]
    )
    allowed = allowed[:, None]
    valid_blk = valid.reshape(nseq, 1, nb, BLOCK, 1)

    stream = tokens.astype(jnp.float32)
    normed_one, norm_one_back = jax.vjp(normalize, stream, g1, b1)
    hidden_one = normed_one.astype(jnp.bfloat16)
    query_pre = jnp.dot(hidden_one, query_mat, preferred_element_type=jnp.float32) + bq
    key_pre = jnp.dot(hidden_one, key_mat, preferred_element_type=jnp.float32) + bk
    values = (jnp.dot(hidden_one, value_mat, preferred_element_type=jnp.float32) + bv).astype(jnp.bfloat16)

    def features_of(projected):
        return featurize(rotate(projected.reshape(total, HEADS, HD), position), features)

    query_feat, query_back = jax.vjp(features_of, query_pre)
    key_feat, key_back = jax.vjp(features_of, key_pre)
    pq = to_blocks(query_feat.astype(jnp.bfloat16).reshape(total, HEADS * FEAT), nseq, FEAT)
    pk = window(to_blocks(key_feat.astype(jnp.bfloat16).reshape(total, HEADS * FEAT), nseq, FEAT))
    vb = window(to_blocks(values, nseq, HD))

    scores = jnp.einsum("shnqf,shnkf->shnqk", pq, pk, preferred_element_type=jnp.float32)
    scores = jnp.where(allowed, scores, 0.0)
    denominator = jnp.sum(scores, axis=-1, keepdims=True)
    scores_low = scores.astype(jnp.bfloat16)
    numerator = jnp.einsum("shnqk,shnkd->shnqd", scores_low, vb, preferred_element_type=jnp.float32)
    mixed = numerator / denominator * valid_blk
    attended = from_blocks(mixed).astype(jnp.bfloat16)
    residual = stream + (jnp.dot(attended, proj_mat, preferred_element_type=jnp.float32) + bo)
    normed_two, norm_two_back = jax.vjp(normalize, residual, g2, b2)
    hidden_two = normed_two.astype(jnp.bfloat16)
    upper = jnp.dot(hidden_two, up_mat, preferred_element_type=jnp.float32) + bu
    activated, slope = gelu_parts(upper)
    act_low = activated.astype(jnp.bfloat16)
    result = residual + (jnp.dot(act_low, down_mat, preferred_element_type=jnp.float32) + bd)
    output = result.astype(jnp.bfloat16)

    upward = cotangent
    grad_out = upward.astype(jnp.float32)
    down_grad = contract_rows(act_low, upward)
    down_share = reduce_rows(down_grad)
    down_bias_grad = column_sums(upward)
    grad_act = times_transposed(upward, down_mat)
    grad_upper = (grad_act * slope).astype(jnp.bfloat16)
    up_grad = contract_rows(hidden_two, grad_upper)
    up_share = reduce_rows(up_grad)
    up_bias_grad = column_sums(grad_upper)
    grad_hidden_two = times_transposed(grad_upper, up_mat)
    grad_residual_norm, gain_two_grad, shift_two_grad = norm_two_back(grad_hidden_two)
    grad_residual = grad_out + grad_residual_norm
    grad_proj_in = grad_residual.astype(jnp.bfloat16)
    proj_grad = contract_rows(attended, grad_proj_in)
    proj_share = reduce_rows(proj_grad)
    proj_bias_grad = column_sums(grad_proj_in)
    grad_attended = times_transposed(grad_proj_in, proj_mat)

    head_grad = to_blocks(grad_attended, nseq, HD)
    scaled = head_grad * valid_blk
    grad_num = (scaled / denominator).astype(jnp.bfloat16)
    grad_den = -jnp.sum(scaled * numerator, axis=-1, keepdims=True) / (denominator * denominator)
    grad_scores = jnp.einsum("shnqd,shnkd->shnqk", grad_num, vb, preferred_element_type=jnp.float32)
    grad_scores = (grad_scores + grad_den).astype(jnp.bfloat16)
    grad_scores = jnp.where(allowed, grad_scores, jnp.zeros((), jnp.bfloat16))
    grad_vwin = jnp.einsum("shnqk,shnqd->shnkd", scores_low, grad_num, preferred_element_type=jnp.float32)
    grad_value = from_blocks(unwindow(grad_vwin)).astype(jnp.bfloat16)
    value_grad = contract_rows(hidden_one, grad_value)
    value_share = reduce_rows(value_grad)
    value_bias_grad = column_sums(grad_value)
    grad_qf = jnp.einsum("shnqk,shnkf->shnqf", grad_scores, pk, preferred_element_type=jnp.float32)
    grad_kwin = jnp.einsum("shnqk,shnqf->shnkf", grad_scores, pq, preferred_element_type=jnp.float32)
    grad_qf = from_blocks(grad_qf).reshape(total, HEADS, FEAT)
    grad_kf = from_blocks(unwindow(grad_kwin)).reshape(total, HEADS, FEAT)
    grad_key = key_back(grad_kf)[0].astype(jnp.bfloat16)
    key_grad = contract_rows(hidden_one, grad_key)
    key_share = reduce_rows(key_grad)
    key_bias_grad = column_sums(grad_key)
    grad_query = query_back(grad_qf)[0].astype(jnp.bfloat16)
    query_grad = contract_rows(hidden_one, grad_query)
    query_bias_grad = column_sums(grad_query)
    grad_hidden_one = (
        times_transposed(grad_query, query_mat)
        + times_transposed(grad_key, key_mat)
        + times_transposed(grad_value, value_mat)
    )
    grad_stream_norm, gain_one_grad, shift_one_grad = norm_one_back(grad_hidden_one)
    input_grad = grad_residual + grad_stream_norm

    small_grads = (
        gain_one_grad,
        shift_one_grad,
        query_bias_grad,
        key_bias_grad,
        value_bias_grad,
        proj_bias_grad,
        gain_two_grad,
        shift_two_grad,
        down_bias_grad,
        up_bias_grad,
    )
    query_ext_share = reduce_rows(jnp.concatenate([query_grad, as_columns(small_grads, D)], axis=1))
    query_share = query_ext_share[:, :D]
    small_out = []
    offset = D
    for cols in small_cols:
        small_out.append(query_ext_share[:, offset:offset + cols].reshape(-1))
        offset += cols
    (
        gain_one_share,
        shift_one_share,
        query_bias_share,
        key_bias_share,
        value_bias_share,
        proj_bias_share,
        gain_two_share,
        shift_two_share,
        down_bias_share,
        up_bias_share,
    ) = small_out
    return (
        output,
        input_grad,
        gain_one_share,
        shift_one_share,
        query_share,
        query_bias_share,
        key_share,
        key_bias_share,
        value_share,
        value_bias_share,
        proj_share,
        proj_bias_share,
        gain_two_share,
        shift_two_share,
        up_share,
        up_bias_share,
        down_share,
        down_bias_share,
    )


def solution(mesh):
    in_specs = (
        P(("wide", "narrow"), None),
        P(("wide", "narrow"), None),
        P(("wide", "narrow"), None),
        P(),
        P("wide"),
        P("wide"),
        P("wide", None),
        P("wide"),
        P("wide", None),
        P("wide"),
        P("wide", None),
        P("wide"),
        P("wide", None),
        P("wide"),
        P("wide"),
        P("wide"),
        P("wide", None),
        P("wide"),
        P("wide", None),
        P("wide"),
    )
    out_specs = (
        P(("wide", "narrow"), None),
        P(("wide", "narrow"), None),
        P("wide"),
        P("wide"),
        P("wide", None),
        P("wide"),
        P("wide", None),
        P("wide"),
        P("wide", None),
        P("wide"),
        P("wide", None),
        P("wide"),
        P("wide"),
        P("wide"),
        P("wide", None),
        P("wide"),
        P("wide", None),
        P("wide"),
    )
    return jax.shard_map(
        on_device, mesh=mesh, in_specs=in_specs, out_specs=out_specs, check_vma=False
    )
```

```python
from functools import partial
import math

import jax
import jax.numpy as jnp
from jax import lax
from jax.sharding import PartitionSpec as P

D = 768
HEADS = 12
HD = 64
FEAT = 32
SEGS = 24
BLOCK = 128

EPSILON = 1e-05
HIGHEST = lax.Precision.HIGHEST


def pieces(lens_row, seq_len):
    seg_end = jnp.cumsum(lens_row)
    seg_start = seg_end - lens_row
    places = jnp.arange(seq_len, dtype=jnp.int32)
    segment = jnp.sum((places[:, None] >= seg_end[None, :]).astype(jnp.int32), axis=1)
    slots = jnp.arange(SEGS, dtype=jnp.int32)
    begins = jnp.sum(jnp.where(segment[:, None] == slots[None, :], seg_start[None, :], 0), axis=1)
    position = places - begins
    valid = (segment < SEGS - 1).astype(jnp.float32)
    return (position, valid, segment)


def rotate(heads_field, position):
    half = HD // 2
    rates = jnp.exp(jnp.arange(half, dtype=jnp.float32) * (-2.0 * math.log(10000.0) / HD))
    angles = position.astype(jnp.float32)[:, None] * rates[None, :]
    cosine = jnp.cos(angles)[:, None, :]
    sine = jnp.sin(angles)[:, None, :]
    first = heads_field[..., :half]
    second = heads_field[..., half:]
    return jnp.concatenate(
        [first * cosine - second * sine, second * cosine + first * sine], axis=-1
    )


def featurize(rotated, features):
    table = features.reshape(HD, HEADS, FEAT)
    scores = jnp.einsum("lhe,ehm->lhm", rotated, table, precision=HIGHEST) * 0.125
    return jax.nn.elu(scores) + 1.0


def normalize(stream, gain, shift):
    average = jnp.mean(stream, axis=-1, keepdims=True)
    centered = stream - average
    variance = jnp.mean(centered * centered, axis=-1, keepdims=True)
    return centered * lax.rsqrt(variance + EPSILON) * gain + shift


def contract_rows(left, right):
    return lax.dot_general(
        left, right, (((0,), (0,)), ((), ())), preferred_element_type=jnp.float32
    )


def times_transposed(left, right):
    return lax.dot_general(
        left, right, (((1,), (1,)), ((), ())), preferred_element_type=jnp.float32
    )


def column_sums(matrix):
    return jnp.sum(matrix.astype(jnp.float32), axis=0)


def gather_rows(shard):
    return lax.all_gather(shard, "wide", axis=0, tiled=True)


def narrow_sum(share):
    size = lax.psum(1, "narrow")
    steps = size.bit_length() - 1
    assert 1 << steps == size
    me = lax.axis_index("narrow")
    rows = share.shape[0]
    assert rows % size == 0
    acc = share.astype(jnp.float32)
    for k in range(steps):
        half = acc.shape[0] // 2
        upper = ((me >> k) & 1) == 1
        lo, hi = acc[:half], acc[half:]
        keep = jnp.where(upper, hi, lo)
        send = jnp.where(upper, lo, hi).astype(jnp.bfloat16)
        pairs = [(i, i ^ (1 << k)) for i in range(size)]
        acc = keep + lax.ppermute(send, "narrow", pairs).astype(jnp.float32)
    part = acc.astype(jnp.bfloat16)
    for k in reversed(range(steps)):
        upper = ((me >> k) & 1) == 1
        pairs = [(i, i ^ (1 << k)) for i in range(size)]
        other = lax.ppermute(part, "narrow", pairs)
        part = jnp.where(upper, jnp.concatenate([other, part]), jnp.concatenate([part, other]))
    return part.astype(jnp.float32)


def reduce_rows(full):
    share = lax.psum_scatter(full.astype(jnp.bfloat16), "wide", scatter_dimension=0, tiled=True)
    return narrow_sum(share)


def gelu_parts(upper):
    cdf = 0.5 * (1.0 + lax.erf(upper * math.sqrt(0.5)))
    slope = cdf + upper * jnp.exp(-0.5 * upper * upper) * (1.0 / math.sqrt(2.0 * math.pi))
    return upper * cdf, slope


def to_blocks(field, nseq, width):
    seq_len = field.shape[0] // nseq
    nb = seq_len // BLOCK
    return jnp.transpose(field.reshape(nseq, nb, BLOCK, HEADS, width), (0, 3, 1, 2, 4))


def from_blocks(blocks):
    nseq, heads, nb, block, width = blocks.shape
    return jnp.transpose(blocks, (0, 2, 3, 1, 4)).reshape(nseq * nb * block, heads * width)


def window(blocks, fill=0):
    pad = [(0, 0)] * blocks.ndim
    pad[-3] = (1, 0)
    prev = jnp.pad(blocks, pad, constant_values=fill)[..., :-1, :, :]
    return jnp.concatenate([prev, blocks], axis=-2)


def unwindow(win):
    own = win[..., BLOCK:, :]
    nxt = win[..., 1:, :BLOCK, :]
    pad = [(0, 0)] * win.ndim
    pad[-3] = (0, 1)
    return own + jnp.pad(nxt, pad)


def as_columns(vectors, rows):
    return jnp.concatenate([v.reshape(rows, -1) for v in vectors], axis=1)


def on_device(
    tokens,
    cotangent,
    lengths,
    features,
    ln1_gain,
    ln1_bias,
    q_weight,
    q_bias,
    k_weight,
    k_bias,
    v_weight,
    v_bias,
    out_weight,
    out_bias,
    ln2_gain,
    ln2_bias,
    up_weight,
    up_bias,
    down_weight,
    down_bias,
):
    nseq = lengths.shape[0]
    total = tokens.shape[0]
    seq_len = total // nseq
    nb = seq_len // BLOCK
    shard_rows = ln1_gain.shape[0]
    wide = D // shard_rows

    small_shards = (ln1_gain, ln1_bias, q_bias, k_bias, v_bias, out_bias, ln2_gain, ln2_bias, down_bias, up_bias)
    small_cols = [piece.shape[0] // shard_rows for piece in small_shards]
    first = gather_rows(
        jnp.concatenate([q_weight, k_weight, v_weight, as_columns(small_shards, shard_rows)], axis=1)
    )
    query_mat = first[:, :D]
    key_mat = first[:, D:2 * D]
    value_mat = first[:, 2 * D:3 * D]
    smalls = []
    offset = 3 * D
    for cols in small_cols:
        smalls.append(first[:, offset:offset + cols].astype(jnp.float32).reshape(-1))
        offset += cols
    g1, b1, bq, bk, bv, bo, g2, b2, bd, bu = smalls
    ff = up_weight.shape[1]
    second = gather_rows(
        jnp.concatenate([out_weight, up_weight, down_weight.reshape(shard_rows, -1)], axis=1)
    )
    proj_mat = second[:, :D]
    up_mat = second[:, D:D + ff]
    down_mat = second[:, D + ff:].reshape(ff, D)

    position, valid, segment = jax.vmap(partial(pieces, seq_len=seq_len))(lengths)
    position = position.reshape(total)
    seg_blocks = segment.reshape(nseq, nb, BLOCK)
    seg_win = window(seg_blocks[..., None], fill=-1)[..., 0]
    rel_q = jnp.arange(BLOCK, dtype=jnp.int32)[:, None]
    rel_k = jnp.arange(2 * BLOCK, dtype=jnp.int32)[None, :]
    allowed = (rel_k <= rel_q + BLOCK)[None, None] & (
        seg_win[:, :, None, :] == seg_blocks[:, :, :, None]
    )
    allowed = allowed[:, None]
    valid_blk = valid.reshape(nseq, 1, nb, BLOCK, 1)

    stream = tokens.astype(jnp.float32)
    normed_one, norm_one_back = jax.vjp(normalize, stream, g1, b1)
    hidden_one = normed_one.astype(jnp.bfloat16)
    query_pre = jnp.dot(hidden_one, query_mat, preferred_element_type=jnp.float32) + bq
    key_pre = jnp.dot(hidden_one, key_mat, preferred_element_type=jnp.float32) + bk
    values = (jnp.dot(hidden_one, value_mat, preferred_element_type=jnp.float32) + bv).astype(jnp.bfloat16)

    def features_of(projected):
        return featurize(rotate(projected.reshape(total, HEADS, HD), position), features)

    query_feat, query_back = jax.vjp(features_of, query_pre)
    key_feat, key_back = jax.vjp(features_of, key_pre)
    pq = to_blocks(query_feat.astype(jnp.bfloat16).reshape(total, HEADS * FEAT), nseq, FEAT)
    pk = window(to_blocks(key_feat.astype(jnp.bfloat16).reshape(total, HEADS * FEAT), nseq, FEAT))
    vb = window(to_blocks(values, nseq, HD))

    scores = jnp.einsum("shnqf,shnkf->shnqk", pq, pk, preferred_element_type=jnp.float32)
    scores = jnp.where(allowed, scores, 0.0)
    denominator = jnp.sum(scores, axis=-1, keepdims=True)
    scores_low = scores.astype(jnp.bfloat16)
    numerator = jnp.einsum("shnqk,shnkd->shnqd", scores_low, vb, preferred_element_type=jnp.float32)
    mixed = numerator / denominator * valid_blk
    attended = from_blocks(mixed).astype(jnp.bfloat16)
    residual = stream + (jnp.dot(attended, proj_mat, preferred_element_type=jnp.float32) + bo)
    normed_two, norm_two_back = jax.vjp(normalize, residual, g2, b2)
    hidden_two = normed_two.astype(jnp.bfloat16)
    upper = jnp.dot(hidden_two, up_mat, preferred_element_type=jnp.float32) + bu
    activated, slope = gelu_parts(upper)
    act_low = activated.astype(jnp.bfloat16)
    result = residual + (jnp.dot(act_low, down_mat, preferred_element_type=jnp.float32) + bd)
    output = result.astype(jnp.bfloat16)

    upward = cotangent
    grad_out = upward.astype(jnp.float32)
    grad_act = times_transposed(upward, down_mat)
    grad_upper = (grad_act * slope).astype(jnp.bfloat16)
    grad_hidden_two = times_transposed(grad_upper, up_mat)
    grad_residual_norm, gain_two_grad, shift_two_grad = norm_two_back(grad_hidden_two)
    grad_residual = grad_out + grad_residual_norm
    grad_proj_in = grad_residual.astype(jnp.bfloat16)
    grad_attended = times_transposed(grad_proj_in, proj_mat)
    down_grad = contract_rows(act_low, upward).astype(jnp.bfloat16)
    up_grad = contract_rows(hidden_two, grad_upper).astype(jnp.bfloat16)
    proj_grad = contract_rows(attended, grad_proj_in).astype(jnp.bfloat16)
    packed_one = jnp.concatenate([down_grad.reshape(D, -1), up_grad, proj_grad], axis=1)
    packed_one, grad_attended = lax.optimization_barrier((packed_one, grad_attended))
    scattered_one = lax.psum_scatter(packed_one, "wide", scatter_dimension=0, tiled=True)
    down_bias_grad = column_sums(upward)
    up_bias_grad = column_sums(grad_upper)
    proj_bias_grad = column_sums(grad_proj_in)

    head_grad = to_blocks(grad_attended, nseq, HD)
    scaled = head_grad * valid_blk
    grad_num = (scaled / denominator).astype(jnp.bfloat16)
    grad_den = -jnp.sum(scaled * numerator, axis=-1, keepdims=True) / (denominator * denominator)
    grad_scores = jnp.einsum("shnqd,shnkd->shnqk", grad_num, vb, preferred_element_type=jnp.float32)
    grad_scores = (grad_scores + grad_den).astype(jnp.bfloat16)
    grad_scores = jnp.where(allowed, grad_scores, jnp.zeros((), jnp.bfloat16))
    grad_vwin = jnp.einsum("shnqk,shnqd->shnkd", scores_low, grad_num, preferred_element_type=jnp.float32)
    grad_value = from_blocks(unwindow(grad_vwin)).astype(jnp.bfloat16)
    grad_qf = jnp.einsum("shnqk,shnkf->shnqf", grad_scores, pk, preferred_element_type=jnp.float32)
    grad_kwin = jnp.einsum("shnqk,shnqf->shnkf", grad_scores, pq, preferred_element_type=jnp.float32)
    grad_qf = from_blocks(grad_qf).reshape(total, HEADS, FEAT)
    grad_kf = from_blocks(unwindow(grad_kwin)).reshape(total, HEADS, FEAT)
    grad_key = key_back(grad_kf)[0].astype(jnp.bfloat16)
    grad_query = query_back(grad_qf)[0].astype(jnp.bfloat16)
    grad_qkv = jnp.concatenate([grad_query, grad_key, grad_value], axis=1)
    scattered_one, grad_qkv = lax.optimization_barrier((scattered_one, grad_qkv))
    share_one = narrow_sum(scattered_one)
    grad_hidden_one = times_transposed(grad_qkv, first[:, :3 * D])
    grad_stream_norm, gain_one_grad, shift_one_grad = norm_one_back(grad_hidden_one)
    input_grad = grad_residual + grad_stream_norm
    qkv_grad = contract_rows(hidden_one, grad_qkv)
    qkv_bias_grad = column_sums(grad_qkv)

    small_grads = (
        gain_one_grad,
        shift_one_grad,
        qkv_bias_grad[:D],
        qkv_bias_grad[D:2 * D],
        qkv_bias_grad[2 * D:],
        proj_bias_grad,
        gain_two_grad,
        shift_two_grad,
        down_bias_grad,
        up_bias_grad,
    )
    down_share = share_one[:, :ff].reshape(-1, D)
    up_share = share_one[:, ff:2 * ff]
    proj_share = share_one[:, 2 * ff:]
    share_two = reduce_rows(jnp.concatenate([qkv_grad, as_columns(small_grads, D)], axis=1))
    small_out = []
    offset = 3 * D
    for cols in small_cols:
        small_out.append(share_two[:, offset:offset + cols].reshape(-1))
        offset += cols
    (
        gain_one_share,
        shift_one_share,
        query_bias_share,
        key_bias_share,
        value_bias_share,
        proj_bias_share,
        gain_two_share,
        shift_two_share,
        down_bias_share,
        up_bias_share,
    ) = small_out
    return (
        output,
        input_grad,
        gain_one_share,
        shift_one_share,
        share_two[:, :D],
        query_bias_share,
        share_two[:, D:2 * D],
        key_bias_share,
        share_two[:, 2 * D:3 * D],
        value_bias_share,
        proj_share,
        proj_bias_share,
        gain_two_share,
        shift_two_share,
        up_share,
        up_bias_share,
        down_share,
        down_bias_share,
    )


def solution(mesh):
    in_specs = (
        P(("wide", "narrow"), None),
        P(("wide", "narrow"), None),
        P(("wide", "narrow"), None),
        P(),
        P("wide"),
        P("wide"),
        P("wide", None),
        P("wide"),
        P("wide", None),
        P("wide"),
        P("wide", None),
        P("wide"),
        P("wide", None),
        P("wide"),
        P("wide"),
        P("wide"),
        P("wide", None),
        P("wide"),
        P("wide", None),
        P("wide"),
    )
    out_specs = (
        P(("wide", "narrow"), None),
        P(("wide", "narrow"), None),
        P("wide"),
        P("wide"),
        P("wide", None),
        P("wide"),
        P("wide", None),
        P("wide"),
        P("wide", None),
        P("wide"),
        P("wide", None),
        P("wide"),
        P("wide"),
        P("wide"),
        P("wide", None),
        P("wide"),
        P("wide", None),
        P("wide"),
    )
    return jax.shard_map(
        on_device, mesh=mesh, in_specs=in_specs, out_specs=out_specs, check_vma=False
    )
```

```python
from functools import partial
import math

import jax
import jax.numpy as jnp
from jax import lax
from jax.sharding import PartitionSpec as P

D = 768
HEADS = 12
HD = 64
FEAT = 32
SEGS = 24
BLOCK = 128

EPSILON = 1e-05
HIGHEST = lax.Precision.HIGHEST


def pieces(lens_row, seq_len):
    seg_end = jnp.cumsum(lens_row)
    seg_start = seg_end - lens_row
    places = jnp.arange(seq_len, dtype=jnp.int32)
    segment = jnp.sum((places[:, None] >= seg_end[None, :]).astype(jnp.int32), axis=1)
    slots = jnp.arange(SEGS, dtype=jnp.int32)
    begins = jnp.sum(jnp.where(segment[:, None] == slots[None, :], seg_start[None, :], 0), axis=1)
    position = places - begins
    valid = (segment < SEGS - 1).astype(jnp.float32)
    return (position, valid, segment)


def rotate(heads_field, position):
    half = HD // 2
    rates = jnp.exp(jnp.arange(half, dtype=jnp.float32) * (-2.0 * math.log(10000.0) / HD))
    angles = position.astype(jnp.float32)[:, None] * rates[None, :]
    cosine = jnp.cos(angles)[:, None, :]
    sine = jnp.sin(angles)[:, None, :]
    first = heads_field[..., :half]
    second = heads_field[..., half:]
    return jnp.concatenate(
        [first * cosine - second * sine, second * cosine + first * sine], axis=-1
    )


def featurize(rotated, features):
    table = features.reshape(HD, HEADS, FEAT)
    scores = jnp.einsum("lhe,ehm->lhm", rotated, table, precision=HIGHEST) * 0.125
    return jax.nn.elu(scores) + 1.0


def normalize(stream, gain, shift):
    average = jnp.mean(stream, axis=-1, keepdims=True)
    centered = stream - average
    variance = jnp.mean(centered * centered, axis=-1, keepdims=True)
    return centered * lax.rsqrt(variance + EPSILON) * gain + shift


def contract_rows(left, right):
    return lax.dot_general(
        left, right, (((0,), (0,)), ((), ())), preferred_element_type=jnp.float32
    )


def times_transposed(left, right):
    return lax.dot_general(
        left, right, (((1,), (1,)), ((), ())), preferred_element_type=jnp.float32
    )


def column_sums(matrix):
    return jnp.sum(matrix.astype(jnp.float32), axis=0)


def gather_rows(shard):
    return lax.all_gather(shard, "wide", axis=0, tiled=True)


def narrow_sum(share):
    size = lax.psum(1, "narrow")
    steps = size.bit_length() - 1
    assert 1 << steps == size
    me = lax.axis_index("narrow")
    rows = share.shape[0]
    assert rows % size == 0
    acc = share.astype(jnp.float32)
    for k in range(steps):
        half = acc.shape[0] // 2
        upper = ((me >> k) & 1) == 1
        lo, hi = acc[:half], acc[half:]
        keep = jnp.where(upper, hi, lo)
        send = jnp.where(upper, lo, hi).astype(jnp.bfloat16)
        pairs = [(i, i ^ (1 << k)) for i in range(size)]
        acc = keep + lax.ppermute(send, "narrow", pairs).astype(jnp.float32)
    part = acc.astype(jnp.bfloat16)
    for k in reversed(range(steps)):
        upper = ((me >> k) & 1) == 1
        pairs = [(i, i ^ (1 << k)) for i in range(size)]
        other = lax.ppermute(part, "narrow", pairs)
        part = jnp.where(upper, jnp.concatenate([other, part]), jnp.concatenate([part, other]))
    return part.astype(jnp.float32)


def reduce_rows(full):
    share = lax.psum_scatter(full.astype(jnp.bfloat16), "wide", scatter_dimension=0, tiled=True)
    return narrow_sum(share)


def gelu_parts(upper):
    cdf = 0.5 * (1.0 + lax.erf(upper * math.sqrt(0.5)))
    slope = cdf + upper * jnp.exp(-0.5 * upper * upper) * (1.0 / math.sqrt(2.0 * math.pi))
    return upper * cdf, slope


def to_blocks(field, nseq, width):
    seq_len = field.shape[0] // nseq
    nb = seq_len // BLOCK
    return jnp.transpose(field.reshape(nseq, nb, BLOCK, HEADS, width), (0, 3, 1, 2, 4))


def from_blocks(blocks):
    nseq, heads, nb, block, width = blocks.shape
    return jnp.transpose(blocks, (0, 2, 3, 1, 4)).reshape(nseq * nb * block, heads * width)


def window(blocks, fill=0):
    pad = [(0, 0)] * blocks.ndim
    pad[-3] = (1, 0)
    prev = jnp.pad(blocks, pad, constant_values=fill)[..., :-1, :, :]
    return jnp.concatenate([prev, blocks], axis=-2)


def unwindow(win):
    own = win[..., BLOCK:, :]
    nxt = win[..., 1:, :BLOCK, :]
    pad = [(0, 0)] * win.ndim
    pad[-3] = (0, 1)
    return own + jnp.pad(nxt, pad)


def as_columns(vectors, rows):
    return jnp.concatenate([v.reshape(rows, -1) for v in vectors], axis=1)


def on_device(
    tokens,
    cotangent,
    lengths,
    features,
    ln1_gain,
    ln1_bias,
    q_weight,
    q_bias,
    k_weight,
    k_bias,
    v_weight,
    v_bias,
    out_weight,
    out_bias,
    ln2_gain,
    ln2_bias,
    up_weight,
    up_bias,
    down_weight,
    down_bias,
):
    nseq = lengths.shape[0]
    total = tokens.shape[0]
    seq_len = total // nseq
    nb = seq_len // BLOCK
    shard_rows = ln1_gain.shape[0]
    wide = D // shard_rows

    small_shards = (ln1_gain, ln1_bias, q_bias, k_bias, v_bias, out_bias, ln2_gain, ln2_bias, down_bias, up_bias)
    small_cols = [piece.shape[0] // shard_rows for piece in small_shards]
    first = gather_rows(
        jnp.concatenate([q_weight, k_weight, v_weight, as_columns(small_shards, shard_rows)], axis=1)
    )
    query_mat = first[:, :D]
    key_mat = first[:, D:2 * D]
    value_mat = first[:, 2 * D:3 * D]
    smalls = []
    offset = 3 * D
    for cols in small_cols:
        smalls.append(first[:, offset:offset + cols].astype(jnp.float32).reshape(-1))
        offset += cols
    g1, b1, bq, bk, bv, bo, g2, b2, bd, bu = smalls
    ff = up_weight.shape[1]
    second = gather_rows(jnp.concatenate([out_weight, up_weight], axis=1))
    proj_mat = second[:, :D]
    up_mat = second[:, D:]
    down_mat = gather_rows(down_weight)

    position, valid, segment = jax.vmap(partial(pieces, seq_len=seq_len))(lengths)
    position = position.reshape(total)
    seg_blocks = segment.reshape(nseq, nb, BLOCK)
    seg_win = window(seg_blocks[..., None], fill=-1)[..., 0]
    rel_q = jnp.arange(BLOCK, dtype=jnp.int32)[:, None]
    rel_k = jnp.arange(2 * BLOCK, dtype=jnp.int32)[None, :]
    allowed = (rel_k <= rel_q + BLOCK)[None, None] & (
        seg_win[:, :, None, :] == seg_blocks[:, :, :, None]
    )
    allowed = allowed[:, None]
    valid_blk = valid.reshape(nseq, 1, nb, BLOCK, 1)

    stream = tokens.astype(jnp.float32)
    normed_one, norm_one_back = jax.vjp(normalize, stream, g1, b1)
    hidden_one = normed_one.astype(jnp.bfloat16)
    query_pre = jnp.dot(hidden_one, query_mat, preferred_element_type=jnp.float32) + bq
    key_pre = jnp.dot(hidden_one, key_mat, preferred_element_type=jnp.float32) + bk
    values = (jnp.dot(hidden_one, value_mat, preferred_element_type=jnp.float32) + bv).astype(jnp.bfloat16)

    def features_of(projected):
        return featurize(rotate(projected.reshape(total, HEADS, HD), position), features)

    query_feat, query_back = jax.vjp(features_of, query_pre)
    key_feat, key_back = jax.vjp(features_of, key_pre)
    pq = to_blocks(query_feat.astype(jnp.bfloat16).reshape(total, HEADS * FEAT), nseq, FEAT)
    pk = window(to_blocks(key_feat.astype(jnp.bfloat16).reshape(total, HEADS * FEAT), nseq, FEAT))
    vb = window(to_blocks(values, nseq, HD))

    scores = jnp.einsum("shnqf,shnkf->shnqk", pq, pk, preferred_element_type=jnp.float32)
    scores = jnp.where(allowed, scores, 0.0)
    denominator = jnp.sum(scores, axis=-1, keepdims=True)
    scores_low = scores.astype(jnp.bfloat16)
    numerator = jnp.einsum("shnqk,shnkd->shnqd", scores_low, vb, preferred_element_type=jnp.float32)
    mixed = numerator / denominator * valid_blk
    attended = from_blocks(mixed).astype(jnp.bfloat16)
    residual = stream + (jnp.dot(attended, proj_mat, preferred_element_type=jnp.float32) + bo)
    normed_two, norm_two_back = jax.vjp(normalize, residual, g2, b2)
    hidden_two = normed_two.astype(jnp.bfloat16)
    upper = jnp.dot(hidden_two, up_mat, preferred_element_type=jnp.float32) + bu
    activated, slope = gelu_parts(upper)
    act_low = activated.astype(jnp.bfloat16)
    result = residual + (jnp.dot(act_low, down_mat, preferred_element_type=jnp.float32) + bd)
    output = result.astype(jnp.bfloat16)

    upward = cotangent
    grad_out = upward.astype(jnp.float32)
    grad_act = times_transposed(upward, down_mat)
    grad_upper = (grad_act * slope).astype(jnp.bfloat16)
    grad_hidden_two = times_transposed(grad_upper, up_mat)
    grad_residual_norm, gain_two_grad, shift_two_grad = norm_two_back(grad_hidden_two)
    grad_residual = grad_out + grad_residual_norm
    grad_proj_in = grad_residual.astype(jnp.bfloat16)
    grad_attended = times_transposed(grad_proj_in, proj_mat)
    down_grad = contract_rows(act_low, upward).astype(jnp.bfloat16)
    up_grad = contract_rows(hidden_two, grad_upper).astype(jnp.bfloat16)
    proj_grad = contract_rows(attended, grad_proj_in).astype(jnp.bfloat16)
    packed_one = jnp.concatenate([up_grad, proj_grad], axis=1)
    down_grad, packed_one, grad_attended = lax.optimization_barrier((down_grad, packed_one, grad_attended))
    scattered_down = lax.psum_scatter(down_grad, "wide", scatter_dimension=0, tiled=True)
    scattered_one = lax.psum_scatter(packed_one, "wide", scatter_dimension=0, tiled=True)
    down_bias_grad = column_sums(upward)
    up_bias_grad = column_sums(grad_upper)
    proj_bias_grad = column_sums(grad_proj_in)

    head_grad = to_blocks(grad_attended, nseq, HD)
    scaled = head_grad * valid_blk
    grad_num = (scaled / denominator).astype(jnp.bfloat16)
    grad_den = -jnp.sum(scaled * numerator, axis=-1, keepdims=True) / (denominator * denominator)
    grad_scores = jnp.einsum("shnqd,shnkd->shnqk", grad_num, vb, preferred_element_type=jnp.float32)
    grad_scores = (grad_scores + grad_den).astype(jnp.bfloat16)
    grad_scores = jnp.where(allowed, grad_scores, jnp.zeros((), jnp.bfloat16))
    grad_vwin = jnp.einsum("shnqk,shnqd->shnkd", scores_low, grad_num, preferred_element_type=jnp.float32)
    grad_value = from_blocks(unwindow(grad_vwin)).astype(jnp.bfloat16)
    grad_qf = jnp.einsum("shnqk,shnkf->shnqf", grad_scores, pk, preferred_element_type=jnp.float32)
    grad_kwin = jnp.einsum("shnqk,shnqf->shnkf", grad_scores, pq, preferred_element_type=jnp.float32)
    grad_qf = from_blocks(grad_qf).reshape(total, HEADS, FEAT)
    grad_kf = from_blocks(unwindow(grad_kwin)).reshape(total, HEADS, FEAT)
    grad_key = key_back(grad_kf)[0].astype(jnp.bfloat16)
    grad_query = query_back(grad_qf)[0].astype(jnp.bfloat16)
    grad_qkv = jnp.concatenate([grad_query, grad_key, grad_value], axis=1)
    scattered_down, scattered_one, grad_qkv = lax.optimization_barrier((scattered_down, scattered_one, grad_qkv))
    down_share = lax.psum(scattered_down, "narrow")
    share_one = lax.psum(scattered_one, "narrow")
    grad_hidden_one = times_transposed(grad_qkv, first[:, :3 * D])
    grad_stream_norm, gain_one_grad, shift_one_grad = norm_one_back(grad_hidden_one)
    input_grad = grad_residual + grad_stream_norm
    qkv_grad = contract_rows(hidden_one, grad_qkv)
    qkv_bias_grad = column_sums(grad_qkv)

    small_grads = (
        gain_one_grad,
        shift_one_grad,
        qkv_bias_grad[:D],
        qkv_bias_grad[D:2 * D],
        qkv_bias_grad[2 * D:],
        proj_bias_grad,
        gain_two_grad,
        shift_two_grad,
        down_bias_grad,
        up_bias_grad,
    )
    packed_two = jnp.concatenate([qkv_grad, as_columns(small_grads, D)], axis=1)
    down_share, share_one, packed_two = lax.optimization_barrier((down_share, share_one, packed_two))
    down_share = down_share.astype(jnp.float32)
    up_share = share_one[:, :ff].astype(jnp.float32)
    proj_share = share_one[:, ff:].astype(jnp.float32)
    share_two = reduce_rows(packed_two)
    small_out = []
    offset = 3 * D
    for cols in small_cols:
        small_out.append(share_two[:, offset:offset + cols].reshape(-1))
        offset += cols
    (
        gain_one_share,
        shift_one_share,
        query_bias_share,
        key_bias_share,
        value_bias_share,
        proj_bias_share,
        gain_two_share,
        shift_two_share,
        down_bias_share,
        up_bias_share,
    ) = small_out
    return (
        output,
        input_grad,
        gain_one_share,
        shift_one_share,
        share_two[:, :D],
        query_bias_share,
        share_two[:, D:2 * D],
        key_bias_share,
        share_two[:, 2 * D:3 * D],
        value_bias_share,
        proj_share,
        proj_bias_share,
        gain_two_share,
        shift_two_share,
        up_share,
        up_bias_share,
        down_share,
        down_bias_share,
    )


def solution(mesh):
    in_specs = (
        P(("wide", "narrow"), None),
        P(("wide", "narrow"), None),
        P(("wide", "narrow"), None),
        P(),
        P("wide"),
        P("wide"),
        P("wide", None),
        P("wide"),
        P("wide", None),
        P("wide"),
        P("wide", None),
        P("wide"),
        P("wide", None),
        P("wide"),
        P("wide"),
        P("wide"),
        P("wide", None),
        P("wide"),
        P("wide", None),
        P("wide"),
    )
    out_specs = (
        P(("wide", "narrow"), None),
        P(("wide", "narrow"), None),
        P("wide"),
        P("wide"),
        P("wide", None),
        P("wide"),
        P("wide", None),
        P("wide"),
        P("wide", None),
        P("wide"),
        P("wide", None),
        P("wide"),
        P("wide"),
        P("wide"),
        P("wide", None),
        P("wide"),
        P("wide", None),
        P("wide"),
    )
    return jax.shard_map(
        on_device, mesh=mesh, in_specs=in_specs, out_specs=out_specs, check_vma=False
    )
```

```python
from functools import partial
import math

import jax
import jax.numpy as jnp
from jax import lax
from jax.sharding import PartitionSpec as P

D = 768
HEADS = 12
HD = 64
FEAT = 32
SEGS = 24
BLOCK = 128

EPSILON = 1e-05
HIGHEST = lax.Precision.HIGHEST


def pieces(lens_row, seq_len):
    seg_end = jnp.cumsum(lens_row)
    seg_start = seg_end - lens_row
    places = jnp.arange(seq_len, dtype=jnp.int32)
    segment = jnp.sum((places[:, None] >= seg_end[None, :]).astype(jnp.int32), axis=1)
    slots = jnp.arange(SEGS, dtype=jnp.int32)
    begins = jnp.sum(jnp.where(segment[:, None] == slots[None, :], seg_start[None, :], 0), axis=1)
    position = places - begins
    valid = (segment < SEGS - 1).astype(jnp.float32)
    return (position, valid, segment)


def rotate(heads_field, position):
    half = HD // 2
    rates = jnp.exp(jnp.arange(half, dtype=jnp.float32) * (-2.0 * math.log(10000.0) / HD))
    angles = position.astype(jnp.float32)[:, None] * rates[None, :]
    cosine = jnp.cos(angles)[:, None, :]
    sine = jnp.sin(angles)[:, None, :]
    first = heads_field[..., :half]
    second = heads_field[..., half:]
    return jnp.concatenate(
        [first * cosine - second * sine, second * cosine + first * sine], axis=-1
    )


def featurize(rotated, features):
    table = features.reshape(HD, HEADS, FEAT)
    scores = jnp.einsum("lhe,ehm->lhm", rotated, table, precision=HIGHEST) * 0.125
    return jax.nn.elu(scores) + 1.0


def normalize(stream, gain, shift):
    average = jnp.mean(stream, axis=-1, keepdims=True)
    centered = stream - average
    variance = jnp.mean(centered * centered, axis=-1, keepdims=True)
    return centered * lax.rsqrt(variance + EPSILON) * gain + shift


def contract_rows(left, right):
    return lax.dot_general(
        left, right, (((0,), (0,)), ((), ())), preferred_element_type=jnp.float32
    )


def times_transposed(left, right):
    return lax.dot_general(
        left, right, (((1,), (1,)), ((), ())), preferred_element_type=jnp.float32
    )


def column_sums(matrix):
    return jnp.sum(matrix.astype(jnp.float32), axis=0)


def gather_rows(shard):
    return lax.all_gather(shard, "wide", axis=0, tiled=True)


def narrow_sum(share):
    size = lax.psum(1, "narrow")
    steps = size.bit_length() - 1
    assert 1 << steps == size
    me = lax.axis_index("narrow")
    rows = share.shape[0]
    assert rows % size == 0
    acc = share.astype(jnp.float32)
    for k in range(steps):
        half = acc.shape[0] // 2
        upper = ((me >> k) & 1) == 1
        lo, hi = acc[:half], acc[half:]
        keep = jnp.where(upper, hi, lo)
        send = jnp.where(upper, lo, hi).astype(jnp.bfloat16)
        pairs = [(i, i ^ (1 << k)) for i in range(size)]
        acc = keep + lax.ppermute(send, "narrow", pairs).astype(jnp.float32)
    part = acc.astype(jnp.bfloat16)
    for k in reversed(range(steps)):
        upper = ((me >> k) & 1) == 1
        pairs = [(i, i ^ (1 << k)) for i in range(size)]
        other = lax.ppermute(part, "narrow", pairs)
        part = jnp.where(upper, jnp.concatenate([other, part]), jnp.concatenate([part, other]))
    return part.astype(jnp.float32)


def reduce_rows(full):
    share = lax.psum_scatter(full.astype(jnp.bfloat16), "wide", scatter_dimension=0, tiled=True)
    return narrow_sum(share)


def gelu_parts(upper):
    cdf = 0.5 * (1.0 + lax.erf(upper * math.sqrt(0.5)))
    slope = cdf + upper * jnp.exp(-0.5 * upper * upper) * (1.0 / math.sqrt(2.0 * math.pi))
    return upper * cdf, slope


def to_blocks(field, nseq, width):
    seq_len = field.shape[0] // nseq
    nb = seq_len // BLOCK
    return jnp.transpose(field.reshape(nseq, nb, BLOCK, HEADS, width), (0, 3, 1, 2, 4))


def from_blocks(blocks):
    nseq, heads, nb, block, width = blocks.shape
    return jnp.transpose(blocks, (0, 2, 3, 1, 4)).reshape(nseq * nb * block, heads * width)


def window(blocks, fill=0):
    pad = [(0, 0)] * blocks.ndim
    pad[-3] = (1, 0)
    prev = jnp.pad(blocks, pad, constant_values=fill)[..., :-1, :, :]
    return jnp.concatenate([prev, blocks], axis=-2)


def unwindow(win):
    own = win[..., BLOCK:, :]
    nxt = win[..., 1:, :BLOCK, :]
    pad = [(0, 0)] * win.ndim
    pad[-3] = (0, 1)
    return own + jnp.pad(nxt, pad)


def as_columns(vectors, rows):
    cols = jnp.concatenate([v.reshape(rows, -1) for v in vectors], axis=1)
    pad = -cols.shape[1] % 128
    return jnp.pad(cols, ((0, 0), (0, pad)))


def on_device(
    tokens,
    cotangent,
    lengths,
    features,
    ln1_gain,
    ln1_bias,
    q_weight,
    q_bias,
    k_weight,
    k_bias,
    v_weight,
    v_bias,
    out_weight,
    out_bias,
    ln2_gain,
    ln2_bias,
    up_weight,
    up_bias,
    down_weight,
    down_bias,
):
    nseq = lengths.shape[0]
    total = tokens.shape[0]
    seq_len = total // nseq
    nb = seq_len // BLOCK
    shard_rows = ln1_gain.shape[0]
    wide = D // shard_rows

    small_shards = (ln1_gain, ln1_bias, q_bias, k_bias, v_bias, out_bias, ln2_gain, ln2_bias, down_bias, up_bias)
    small_cols = [piece.shape[0] // shard_rows for piece in small_shards]
    first = gather_rows(
        jnp.concatenate([q_weight, k_weight, v_weight, as_columns(small_shards, shard_rows)], axis=1)
    )
    query_mat = first[:, :D]
    key_mat = first[:, D:2 * D]
    value_mat = first[:, 2 * D:3 * D]
    smalls = []
    offset = 3 * D
    for cols in small_cols:
        smalls.append(first[:, offset:offset + cols].astype(jnp.float32).reshape(-1))
        offset += cols
    g1, b1, bq, bk, bv, bo, g2, b2, bd, bu = smalls
    ff = up_weight.shape[1]
    second = gather_rows(jnp.concatenate([out_weight, up_weight], axis=1))
    proj_mat = second[:, :D]
    up_mat = second[:, D:]
    down_mat = gather_rows(down_weight)

    position, valid, segment = jax.vmap(partial(pieces, seq_len=seq_len))(lengths)
    position = position.reshape(total)
    seg_blocks = segment.reshape(nseq, nb, BLOCK)
    seg_win = window(seg_blocks[..., None], fill=-1)[..., 0]
    rel_q = jnp.arange(BLOCK, dtype=jnp.int32)[:, None]
    rel_k = jnp.arange(2 * BLOCK, dtype=jnp.int32)[None, :]
    allowed = (rel_k <= rel_q + BLOCK)[None, None] & (
        seg_win[:, :, None, :] == seg_blocks[:, :, :, None]
    )
    allowed = allowed[:, None]
    valid_blk = valid.reshape(nseq, 1, nb, BLOCK, 1)

    stream = tokens.astype(jnp.float32)
    normed_one, norm_one_back = jax.vjp(normalize, stream, g1, b1)
    hidden_one = normed_one.astype(jnp.bfloat16)
    query_pre = jnp.dot(hidden_one, query_mat, preferred_element_type=jnp.float32) + bq
    key_pre = jnp.dot(hidden_one, key_mat, preferred_element_type=jnp.float32) + bk
    values = (jnp.dot(hidden_one, value_mat, preferred_element_type=jnp.float32) + bv).astype(jnp.bfloat16)

    def features_of(projected):
        return featurize(rotate(projected.reshape(total, HEADS, HD), position), features)

    query_feat, query_back = jax.vjp(features_of, query_pre)
    key_feat, key_back = jax.vjp(features_of, key_pre)
    pq = to_blocks(query_feat.astype(jnp.bfloat16).reshape(total, HEADS * FEAT), nseq, FEAT)
    pk = window(to_blocks(key_feat.astype(jnp.bfloat16).reshape(total, HEADS * FEAT), nseq, FEAT))
    vb = window(to_blocks(values, nseq, HD))

    scores = jnp.einsum("shnqf,shnkf->shnqk", pq, pk, preferred_element_type=jnp.float32)
    scores = jnp.where(allowed, scores, 0.0)
    denominator = jnp.sum(scores, axis=-1, keepdims=True)
    scores_low = scores.astype(jnp.bfloat16)
    numerator = jnp.einsum("shnqk,shnkd->shnqd", scores_low, vb, preferred_element_type=jnp.float32)
    mixed = numerator / denominator * valid_blk
    attended = from_blocks(mixed).astype(jnp.bfloat16)
    residual = stream + (jnp.dot(attended, proj_mat, preferred_element_type=jnp.float32) + bo)
    normed_two, norm_two_back = jax.vjp(normalize, residual, g2, b2)
    hidden_two = normed_two.astype(jnp.bfloat16)
    upper = jnp.dot(hidden_two, up_mat, preferred_element_type=jnp.float32) + bu
    activated, slope = gelu_parts(upper)
    act_low = activated.astype(jnp.bfloat16)

    upward = cotangent
    grad_out = upward.astype(jnp.float32)
    down_grad = contract_rows(act_low, upward).astype(jnp.bfloat16)
    down_grad, upward = lax.optimization_barrier((down_grad, upward))
    scattered_down = lax.psum_scatter(down_grad, "wide", scatter_dimension=0, tiled=True)
    grad_act = times_transposed(upward, down_mat)
    grad_upper = (grad_act * slope).astype(jnp.bfloat16)
    grad_hidden_two = times_transposed(grad_upper, up_mat)
    grad_residual_norm, gain_two_grad, shift_two_grad = norm_two_back(grad_hidden_two)
    grad_residual = grad_out + grad_residual_norm
    grad_proj_in = grad_residual.astype(jnp.bfloat16)
    grad_attended = times_transposed(grad_proj_in, proj_mat)
    up_grad = contract_rows(hidden_two, grad_upper).astype(jnp.bfloat16)
    proj_grad = contract_rows(attended, grad_proj_in).astype(jnp.bfloat16)
    packed_one = jnp.concatenate([up_grad, proj_grad], axis=1)
    packed_one, grad_attended = lax.optimization_barrier((packed_one, grad_attended))
    scattered_one = lax.psum_scatter(packed_one, "wide", scatter_dimension=0, tiled=True)
    down_bias_grad = column_sums(upward)
    up_bias_grad = column_sums(grad_upper)
    proj_bias_grad = column_sums(grad_proj_in)

    head_grad = to_blocks(grad_attended, nseq, HD)
    scaled = head_grad * valid_blk
    grad_num = (scaled / denominator).astype(jnp.bfloat16)
    grad_den = -jnp.sum(scaled * numerator, axis=-1, keepdims=True) / (denominator * denominator)
    grad_scores = jnp.einsum("shnqd,shnkd->shnqk", grad_num, vb, preferred_element_type=jnp.float32)
    grad_scores = (grad_scores + grad_den).astype(jnp.bfloat16)
    grad_scores = jnp.where(allowed, grad_scores, jnp.zeros((), jnp.bfloat16))
    grad_vwin = jnp.einsum("shnqk,shnqd->shnkd", scores_low, grad_num, preferred_element_type=jnp.float32)
    grad_value = from_blocks(unwindow(grad_vwin)).astype(jnp.bfloat16)
    grad_qf = jnp.einsum("shnqk,shnkf->shnqf", grad_scores, pk, preferred_element_type=jnp.float32)
    grad_kwin = jnp.einsum("shnqk,shnqf->shnkf", grad_scores, pq, preferred_element_type=jnp.float32)
    grad_qf = from_blocks(grad_qf).reshape(total, HEADS, FEAT)
    grad_kf = from_blocks(unwindow(grad_kwin)).reshape(total, HEADS, FEAT)
    grad_key = key_back(grad_kf)[0].astype(jnp.bfloat16)
    grad_query = query_back(grad_qf)[0].astype(jnp.bfloat16)
    grad_qkv = jnp.concatenate([grad_query, grad_key, grad_value], axis=1)
    scattered_down, scattered_one, grad_qkv = lax.optimization_barrier((scattered_down, scattered_one, grad_qkv))
    down_share = lax.psum(scattered_down, "narrow")
    share_one = lax.psum(scattered_one, "narrow")
    grad_hidden_one = times_transposed(grad_qkv, first[:, :3 * D])
    grad_stream_norm, gain_one_grad, shift_one_grad = norm_one_back(grad_hidden_one)
    qkv_grad = contract_rows(hidden_one, grad_qkv)
    qkv_bias_grad = column_sums(grad_qkv)

    small_grads = (
        gain_one_grad,
        shift_one_grad,
        qkv_bias_grad[:D],
        qkv_bias_grad[D:2 * D],
        qkv_bias_grad[2 * D:],
        proj_bias_grad,
        gain_two_grad,
        shift_two_grad,
        down_bias_grad,
        up_bias_grad,
    )
    packed_two = jnp.concatenate([qkv_grad, as_columns(small_grads, D)], axis=1)
    down_share, share_one, packed_two = lax.optimization_barrier((down_share, share_one, packed_two))
    down_share = down_share.astype(jnp.float32)
    up_share = share_one[:, :ff].astype(jnp.float32)
    proj_share = share_one[:, ff:].astype(jnp.float32)
    packed_two, act_late, residual_late, grad_residual_late, grad_stream_late = lax.optimization_barrier(
        (packed_two, act_low, residual, grad_residual, grad_stream_norm)
    )
    scattered_two = lax.psum_scatter(packed_two, "wide", scatter_dimension=0, tiled=True)
    result = residual_late + (jnp.dot(act_late, down_mat, preferred_element_type=jnp.float32) + bd)
    output = result.astype(jnp.bfloat16)
    input_grad = grad_residual_late + grad_stream_late
    scattered_two, output, input_grad = lax.optimization_barrier((scattered_two, output, input_grad))
    share_two = narrow_sum(scattered_two)
    small_out = []
    offset = 3 * D
    for cols in small_cols:
        small_out.append(share_two[:, offset:offset + cols].reshape(-1))
        offset += cols
    (
        gain_one_share,
        shift_one_share,
        query_bias_share,
        key_bias_share,
        value_bias_share,
        proj_bias_share,
        gain_two_share,
        shift_two_share,
        down_bias_share,
        up_bias_share,
    ) = small_out
    return (
        output,
        input_grad,
        gain_one_share,
        shift_one_share,
        share_two[:, :D],
        query_bias_share,
        share_two[:, D:2 * D],
        key_bias_share,
        share_two[:, 2 * D:3 * D],
        value_bias_share,
        proj_share,
        proj_bias_share,
        gain_two_share,
        shift_two_share,
        up_share,
        up_bias_share,
        down_share,
        down_bias_share,
    )


def solution(mesh):
    in_specs = (
        P(("wide", "narrow"), None),
        P(("wide", "narrow"), None),
        P(("wide", "narrow"), None),
        P(),
        P("wide"),
        P("wide"),
        P("wide", None),
        P("wide"),
        P("wide", None),
        P("wide"),
        P("wide", None),
        P("wide"),
        P("wide", None),
        P("wide"),
        P("wide"),
        P("wide"),
        P("wide", None),
        P("wide"),
        P("wide", None),
        P("wide"),
    )
    out_specs = (
        P(("wide", "narrow"), None),
        P(("wide", "narrow"), None),
        P("wide"),
        P("wide"),
        P("wide", None),
        P("wide"),
        P("wide", None),
        P("wide"),
        P("wide", None),
        P("wide"),
        P("wide", None),
        P("wide"),
        P("wide"),
        P("wide"),
        P("wide", None),
        P("wide"),
        P("wide", None),
        P("wide"),
    )
    return jax.shard_map(
        on_device, mesh=mesh, in_specs=in_specs, out_specs=out_specs, check_vma=False
    )
```

```python
from functools import partial
import math

import jax
import jax.numpy as jnp
from jax import lax
from jax.sharding import PartitionSpec as P
from jax.experimental import pallas as pl
from jax.experimental.pallas import tpu as pltpu

D = 768
HEADS = 12
HD = 64
FEAT = 32
SEGS = 24
BLOCK = 128

EPSILON = 1e-05
HIGHEST = lax.Precision.HIGHEST


def pieces(lens_row, seq_len):
    seg_end = jnp.cumsum(lens_row)
    seg_start = seg_end - lens_row
    places = jnp.arange(seq_len, dtype=jnp.int32)
    segment = jnp.sum((places[:, None] >= seg_end[None, :]).astype(jnp.int32), axis=1)
    slots = jnp.arange(SEGS, dtype=jnp.int32)
    begins = jnp.sum(jnp.where(segment[:, None] == slots[None, :], seg_start[None, :], 0), axis=1)
    position = places - begins
    valid = (segment < SEGS - 1).astype(jnp.float32)
    return (position, valid, segment)


def rotate(heads_field, position):
    half = HD // 2
    rates = jnp.exp(jnp.arange(half, dtype=jnp.float32) * (-2.0 * math.log(10000.0) / HD))
    angles = position.astype(jnp.float32)[:, None] * rates[None, :]
    cosine = jnp.cos(angles)[:, None, :]
    sine = jnp.sin(angles)[:, None, :]
    first = heads_field[..., :half]
    second = heads_field[..., half:]
    return jnp.concatenate(
        [first * cosine - second * sine, second * cosine + first * sine], axis=-1
    )


def featurize(rotated, features):
    table = features.reshape(HD, HEADS, FEAT)
    scores = jnp.einsum("lhe,ehm->lhm", rotated, table, precision=HIGHEST) * 0.125
    return jax.nn.elu(scores) + 1.0


def normalize(stream, gain, shift):
    average = jnp.mean(stream, axis=-1, keepdims=True)
    centered = stream - average
    variance = jnp.mean(centered * centered, axis=-1, keepdims=True)
    return centered * lax.rsqrt(variance + EPSILON) * gain + shift


def contract_rows(left, right):
    return lax.dot_general(
        left, right, (((0,), (0,)), ((), ())), preferred_element_type=jnp.float32
    )


def times_transposed(left, right):
    return lax.dot_general(
        left, right, (((1,), (1,)), ((), ())), preferred_element_type=jnp.float32
    )


def column_sums(matrix):
    return jnp.sum(matrix.astype(jnp.float32), axis=0)


def gather_rows(shard):
    return lax.all_gather(shard, "wide", axis=0, tiled=True)


def narrow_sum(share):
    size = lax.psum(1, "narrow")
    steps = size.bit_length() - 1
    assert 1 << steps == size
    me = lax.axis_index("narrow")
    rows = share.shape[0]
    assert rows % size == 0
    acc = share.astype(jnp.float32)
    for k in range(steps):
        half = acc.shape[0] // 2
        upper = ((me >> k) & 1) == 1
        lo, hi = acc[:half], acc[half:]
        keep = jnp.where(upper, hi, lo)
        send = jnp.where(upper, lo, hi).astype(jnp.bfloat16)
        pairs = [(i, i ^ (1 << k)) for i in range(size)]
        acc = keep + lax.ppermute(send, "narrow", pairs).astype(jnp.float32)
    part = acc.astype(jnp.bfloat16)
    for k in reversed(range(steps)):
        upper = ((me >> k) & 1) == 1
        pairs = [(i, i ^ (1 << k)) for i in range(size)]
        other = lax.ppermute(part, "narrow", pairs)
        part = jnp.where(upper, jnp.concatenate([other, part]), jnp.concatenate([part, other]))
    return part.astype(jnp.float32)


def reduce_rows(full):
    share = lax.psum_scatter(full.astype(jnp.bfloat16), "wide", scatter_dimension=0, tiled=True)
    return narrow_sum(share)


def gelu_parts(upper):
    cdf = 0.5 * (1.0 + lax.erf(upper * math.sqrt(0.5)))
    slope = cdf + upper * jnp.exp(-0.5 * upper * upper) * (1.0 / math.sqrt(2.0 * math.pi))
    return upper * cdf, slope


def to_blocks(field, nseq, width):
    seq_len = field.shape[0] // nseq
    nb = seq_len // BLOCK
    return jnp.transpose(field.reshape(nseq, nb, BLOCK, HEADS, width), (0, 3, 1, 2, 4))


def from_blocks(blocks):
    nseq, heads, nb, block, width = blocks.shape
    return jnp.transpose(blocks, (0, 2, 3, 1, 4)).reshape(nseq * nb * block, heads * width)


def window(blocks, fill=0):
    pad = [(0, 0)] * blocks.ndim
    pad[-3] = (1, 0)
    prev = jnp.pad(blocks, pad, constant_values=fill)[..., :-1, :, :]
    return jnp.concatenate([prev, blocks], axis=-2)


def unwindow(win):
    own = win[..., BLOCK:, :]
    nxt = win[..., 1:, :BLOCK, :]
    pad = [(0, 0)] * win.ndim
    pad[-3] = (0, 1)
    return own + jnp.pad(nxt, pad)


def _scores(pq, pk, h, mask):
    q = pq[:, h * FEAT:(h + 1) * FEAT]
    k = pk[:, h * FEAT:(h + 1) * FEAT]
    s = lax.dot_general(q, k, (((1,), (1,)), ((), ())), preferred_element_type=jnp.float32)
    return q, k, jnp.where(mask, s, 0.0)


def _attn_fwd_kernel(pq_ref, pkp_ref, pkc_ref, vbp_ref, vbc_ref, mask_ref, valid_ref, o_ref):
    mask = mask_ref[0] > 0.5
    valid = valid_ref[...]
    pq = pq_ref[...]
    pk = jnp.concatenate([pkp_ref[...], pkc_ref[...]], axis=0)
    vb = jnp.concatenate([vbp_ref[...], vbc_ref[...]], axis=0)
    for h in range(HEADS):
        _, _, a = _scores(pq, pk, h, mask)
        den = jnp.sum(a, axis=1, keepdims=True)
        v = vb[:, h * HD:(h + 1) * HD]
        num = jnp.dot(a.astype(jnp.bfloat16), v, preferred_element_type=jnp.float32)
        o_ref[:, h * HD:(h + 1) * HD] = (num / den * valid).astype(o_ref.dtype)


def _attn_bwd_kernel(pq_ref, pkp_ref, pkc_ref, vbp_ref, vbc_ref, mask_ref, valid_ref, g_ref, gq_ref, gk_ref, gv_ref):
    i = pl.program_id(1)

    @pl.when(i == 0)
    def _():
        gk_ref[...] = jnp.zeros_like(gk_ref)
        gv_ref[...] = jnp.zeros_like(gv_ref)

    mask = mask_ref[0] > 0.5
    valid = valid_ref[...]
    pq = pq_ref[...]
    pk = jnp.concatenate([pkp_ref[...], pkc_ref[...]], axis=0)
    vb = jnp.concatenate([vbp_ref[...], vbc_ref[...]], axis=0)
    prev = jnp.maximum(i - 1, 0)
    gks = []
    gvs = []
    for h in range(HEADS):
        q, k, a = _scores(pq, pk, h, mask)
        den = jnp.sum(a, axis=1, keepdims=True)
        a_low = a.astype(jnp.bfloat16)
        v = vb[:, h * HD:(h + 1) * HD]
        num = jnp.dot(a_low, v, preferred_element_type=jnp.float32)
        g = g_ref[:, h * HD:(h + 1) * HD] * valid
        gnum = (g / den).astype(jnp.bfloat16)
        gden = -jnp.sum(g * num, axis=1, keepdims=True) / (den * den)
        ga = lax.dot_general(gnum, v, (((1,), (1,)), ((), ())), preferred_element_type=jnp.float32)
        ga = jnp.where(mask, (ga + gden).astype(jnp.bfloat16), jnp.zeros((), jnp.bfloat16))
        gq_ref[:, h * FEAT:(h + 1) * FEAT] = jnp.dot(ga, k, preferred_element_type=jnp.float32)
        gk_win = lax.dot_general(ga, q, (((0,), (0,)), ((), ())), preferred_element_type=jnp.float32)
        gv_win = lax.dot_general(a_low, gnum, (((0,), (0,)), ((), ())), preferred_element_type=jnp.float32)
        gks.append(gk_win)
        gvs.append(gv_win)
    gk_all = jnp.concatenate(gks, axis=1)
    gv_all = jnp.concatenate(gvs, axis=1)
    gk_ref[0, i] += gk_all[BLOCK:]
    gv_ref[0, i] += gv_all[BLOCK:]
    gk_ref[0, prev] += gk_all[:BLOCK]
    gv_ref[0, prev] += gv_all[:BLOCK]


def _specs(nb):
    def at(i_shift):
        def index(s, i):
            return (s * nb + jnp.maximum(i + i_shift, 0), 0)
        return index
    return [
        pl.BlockSpec((BLOCK, HEADS * FEAT), at(0)),
        pl.BlockSpec((BLOCK, HEADS * FEAT), at(-1)),
        pl.BlockSpec((BLOCK, HEADS * FEAT), at(0)),
        pl.BlockSpec((BLOCK, HEADS * HD), at(-1)),
        pl.BlockSpec((BLOCK, HEADS * HD), at(0)),
        pl.BlockSpec((1, BLOCK, 2 * BLOCK), lambda s, i: (s * nb + i, 0, 0)),
        pl.BlockSpec((BLOCK, 1), at(0)),
    ]


def attention_forward(pq, pk, vb, mask, valid, nseq):
    total = pq.shape[0]
    nb = total // nseq // BLOCK
    flops = 2 * total * 2 * BLOCK * HEADS * (FEAT + HD)
    return pl.pallas_call(
        _attn_fwd_kernel,
        grid=(nseq, nb),
        in_specs=_specs(nb),
        out_specs=pl.BlockSpec((BLOCK, HEADS * HD), lambda s, i: (s * nb + i, 0)),
        out_shape=jax.ShapeDtypeStruct((total, HEADS * HD), jnp.bfloat16),
        compiler_params=pltpu.CompilerParams(dimension_semantics=("arbitrary", "arbitrary")),
        cost_estimate=pl.CostEstimate(flops=flops, transcendentals=0, bytes_accessed=total * (384 * 4 + 768 * 6 + 1024)),
    )(pq, pk, pk, vb, vb, mask, valid)


def attention_backward(pq, pk, vb, mask, valid, grad, nseq):
    total = pq.shape[0]
    seq_len = total // nseq
    nb = seq_len // BLOCK
    flops = 2 * total * 2 * BLOCK * HEADS * (3 * FEAT + 3 * HD)
    gq, gk, gv = pl.pallas_call(
        _attn_bwd_kernel,
        grid=(nseq, nb),
        in_specs=_specs(nb) + [pl.BlockSpec((BLOCK, HEADS * HD), lambda s, i: (s * nb + i, 0))],
        out_specs=[
            pl.BlockSpec((BLOCK, HEADS * FEAT), lambda s, i: (s * nb + i, 0)),
            pl.BlockSpec((1, nb, BLOCK, HEADS * FEAT), lambda s, i: (s, 0, 0, 0)),
            pl.BlockSpec((1, nb, BLOCK, HEADS * HD), lambda s, i: (s, 0, 0, 0)),
        ],
        out_shape=[
            jax.ShapeDtypeStruct((total, HEADS * FEAT), jnp.float32),
            jax.ShapeDtypeStruct((nseq, nb, BLOCK, HEADS * FEAT), jnp.float32),
            jax.ShapeDtypeStruct((nseq, nb, BLOCK, HEADS * HD), jnp.float32),
        ],
        compiler_params=pltpu.CompilerParams(dimension_semantics=("arbitrary", "arbitrary")),
        cost_estimate=pl.CostEstimate(flops=flops, transcendentals=0, bytes_accessed=total * (384 * 12 + 768 * 14 + 1024)),
    )(pq, pk, pk, vb, vb, mask, valid, grad)
    return gq, gk.reshape(total, HEADS * FEAT), gv.reshape(total, HEADS * HD)


def as_columns(vectors, rows):
    cols = jnp.concatenate([v.reshape(rows, -1) for v in vectors], axis=1)
    pad = -cols.shape[1] % 128
    return jnp.pad(cols, ((0, 0), (0, pad)))


def on_device(
    tokens,
    cotangent,
    lengths,
    features,
    ln1_gain,
    ln1_bias,
    q_weight,
    q_bias,
    k_weight,
    k_bias,
    v_weight,
    v_bias,
    out_weight,
    out_bias,
    ln2_gain,
    ln2_bias,
    up_weight,
    up_bias,
    down_weight,
    down_bias,
):
    nseq = lengths.shape[0]
    total = tokens.shape[0]
    seq_len = total // nseq
    nb = seq_len // BLOCK
    shard_rows = ln1_gain.shape[0]
    wide = D // shard_rows

    small_shards = (ln1_gain, ln1_bias, q_bias, k_bias, v_bias, out_bias, ln2_gain, ln2_bias, down_bias, up_bias)
    small_cols = [piece.shape[0] // shard_rows for piece in small_shards]
    first = gather_rows(
        jnp.concatenate([q_weight, k_weight, v_weight, as_columns(small_shards, shard_rows)], axis=1)
    )
    query_mat = first[:, :D]
    key_mat = first[:, D:2 * D]
    value_mat = first[:, 2 * D:3 * D]
    smalls = []
    offset = 3 * D
    for cols in small_cols:
        smalls.append(first[:, offset:offset + cols].astype(jnp.float32).reshape(-1))
        offset += cols
    g1, b1, bq, bk, bv, bo, g2, b2, bd, bu = smalls
    ff = up_weight.shape[1]
    second = gather_rows(jnp.concatenate([out_weight, up_weight], axis=1))
    proj_mat = second[:, :D]
    up_mat = second[:, D:]
    down_mat = gather_rows(down_weight)

    position, valid, segment = jax.vmap(partial(pieces, seq_len=seq_len))(lengths)
    position = position.reshape(total)
    seg_blocks = segment.reshape(nseq, nb, BLOCK)
    seg_win = window(seg_blocks[..., None], fill=-1)[..., 0]
    rel_q = jnp.arange(BLOCK, dtype=jnp.int32)[:, None]
    rel_k = jnp.arange(2 * BLOCK, dtype=jnp.int32)[None, :]
    allowed = (rel_k <= rel_q + BLOCK)[None, None] & (
        seg_win[:, :, None, :] == seg_blocks[:, :, :, None]
    )
    mask = allowed.reshape(nseq * nb, BLOCK, 2 * BLOCK).astype(jnp.float32)
    valid_col = valid.reshape(total, 1)

    stream = tokens.astype(jnp.float32)
    normed_one, norm_one_back = jax.vjp(normalize, stream, g1, b1)
    hidden_one = normed_one.astype(jnp.bfloat16)
    query_pre = jnp.dot(hidden_one, query_mat, preferred_element_type=jnp.float32) + bq
    key_pre = jnp.dot(hidden_one, key_mat, preferred_element_type=jnp.float32) + bk
    values = (jnp.dot(hidden_one, value_mat, preferred_element_type=jnp.float32) + bv).astype(jnp.bfloat16)

    def features_of(projected):
        return featurize(rotate(projected.reshape(total, HEADS, HD), position), features)

    query_feat, query_back = jax.vjp(features_of, query_pre)
    key_feat, key_back = jax.vjp(features_of, key_pre)
    pq = query_feat.astype(jnp.bfloat16).reshape(total, HEADS * FEAT)
    pk = key_feat.astype(jnp.bfloat16).reshape(total, HEADS * FEAT)
    attended = attention_forward(pq, pk, values, mask, valid_col, nseq)
    residual = stream + (jnp.dot(attended, proj_mat, preferred_element_type=jnp.float32) + bo)
    normed_two, norm_two_back = jax.vjp(normalize, residual, g2, b2)
    hidden_two = normed_two.astype(jnp.bfloat16)
    upper = jnp.dot(hidden_two, up_mat, preferred_element_type=jnp.float32) + bu
    activated, slope = gelu_parts(upper)
    act_low = activated.astype(jnp.bfloat16)

    upward = cotangent
    grad_out = upward.astype(jnp.float32)
    down_grad = contract_rows(act_low, upward).astype(jnp.bfloat16)
    down_grad, upward = lax.optimization_barrier((down_grad, upward))
    scattered_down = lax.psum_scatter(down_grad, "wide", scatter_dimension=0, tiled=True)
    grad_act = times_transposed(upward, down_mat)
    grad_upper = (grad_act * slope).astype(jnp.bfloat16)
    grad_hidden_two = times_transposed(grad_upper, up_mat)
    grad_residual_norm, gain_two_grad, shift_two_grad = norm_two_back(grad_hidden_two)
    grad_residual = grad_out + grad_residual_norm
    grad_proj_in = grad_residual.astype(jnp.bfloat16)
    grad_attended = times_transposed(grad_proj_in, proj_mat)
    up_grad = contract_rows(hidden_two, grad_upper).astype(jnp.bfloat16)
    proj_grad = contract_rows(attended, grad_proj_in).astype(jnp.bfloat16)
    packed_one = jnp.concatenate([up_grad, proj_grad], axis=1)
    packed_one, grad_attended = lax.optimization_barrier((packed_one, grad_attended))
    scattered_one = lax.psum_scatter(packed_one, "wide", scatter_dimension=0, tiled=True)
    down_bias_grad = column_sums(upward)
    up_bias_grad = column_sums(grad_upper)
    proj_bias_grad = column_sums(grad_proj_in)

    grad_qf, grad_kf, grad_vf = attention_backward(pq, pk, values, mask, valid_col, grad_attended, nseq)
    grad_value = grad_vf.astype(jnp.bfloat16)
    grad_qf = grad_qf.reshape(total, HEADS, FEAT)
    grad_kf = grad_kf.reshape(total, HEADS, FEAT)
    grad_key = key_back(grad_kf)[0].astype(jnp.bfloat16)
    grad_query = query_back(grad_qf)[0].astype(jnp.bfloat16)
    grad_qkv = jnp.concatenate([grad_query, grad_key, grad_value], axis=1)
    scattered_down, scattered_one, grad_qkv = lax.optimization_barrier((scattered_down, scattered_one, grad_qkv))
    down_share = lax.psum(scattered_down, "narrow")
    share_one = lax.psum(scattered_one, "narrow")
    grad_hidden_one = times_transposed(grad_qkv, first[:, :3 * D])
    grad_stream_norm, gain_one_grad, shift_one_grad = norm_one_back(grad_hidden_one)
    qkv_grad = contract_rows(hidden_one, grad_qkv)
    qkv_bias_grad = column_sums(grad_qkv)

    small_grads = (
        gain_one_grad,
        shift_one_grad,
        qkv_bias_grad[:D],
        qkv_bias_grad[D:2 * D],
        qkv_bias_grad[2 * D:],
        proj_bias_grad,
        gain_two_grad,
        shift_two_grad,
        down_bias_grad,
        up_bias_grad,
    )
    packed_two = jnp.concatenate([qkv_grad, as_columns(small_grads, D)], axis=1)
    down_share, share_one, packed_two = lax.optimization_barrier((down_share, share_one, packed_two))
    down_share = down_share.astype(jnp.float32)
    up_share = share_one[:, :ff].astype(jnp.float32)
    proj_share = share_one[:, ff:].astype(jnp.float32)
    packed_two, act_late, residual_late, grad_residual_late, grad_stream_late = lax.optimization_barrier(
        (packed_two, act_low, residual, grad_residual, grad_stream_norm)
    )
    scattered_two = lax.psum_scatter(packed_two, "wide", scatter_dimension=0, tiled=True)
    result = residual_late + (jnp.dot(act_late, down_mat, preferred_element_type=jnp.float32) + bd)
    output = result.astype(jnp.bfloat16)
    input_grad = grad_residual_late + grad_stream_late
    scattered_two, output, input_grad = lax.optimization_barrier((scattered_two, output, input_grad))
    share_two = narrow_sum(scattered_two)
    small_out = []
    offset = 3 * D
    for cols in small_cols:
        small_out.append(share_two[:, offset:offset + cols].reshape(-1))
        offset += cols
    (
        gain_one_share,
        shift_one_share,
        query_bias_share,
        key_bias_share,
        value_bias_share,
        proj_bias_share,
        gain_two_share,
        shift_two_share,
        down_bias_share,
        up_bias_share,
    ) = small_out
    return (
        output,
        input_grad,
        gain_one_share,
        shift_one_share,
        share_two[:, :D],
        query_bias_share,
        share_two[:, D:2 * D],
        key_bias_share,
        share_two[:, 2 * D:3 * D],
        value_bias_share,
        proj_share,
        proj_bias_share,
        gain_two_share,
        shift_two_share,
        up_share,
        up_bias_share,
        down_share,
        down_bias_share,
    )


def solution(mesh):
    in_specs = (
        P(("wide", "narrow"), None),
        P(("wide", "narrow"), None),
        P(("wide", "narrow"), None),
        P(),
        P("wide"),
        P("wide"),
        P("wide", None),
        P("wide"),
        P("wide", None),
        P("wide"),
        P("wide", None),
        P("wide"),
        P("wide", None),
        P("wide"),
        P("wide"),
        P("wide"),
        P("wide", None),
        P("wide"),
        P("wide", None),
        P("wide"),
    )
    out_specs = (
        P(("wide", "narrow"), None),
        P(("wide", "narrow"), None),
        P("wide"),
        P("wide"),
        P("wide", None),
        P("wide"),
        P("wide", None),
        P("wide"),
        P("wide", None),
        P("wide"),
        P("wide", None),
        P("wide"),
        P("wide"),
        P("wide"),
        P("wide", None),
        P("wide"),
        P("wide", None),
        P("wide"),
    )
    return jax.shard_map(
        on_device, mesh=mesh, in_specs=in_specs, out_specs=out_specs, check_vma=False
    )
```

```python
from functools import partial
import math

import jax
import jax.numpy as jnp
from jax import lax
from jax.sharding import PartitionSpec as P

D = 768
HEADS = 12
HD = 64
FEAT = 32
SEGS = 24
BLOCK = 128

EPSILON = 1e-05
HIGHEST = lax.Precision.HIGHEST


def pieces(lens_row, seq_len):
    seg_end = jnp.cumsum(lens_row)
    seg_start = seg_end - lens_row
    places = jnp.arange(seq_len, dtype=jnp.int32)
    segment = jnp.sum((places[:, None] >= seg_end[None, :]).astype(jnp.int32), axis=1)
    slots = jnp.arange(SEGS, dtype=jnp.int32)
    begins = jnp.sum(jnp.where(segment[:, None] == slots[None, :], seg_start[None, :], 0), axis=1)
    position = places - begins
    valid = (segment < SEGS - 1).astype(jnp.float32)
    return (position, valid, segment)


def rotate(heads_field, position):
    half = HD // 2
    rates = jnp.exp(jnp.arange(half, dtype=jnp.float32) * (-2.0 * math.log(10000.0) / HD))
    angles = position.astype(jnp.float32)[:, None] * rates[None, :]
    cosine = jnp.cos(angles)[:, None, :]
    sine = jnp.sin(angles)[:, None, :]
    first = heads_field[..., :half]
    second = heads_field[..., half:]
    return jnp.concatenate(
        [first * cosine - second * sine, second * cosine + first * sine], axis=-1
    )


def featurize(rotated, features):
    table = features.reshape(HD, HEADS, FEAT)
    scores = jnp.einsum("lhe,ehm->lhm", rotated, table, precision=HIGHEST) * 0.125
    return jax.nn.elu(scores) + 1.0


def normalize(stream, gain, shift):
    average = jnp.mean(stream, axis=-1, keepdims=True)
    centered = stream - average
    variance = jnp.mean(centered * centered, axis=-1, keepdims=True)
    return centered * lax.rsqrt(variance + EPSILON) * gain + shift


def contract_rows(left, right):
    return lax.dot_general(
        left, right, (((0,), (0,)), ((), ())), preferred_element_type=jnp.float32
    )


def times_transposed(left, right):
    return lax.dot_general(
        left, right, (((1,), (1,)), ((), ())), preferred_element_type=jnp.float32
    )


def column_sums(matrix):
    return jnp.sum(matrix.astype(jnp.float32), axis=0)


def gather_rows(shard):
    return lax.all_gather(shard, "wide", axis=0, tiled=True)


def narrow_sum(share):
    size = lax.psum(1, "narrow")
    steps = size.bit_length() - 1
    assert 1 << steps == size
    me = lax.axis_index("narrow")
    rows = share.shape[0]
    assert rows % size == 0
    acc = share.astype(jnp.float32)
    for k in range(steps):
        half = acc.shape[0] // 2
        upper = ((me >> k) & 1) == 1
        lo, hi = acc[:half], acc[half:]
        keep = jnp.where(upper, hi, lo)
        send = jnp.where(upper, lo, hi).astype(jnp.bfloat16)
        pairs = [(i, i ^ (1 << k)) for i in range(size)]
        acc = keep + lax.ppermute(send, "narrow", pairs).astype(jnp.float32)
    part = acc.astype(jnp.bfloat16)
    for k in reversed(range(steps)):
        upper = ((me >> k) & 1) == 1
        pairs = [(i, i ^ (1 << k)) for i in range(size)]
        other = lax.ppermute(part, "narrow", pairs)
        part = jnp.where(upper, jnp.concatenate([other, part]), jnp.concatenate([part, other]))
    return part.astype(jnp.float32)


def reduce_rows(full):
    share = lax.psum_scatter(full.astype(jnp.bfloat16), "wide", scatter_dimension=0, tiled=True)
    return narrow_sum(share)


def gelu_parts(upper):
    cdf = 0.5 * (1.0 + lax.erf(upper * math.sqrt(0.5)))
    slope = cdf + upper * jnp.exp(-0.5 * upper * upper) * (1.0 / math.sqrt(2.0 * math.pi))
    return upper * cdf, slope


def to_blocks(field, nseq, width):
    seq_len = field.shape[0] // nseq
    nb = seq_len // BLOCK
    return jnp.transpose(field.reshape(nseq, nb, BLOCK, HEADS, width), (0, 3, 1, 2, 4))


def from_blocks(blocks):
    nseq, heads, nb, block, width = blocks.shape
    return jnp.transpose(blocks, (0, 2, 3, 1, 4)).reshape(nseq * nb * block, heads * width)


def window(blocks, fill=0):
    pad = [(0, 0)] * blocks.ndim
    pad[-3] = (1, 0)
    prev = jnp.pad(blocks, pad, constant_values=fill)[..., :-1, :, :]
    return jnp.concatenate([prev, blocks], axis=-2)


def unwindow(win):
    own = win[..., BLOCK:, :]
    nxt = win[..., 1:, :BLOCK, :]
    pad = [(0, 0)] * win.ndim
    pad[-3] = (0, 1)
    return own + jnp.pad(nxt, pad)


def as_columns(vectors, rows):
    return jnp.concatenate([v.reshape(rows, -1) for v in vectors], axis=1)


def on_device(
    tokens,
    cotangent,
    lengths,
    features,
    ln1_gain,
    ln1_bias,
    q_weight,
    q_bias,
    k_weight,
    k_bias,
    v_weight,
    v_bias,
    out_weight,
    out_bias,
    ln2_gain,
    ln2_bias,
    up_weight,
    up_bias,
    down_weight,
    down_bias,
):
    nseq = lengths.shape[0]
    total = tokens.shape[0]
    seq_len = total // nseq
    nb = seq_len // BLOCK
    shard_rows = ln1_gain.shape[0]
    wide = D // shard_rows

    small_shards = (ln1_gain, ln1_bias, q_bias, k_bias, v_bias, out_bias, ln2_gain, ln2_bias, down_bias, up_bias)
    small_cols = [piece.shape[0] // shard_rows for piece in small_shards]
    first = gather_rows(
        jnp.concatenate([q_weight, k_weight, v_weight, as_columns(small_shards, shard_rows)], axis=1)
    )
    query_mat = first[:, :D]
    key_mat = first[:, D:2 * D]
    value_mat = first[:, 2 * D:3 * D]
    smalls = []
    offset = 3 * D
    for cols in small_cols:
        smalls.append(first[:, offset:offset + cols].astype(jnp.float32).reshape(-1))
        offset += cols
    g1, b1, bq, bk, bv, bo, g2, b2, bd, bu = smalls
    ff = up_weight.shape[1]
    second = gather_rows(jnp.concatenate([out_weight, up_weight], axis=1))
    proj_mat = second[:, :D]
    up_mat = second[:, D:]
    down_mat = gather_rows(down_weight)

    position, valid, segment = jax.vmap(partial(pieces, seq_len=seq_len))(lengths)
    position = position.reshape(total)
    seg_blocks = segment.reshape(nseq, nb, BLOCK)
    seg_win = window(seg_blocks[..., None], fill=-1)[..., 0]
    rel_q = jnp.arange(BLOCK, dtype=jnp.int32)[:, None]
    rel_k = jnp.arange(2 * BLOCK, dtype=jnp.int32)[None, :]
    allowed = (rel_k <= rel_q + BLOCK)[None, None] & (
        seg_win[:, :, None, :] == seg_blocks[:, :, :, None]
    )
    allowed = allowed[:, None]
    valid_blk = valid.reshape(nseq, 1, nb, BLOCK, 1)

    stream = tokens.astype(jnp.float32)
    normed_one, norm_one_back = jax.vjp(normalize, stream, g1, b1)
    hidden_one = normed_one.astype(jnp.bfloat16)
    query_pre = jnp.dot(hidden_one, query_mat, preferred_element_type=jnp.float32) + bq
    key_pre = jnp.dot(hidden_one, key_mat, preferred_element_type=jnp.float32) + bk
    values = (jnp.dot(hidden_one, value_mat, preferred_element_type=jnp.float32) + bv).astype(jnp.bfloat16)

    def features_of(projected):
        return featurize(rotate(projected.reshape(total, HEADS, HD), position), features)

    query_feat, query_back = jax.vjp(features_of, query_pre)
    key_feat, key_back = jax.vjp(features_of, key_pre)
    pq = to_blocks(query_feat.astype(jnp.bfloat16).reshape(total, HEADS * FEAT), nseq, FEAT)
    pk = window(to_blocks(key_feat.astype(jnp.bfloat16).reshape(total, HEADS * FEAT), nseq, FEAT))
    vb = window(to_blocks(values, nseq, HD))

    scores = jnp.einsum("shnqf,shnkf->shnqk", pq, pk, preferred_element_type=jnp.float32)
    scores = jnp.where(allowed, scores, 0.0)
    denominator = jnp.sum(scores, axis=-1, keepdims=True)
    scores_low = scores.astype(jnp.bfloat16)
    numerator = jnp.einsum("shnqk,shnkd->shnqd", scores_low, vb, preferred_element_type=jnp.float32)
    mixed = numerator / denominator * valid_blk
    attended = from_blocks(mixed).astype(jnp.bfloat16)
    residual = stream + (jnp.dot(attended, proj_mat, preferred_element_type=jnp.float32) + bo)
    normed_two, norm_two_back = jax.vjp(normalize, residual, g2, b2)
    hidden_two = normed_two.astype(jnp.bfloat16)
    upper = jnp.dot(hidden_two, up_mat, preferred_element_type=jnp.float32) + bu
    activated, slope = gelu_parts(upper)
    act_low = activated.astype(jnp.bfloat16)
    result = residual + (jnp.dot(act_low, down_mat, preferred_element_type=jnp.float32) + bd)
    output = result.astype(jnp.bfloat16)

    upward = cotangent
    grad_out = upward.astype(jnp.float32)
    down_grad = contract_rows(act_low, upward).astype(jnp.bfloat16)
    down_grad, upward = lax.optimization_barrier((down_grad, upward))
    scattered_down = lax.psum_scatter(down_grad, "wide", scatter_dimension=0, tiled=True)
    grad_act = times_transposed(upward, down_mat)
    grad_upper = (grad_act * slope).astype(jnp.bfloat16)
    grad_hidden_two = times_transposed(grad_upper, up_mat)
    grad_residual_norm, gain_two_grad, shift_two_grad = norm_two_back(grad_hidden_two)
    grad_residual = grad_out + grad_residual_norm
    grad_proj_in = grad_residual.astype(jnp.bfloat16)
    grad_attended = times_transposed(grad_proj_in, proj_mat)
    up_grad = contract_rows(hidden_two, grad_upper).astype(jnp.bfloat16)
    proj_grad = contract_rows(attended, grad_proj_in).astype(jnp.bfloat16)
    packed_one = jnp.concatenate([up_grad, proj_grad], axis=1)
    packed_one, grad_attended = lax.optimization_barrier((packed_one, grad_attended))
    scattered_one = lax.psum_scatter(packed_one, "wide", scatter_dimension=0, tiled=True)
    down_bias_grad = column_sums(upward)
    up_bias_grad = column_sums(grad_upper)
    proj_bias_grad = column_sums(grad_proj_in)

    head_grad = to_blocks(grad_attended, nseq, HD)
    scaled = head_grad * valid_blk
    grad_num = (scaled / denominator).astype(jnp.bfloat16)
    grad_den = -jnp.sum(scaled * numerator, axis=-1, keepdims=True) / (denominator * denominator)
    grad_scores = jnp.einsum("shnqd,shnkd->shnqk", grad_num, vb, preferred_element_type=jnp.float32)
    grad_scores = (grad_scores + grad_den).astype(jnp.bfloat16)
    grad_scores = jnp.where(allowed, grad_scores, jnp.zeros((), jnp.bfloat16))
    grad_vwin = jnp.einsum("shnqk,shnqd->shnkd", scores_low, grad_num, preferred_element_type=jnp.float32)
    grad_value = from_blocks(unwindow(grad_vwin)).astype(jnp.bfloat16)
    grad_qf = jnp.einsum("shnqk,shnkf->shnqf", grad_scores, pk, preferred_element_type=jnp.float32)
    grad_kwin = jnp.einsum("shnqk,shnqf->shnkf", grad_scores, pq, preferred_element_type=jnp.float32)
    scattered_down, scattered_one, grad_qf, grad_kwin = lax.optimization_barrier(
        (scattered_down, scattered_one, grad_qf, grad_kwin)
    )
    grad_qf = from_blocks(grad_qf).reshape(total, HEADS, FEAT)
    grad_kf = from_blocks(unwindow(grad_kwin)).reshape(total, HEADS, FEAT)
    grad_key = key_back(grad_kf)[0].astype(jnp.bfloat16)
    grad_query = query_back(grad_qf)[0].astype(jnp.bfloat16)
    grad_qkv = jnp.concatenate([grad_query, grad_key, grad_value], axis=1)
    down_share = lax.psum(scattered_down, "narrow")
    share_one = lax.psum(scattered_one, "narrow")
    grad_hidden_one = times_transposed(grad_qkv, first[:, :3 * D])
    grad_stream_norm, gain_one_grad, shift_one_grad = norm_one_back(grad_hidden_one)
    input_grad = grad_residual + grad_stream_norm
    qkv_grad = contract_rows(hidden_one, grad_qkv)
    qkv_bias_grad = column_sums(grad_qkv)

    small_grads = (
        gain_one_grad,
        shift_one_grad,
        qkv_bias_grad[:D],
        qkv_bias_grad[D:2 * D],
        qkv_bias_grad[2 * D:],
        proj_bias_grad,
        gain_two_grad,
        shift_two_grad,
        down_bias_grad,
        up_bias_grad,
    )
    packed_two = jnp.concatenate([qkv_grad, as_columns(small_grads, D)], axis=1)
    down_share, share_one, packed_two = lax.optimization_barrier((down_share, share_one, packed_two))
    down_share = down_share.astype(jnp.float32)
    up_share = share_one[:, :ff].astype(jnp.float32)
    proj_share = share_one[:, ff:].astype(jnp.float32)
    share_two = reduce_rows(packed_two)
    small_out = []
    offset = 3 * D
    for cols in small_cols:
        small_out.append(share_two[:, offset:offset + cols].reshape(-1))
        offset += cols
    (
        gain_one_share,
        shift_one_share,
        query_bias_share,
        key_bias_share,
        value_bias_share,
        proj_bias_share,
        gain_two_share,
        shift_two_share,
        down_bias_share,
        up_bias_share,
    ) = small_out
    return (
        output,
        input_grad,
        gain_one_share,
        shift_one_share,
        share_two[:, :D],
        query_bias_share,
        share_two[:, D:2 * D],
        key_bias_share,
        share_two[:, 2 * D:3 * D],
        value_bias_share,
        proj_share,
        proj_bias_share,
        gain_two_share,
        shift_two_share,
        up_share,
        up_bias_share,
        down_share,
        down_bias_share,
    )


def solution(mesh):
    in_specs = (
        P(("wide", "narrow"), None),
        P(("wide", "narrow"), None),
        P(("wide", "narrow"), None),
        P(),
        P("wide"),
        P("wide"),
        P("wide", None),
        P("wide"),
        P("wide", None),
        P("wide"),
        P("wide", None),
        P("wide"),
        P("wide", None),
        P("wide"),
        P("wide"),
        P("wide"),
        P("wide", None),
        P("wide"),
        P("wide", None),
        P("wide"),
    )
    out_specs = (
        P(("wide", "narrow"), None),
        P(("wide", "narrow"), None),
        P("wide"),
        P("wide"),
        P("wide", None),
        P("wide"),
        P("wide", None),
        P("wide"),
        P("wide", None),
        P("wide"),
        P("wide", None),
        P("wide"),
        P("wide"),
        P("wide"),
        P("wide", None),
        P("wide"),
        P("wide", None),
        P("wide"),
    )
    return jax.shard_map(
        on_device, mesh=mesh, in_specs=in_specs, out_specs=out_specs, check_vma=False
    )
```

```python
from functools import partial
import math

import jax
import jax.numpy as jnp
from jax import lax
from jax.sharding import PartitionSpec as P

D = 768
HEADS = 12
HD = 64
FEAT = 32
SEGS = 24
BLOCK = 128

EPSILON = 1e-05
HIGHEST = lax.Precision.HIGHEST


def pieces(lens_row, seq_len):
    seg_end = jnp.cumsum(lens_row)
    seg_start = seg_end - lens_row
    places = jnp.arange(seq_len, dtype=jnp.int32)
    segment = jnp.sum((places[:, None] >= seg_end[None, :]).astype(jnp.int32), axis=1)
    slots = jnp.arange(SEGS, dtype=jnp.int32)
    begins = jnp.sum(jnp.where(segment[:, None] == slots[None, :], seg_start[None, :], 0), axis=1)
    position = places - begins
    valid = (segment < SEGS - 1).astype(jnp.float32)
    return (position, valid, segment)


def rotate(heads_field, position):
    half = HD // 2
    rates = jnp.exp(jnp.arange(half, dtype=jnp.float32) * (-2.0 * math.log(10000.0) / HD))
    angles = position.astype(jnp.float32)[:, None] * rates[None, :]
    cosine = jnp.cos(angles)[:, None, :]
    sine = jnp.sin(angles)[:, None, :]
    first = heads_field[..., :half]
    second = heads_field[..., half:]
    return jnp.concatenate(
        [first * cosine - second * sine, second * cosine + first * sine], axis=-1
    )


def featurize(rotated, features):
    table = features.reshape(HD, HEADS, FEAT)
    scores = jnp.einsum("lhe,ehm->lhm", rotated, table, precision=HIGHEST) * 0.125
    return jax.nn.elu(scores) + 1.0


def normalize(stream, gain, shift):
    average = jnp.mean(stream, axis=-1, keepdims=True)
    centered = stream - average
    variance = jnp.mean(centered * centered, axis=-1, keepdims=True)
    return centered * lax.rsqrt(variance + EPSILON) * gain + shift


def contract_rows(left, right):
    return lax.dot_general(
        left, right, (((0,), (0,)), ((), ())), preferred_element_type=jnp.float32
    )


def times_transposed(left, right):
    return lax.dot_general(
        left, right, (((1,), (1,)), ((), ())), preferred_element_type=jnp.float32
    )


def column_sums(matrix):
    return jnp.sum(matrix.astype(jnp.float32), axis=0)


def gather_rows(shard):
    return lax.all_gather(shard, "wide", axis=0, tiled=True)


def narrow_sum(share):
    size = lax.psum(1, "narrow")
    steps = size.bit_length() - 1
    assert 1 << steps == size
    me = lax.axis_index("narrow")
    rows = share.shape[0]
    assert rows % size == 0
    acc = share.astype(jnp.float32)
    for k in range(steps):
        half = acc.shape[0] // 2
        upper = ((me >> k) & 1) == 1
        lo, hi = acc[:half], acc[half:]
        keep = jnp.where(upper, hi, lo)
        send = jnp.where(upper, lo, hi).astype(jnp.bfloat16)
        pairs = [(i, i ^ (1 << k)) for i in range(size)]
        acc = keep + lax.ppermute(send, "narrow", pairs).astype(jnp.float32)
    part = acc.astype(jnp.bfloat16)
    for k in reversed(range(steps)):
        upper = ((me >> k) & 1) == 1
        pairs = [(i, i ^ (1 << k)) for i in range(size)]
        other = lax.ppermute(part, "narrow", pairs)
        part = jnp.where(upper, jnp.concatenate([other, part]), jnp.concatenate([part, other]))
    return part.astype(jnp.float32)


def axis_sum(value, axis):
    size = lax.psum(1, axis)
    steps = size.bit_length() - 1
    assert 1 << steps == size
    for k in range(steps):
        pairs = [(i, i ^ (1 << k)) for i in range(size)]
        value = value + lax.ppermute(value, axis, pairs)
    return value


def reduce_rows(full):
    share = lax.psum_scatter(full.astype(jnp.bfloat16), "wide", scatter_dimension=0, tiled=True)
    return narrow_sum(share)


def gelu_parts(upper):
    cdf = 0.5 * (1.0 + lax.erf(upper * math.sqrt(0.5)))
    slope = cdf + upper * jnp.exp(-0.5 * upper * upper) * (1.0 / math.sqrt(2.0 * math.pi))
    return upper * cdf, slope


def to_blocks(field, nseq, width):
    seq_len = field.shape[0] // nseq
    nb = seq_len // BLOCK
    return jnp.transpose(field.reshape(nseq, nb, BLOCK, HEADS, width), (0, 3, 1, 2, 4))


def from_blocks(blocks):
    nseq, heads, nb, block, width = blocks.shape
    return jnp.transpose(blocks, (0, 2, 3, 1, 4)).reshape(nseq * nb * block, heads * width)


def window(blocks, fill=0):
    pad = [(0, 0)] * blocks.ndim
    pad[-3] = (1, 0)
    prev = jnp.pad(blocks, pad, constant_values=fill)[..., :-1, :, :]
    return jnp.concatenate([prev, blocks], axis=-2)


def unwindow(win):
    own = win[..., BLOCK:, :]
    nxt = win[..., 1:, :BLOCK, :]
    pad = [(0, 0)] * win.ndim
    pad[-3] = (0, 1)
    return own + jnp.pad(nxt, pad)


def as_columns(vectors, rows):
    return jnp.concatenate([v.reshape(rows, -1) for v in vectors], axis=1)


def on_device(
    tokens,
    cotangent,
    lengths,
    features,
    ln1_gain,
    ln1_bias,
    q_weight,
    q_bias,
    k_weight,
    k_bias,
    v_weight,
    v_bias,
    out_weight,
    out_bias,
    ln2_gain,
    ln2_bias,
    up_weight,
    up_bias,
    down_weight,
    down_bias,
):
    nseq = lengths.shape[0]
    total = tokens.shape[0]
    seq_len = total // nseq
    nb = seq_len // BLOCK
    shard_rows = ln1_gain.shape[0]
    wide = D // shard_rows

    small_shards = (ln1_gain, ln1_bias, q_bias, k_bias, v_bias, out_bias, ln2_gain, ln2_bias, down_bias, up_bias)
    small_cols = [piece.shape[0] // shard_rows for piece in small_shards]
    first = gather_rows(
        jnp.concatenate([q_weight, k_weight, v_weight, as_columns(small_shards, shard_rows)], axis=1)
    )
    query_mat = first[:, :D]
    key_mat = first[:, D:2 * D]
    value_mat = first[:, 2 * D:3 * D]
    smalls = []
    offset = 3 * D
    for cols in small_cols:
        smalls.append(first[:, offset:offset + cols].astype(jnp.float32).reshape(-1))
        offset += cols
    g1, b1, bq, bk, bv, bo, g2, b2, bd, bu = smalls
    ff = up_weight.shape[1]
    second = gather_rows(jnp.concatenate([out_weight, up_weight], axis=1))
    proj_mat = second[:, :D]
    up_mat = second[:, D:]
    down_mat = gather_rows(down_weight)

    position, valid, segment = jax.vmap(partial(pieces, seq_len=seq_len))(lengths)
    position = position.reshape(total)
    seg_blocks = segment.reshape(nseq, nb, BLOCK)
    seg_win = window(seg_blocks[..., None], fill=-1)[..., 0]
    rel_q = jnp.arange(BLOCK, dtype=jnp.int32)[:, None]
    rel_k = jnp.arange(2 * BLOCK, dtype=jnp.int32)[None, :]
    allowed = (rel_k <= rel_q + BLOCK)[None, None] & (
        seg_win[:, :, None, :] == seg_blocks[:, :, :, None]
    )
    allowed = allowed[:, None]
    valid_blk = valid.reshape(nseq, 1, nb, BLOCK, 1)

    stream = tokens.astype(jnp.float32)
    normed_one, norm_one_back = jax.vjp(normalize, stream, g1, b1)
    hidden_one = normed_one.astype(jnp.bfloat16)
    query_pre = jnp.dot(hidden_one, query_mat, preferred_element_type=jnp.float32) + bq
    key_pre = jnp.dot(hidden_one, key_mat, preferred_element_type=jnp.float32) + bk
    values = (jnp.dot(hidden_one, value_mat, preferred_element_type=jnp.float32) + bv).astype(jnp.bfloat16)

    def features_of(projected):
        return featurize(rotate(projected.reshape(total, HEADS, HD), position), features)

    query_feat, query_back = jax.vjp(features_of, query_pre)
    key_feat, key_back = jax.vjp(features_of, key_pre)
    pq = to_blocks(query_feat.astype(jnp.bfloat16).reshape(total, HEADS * FEAT), nseq, FEAT)
    pk = window(to_blocks(key_feat.astype(jnp.bfloat16).reshape(total, HEADS * FEAT), nseq, FEAT))
    vb = window(to_blocks(values, nseq, HD))

    scores = jnp.einsum("shnqf,shnkf->shnqk", pq, pk, preferred_element_type=jnp.float32)
    scores = jnp.where(allowed, scores, 0.0)
    denominator = jnp.sum(scores, axis=-1, keepdims=True)
    scores_low = scores.astype(jnp.bfloat16)
    numerator = jnp.einsum("shnqk,shnkd->shnqd", scores_low, vb, preferred_element_type=jnp.float32)
    mixed = numerator / denominator * valid_blk
    attended = from_blocks(mixed).astype(jnp.bfloat16)
    residual = stream + (jnp.dot(attended, proj_mat, preferred_element_type=jnp.float32) + bo)
    normed_two, norm_two_back = jax.vjp(normalize, residual, g2, b2)
    hidden_two = normed_two.astype(jnp.bfloat16)
    upper = jnp.dot(hidden_two, up_mat, preferred_element_type=jnp.float32) + bu
    activated, slope = gelu_parts(upper)
    act_low = activated.astype(jnp.bfloat16)
    result = residual + (jnp.dot(act_low, down_mat, preferred_element_type=jnp.float32) + bd)
    output = result.astype(jnp.bfloat16)

    upward = cotangent
    grad_out = upward.astype(jnp.float32)
    down_grad = contract_rows(act_low, upward).astype(jnp.bfloat16)
    down_grad, upward = lax.optimization_barrier((down_grad, upward))
    scattered_down = lax.psum_scatter(down_grad, "wide", scatter_dimension=0, tiled=True)
    grad_act = times_transposed(upward, down_mat)
    grad_upper = (grad_act * slope).astype(jnp.bfloat16)
    grad_hidden_two = times_transposed(grad_upper, up_mat)
    grad_residual_norm, gain_two_grad, shift_two_grad = norm_two_back(grad_hidden_two)
    grad_residual = grad_out + grad_residual_norm
    grad_proj_in = grad_residual.astype(jnp.bfloat16)
    grad_attended = times_transposed(grad_proj_in, proj_mat)
    up_grad = contract_rows(hidden_two, grad_upper).astype(jnp.bfloat16)
    proj_grad = contract_rows(attended, grad_proj_in).astype(jnp.bfloat16)
    packed_one = jnp.concatenate([up_grad, proj_grad], axis=1)
    packed_one, grad_attended = lax.optimization_barrier((packed_one, grad_attended))
    scattered_one = lax.psum_scatter(packed_one, "wide", scatter_dimension=0, tiled=True)
    down_bias_grad = column_sums(upward)
    up_bias_grad = column_sums(grad_upper)
    proj_bias_grad = column_sums(grad_proj_in)

    head_grad = to_blocks(grad_attended, nseq, HD)
    scaled = head_grad * valid_blk
    grad_num = (scaled / denominator).astype(jnp.bfloat16)
    grad_den = -jnp.sum(scaled * numerator, axis=-1, keepdims=True) / (denominator * denominator)
    grad_scores = jnp.einsum("shnqd,shnkd->shnqk", grad_num, vb, preferred_element_type=jnp.float32)
    grad_scores = (grad_scores + grad_den).astype(jnp.bfloat16)
    grad_scores = jnp.where(allowed, grad_scores, jnp.zeros((), jnp.bfloat16))
    grad_vwin = jnp.einsum("shnqk,shnqd->shnkd", scores_low, grad_num, preferred_element_type=jnp.float32)
    grad_value = from_blocks(unwindow(grad_vwin)).astype(jnp.bfloat16)
    grad_qf = jnp.einsum("shnqk,shnkf->shnqf", grad_scores, pk, preferred_element_type=jnp.float32)
    grad_kwin = jnp.einsum("shnqk,shnqf->shnkf", grad_scores, pq, preferred_element_type=jnp.float32)
    scattered_down, scattered_one, grad_qf, grad_kwin = lax.optimization_barrier(
        (scattered_down, scattered_one, grad_qf, grad_kwin)
    )
    grad_qf = from_blocks(grad_qf).reshape(total, HEADS, FEAT)
    grad_kf = from_blocks(unwindow(grad_kwin)).reshape(total, HEADS, FEAT)
    grad_key = key_back(grad_kf)[0].astype(jnp.bfloat16)
    grad_query = query_back(grad_qf)[0].astype(jnp.bfloat16)
    grad_qkv = jnp.concatenate([grad_query, grad_key, grad_value], axis=1)
    down_share = lax.psum(scattered_down, "narrow")
    share_one = lax.psum(scattered_one, "narrow")
    qkv_grad = contract_rows(hidden_one, grad_qkv)
    qkv_bias_grad = column_sums(grad_qkv)

    small_grads = (
        qkv_bias_grad[:D],
        qkv_bias_grad[D:2 * D],
        qkv_bias_grad[2 * D:],
        proj_bias_grad,
        gain_two_grad,
        shift_two_grad,
        down_bias_grad,
        up_bias_grad,
    )
    packed_two = jnp.concatenate([qkv_grad, as_columns(small_grads, D)], axis=1)
    down_share, share_one, packed_two = lax.optimization_barrier((down_share, share_one, packed_two))
    down_share = down_share.astype(jnp.float32)
    up_share = share_one[:, :ff].astype(jnp.float32)
    proj_share = share_one[:, ff:].astype(jnp.float32)
    share_two = reduce_rows(packed_two)
    small_out = []
    offset = 3 * D
    for cols in small_cols[2:]:
        small_out.append(share_two[:, offset:offset + cols].reshape(-1))
        offset += cols
    (
        query_bias_share,
        key_bias_share,
        value_bias_share,
        proj_bias_share,
        gain_two_share,
        shift_two_share,
        down_bias_share,
        up_bias_share,
    ) = small_out

    grad_hidden_one = times_transposed(grad_qkv, first[:, :3 * D])
    grad_stream_norm, gain_one_grad, shift_one_grad = norm_one_back(grad_hidden_one)
    input_grad = grad_residual + grad_stream_norm
    me = lax.axis_index("wide")
    ln1_pair = jnp.stack([gain_one_grad, shift_one_grad])
    ln1_pair = axis_sum(axis_sum(ln1_pair, "wide"), "narrow").reshape(2, wide, shard_rows)
    ln1_pair = lax.dynamic_index_in_dim(ln1_pair, me, axis=1, keepdims=False)
    gain_one_share = ln1_pair[0]
    shift_one_share = ln1_pair[1]
    return (
        output,
        input_grad,
        gain_one_share,
        shift_one_share,
        share_two[:, :D],
        query_bias_share,
        share_two[:, D:2 * D],
        key_bias_share,
        share_two[:, 2 * D:3 * D],
        value_bias_share,
        proj_share,
        proj_bias_share,
        gain_two_share,
        shift_two_share,
        up_share,
        up_bias_share,
        down_share,
        down_bias_share,
    )


def solution(mesh):
    in_specs = (
        P(("wide", "narrow"), None),
        P(("wide", "narrow"), None),
        P(("wide", "narrow"), None),
        P(),
        P("wide"),
        P("wide"),
        P("wide", None),
        P("wide"),
        P("wide", None),
        P("wide"),
        P("wide", None),
        P("wide"),
        P("wide", None),
        P("wide"),
        P("wide"),
        P("wide"),
        P("wide", None),
        P("wide"),
        P("wide", None),
        P("wide"),
    )
    out_specs = (
        P(("wide", "narrow"), None),
        P(("wide", "narrow"), None),
        P("wide"),
        P("wide"),
        P("wide", None),
        P("wide"),
        P("wide", None),
        P("wide"),
        P("wide", None),
        P("wide"),
        P("wide", None),
        P("wide"),
        P("wide"),
        P("wide"),
        P("wide", None),
        P("wide"),
        P("wide", None),
        P("wide"),
    )
    return jax.shard_map(
        on_device, mesh=mesh, in_specs=in_specs, out_specs=out_specs, check_vma=False
    )
```

```python
from functools import partial
import math

import jax
import jax.numpy as jnp
from jax import lax
from jax.sharding import PartitionSpec as P

D = 768
HEADS = 12
HD = 64
FEAT = 32
SEGS = 24
BLOCK = 128

EPSILON = 1e-05
HIGHEST = lax.Precision.HIGHEST


def pieces(lens_row, seq_len):
    seg_end = jnp.cumsum(lens_row)
    seg_start = seg_end - lens_row
    places = jnp.arange(seq_len, dtype=jnp.int32)
    segment = jnp.sum((places[:, None] >= seg_end[None, :]).astype(jnp.int32), axis=1)
    slots = jnp.arange(SEGS, dtype=jnp.int32)
    begins = jnp.sum(jnp.where(segment[:, None] == slots[None, :], seg_start[None, :], 0), axis=1)
    position = places - begins
    valid = (segment < SEGS - 1).astype(jnp.float32)
    return (position, valid, segment)


def rotate(heads_field, position):
    half = HD // 2
    rates = jnp.exp(jnp.arange(half, dtype=jnp.float32) * (-2.0 * math.log(10000.0) / HD))
    angles = position.astype(jnp.float32)[:, None] * rates[None, :]
    cosine = jnp.cos(angles)[:, None, :]
    sine = jnp.sin(angles)[:, None, :]
    first = heads_field[..., :half]
    second = heads_field[..., half:]
    return jnp.concatenate(
        [first * cosine - second * sine, second * cosine + first * sine], axis=-1
    )


def featurize(rotated, features):
    table = features.reshape(HD, HEADS, FEAT)
    scores = jnp.einsum("lhe,ehm->lhm", rotated, table, precision=HIGHEST) * 0.125
    return jax.nn.elu(scores) + 1.0


def normalize(stream, gain, shift):
    average = jnp.mean(stream, axis=-1, keepdims=True)
    centered = stream - average
    variance = jnp.mean(centered * centered, axis=-1, keepdims=True)
    return centered * lax.rsqrt(variance + EPSILON) * gain + shift


def contract_rows(left, right):
    return lax.dot_general(
        left, right, (((0,), (0,)), ((), ())), preferred_element_type=jnp.float32
    )


def times_transposed(left, right):
    return lax.dot_general(
        left, right, (((1,), (1,)), ((), ())), preferred_element_type=jnp.float32
    )


def column_sums(matrix):
    return jnp.sum(matrix.astype(jnp.float32), axis=0)


def gather_rows(shard):
    return lax.all_gather(shard, "wide", axis=0, tiled=True)


def narrow_sum(share):
    size = lax.psum(1, "narrow")
    steps = size.bit_length() - 1
    assert 1 << steps == size
    me = lax.axis_index("narrow")
    rows = share.shape[0]
    assert rows % size == 0
    acc = share.astype(jnp.float32)
    for k in range(steps):
        half = acc.shape[0] // 2
        upper = ((me >> k) & 1) == 1
        lo, hi = acc[:half], acc[half:]
        keep = jnp.where(upper, hi, lo)
        send = jnp.where(upper, lo, hi).astype(jnp.bfloat16)
        pairs = [(i, i ^ (1 << k)) for i in range(size)]
        acc = keep + lax.ppermute(send, "narrow", pairs).astype(jnp.float32)
    part = acc.astype(jnp.bfloat16)
    for k in reversed(range(steps)):
        upper = ((me >> k) & 1) == 1
        pairs = [(i, i ^ (1 << k)) for i in range(size)]
        other = lax.ppermute(part, "narrow", pairs)
        part = jnp.where(upper, jnp.concatenate([other, part]), jnp.concatenate([part, other]))
    return part.astype(jnp.float32)


def axis_sum(value, axis):
    size = lax.psum(1, axis)
    steps = size.bit_length() - 1
    assert 1 << steps == size
    for k in range(steps):
        pairs = [(i, i ^ (1 << k)) for i in range(size)]
        value = value + lax.ppermute(value, axis, pairs)
    return value


def reduce_rows(full):
    share = lax.psum_scatter(full.astype(jnp.bfloat16), "wide", scatter_dimension=0, tiled=True)
    return narrow_sum(share)


def gelu_parts(upper):
    cdf = 0.5 * (1.0 + lax.erf(upper * math.sqrt(0.5)))
    slope = cdf + upper * jnp.exp(-0.5 * upper * upper) * (1.0 / math.sqrt(2.0 * math.pi))
    return upper * cdf, slope


def to_blocks(field, nseq, width):
    seq_len = field.shape[0] // nseq
    nb = seq_len // BLOCK
    return jnp.transpose(field.reshape(nseq, nb, BLOCK, HEADS, width), (0, 3, 1, 2, 4))


def from_blocks(blocks):
    nseq, heads, nb, block, width = blocks.shape
    return jnp.transpose(blocks, (0, 2, 3, 1, 4)).reshape(nseq * nb * block, heads * width)


def window(blocks, fill=0):
    pad = [(0, 0)] * blocks.ndim
    pad[-3] = (1, 0)
    prev = jnp.pad(blocks, pad, constant_values=fill)[..., :-1, :, :]
    return jnp.concatenate([prev, blocks], axis=-2)


def unwindow(win):
    own = win[..., BLOCK:, :]
    nxt = win[..., 1:, :BLOCK, :]
    pad = [(0, 0)] * win.ndim
    pad[-3] = (0, 1)
    return own + jnp.pad(nxt, pad)


def as_columns(vectors, rows):
    return jnp.concatenate([v.reshape(rows, -1) for v in vectors], axis=1)


def on_device(
    tokens,
    cotangent,
    lengths,
    features,
    ln1_gain,
    ln1_bias,
    q_weight,
    q_bias,
    k_weight,
    k_bias,
    v_weight,
    v_bias,
    out_weight,
    out_bias,
    ln2_gain,
    ln2_bias,
    up_weight,
    up_bias,
    down_weight,
    down_bias,
):
    nseq = lengths.shape[0]
    total = tokens.shape[0]
    seq_len = total // nseq
    nb = seq_len // BLOCK
    shard_rows = ln1_gain.shape[0]
    wide = D // shard_rows

    small_shards = (ln1_gain, ln1_bias, q_bias, k_bias, v_bias, out_bias, ln2_gain, ln2_bias, down_bias, up_bias)
    small_cols = [piece.shape[0] // shard_rows for piece in small_shards]
    first_q = gather_rows(jnp.concatenate([q_weight, as_columns(small_shards, shard_rows)], axis=1))
    first_kv = gather_rows(jnp.concatenate([k_weight, v_weight], axis=1))
    first = jnp.concatenate([first_q[:, :D], first_kv, first_q[:, D:]], axis=1)
    query_mat = first[:, :D]
    key_mat = first[:, D:2 * D]
    value_mat = first[:, 2 * D:3 * D]
    smalls = []
    offset = 3 * D
    for cols in small_cols:
        smalls.append(first[:, offset:offset + cols].astype(jnp.float32).reshape(-1))
        offset += cols
    g1, b1, bq, bk, bv, bo, g2, b2, bd, bu = smalls
    ff = up_weight.shape[1]
    second = gather_rows(jnp.concatenate([out_weight, up_weight], axis=1))
    proj_mat = second[:, :D]
    up_mat = second[:, D:]
    down_mat = gather_rows(down_weight)

    position, valid, segment = jax.vmap(partial(pieces, seq_len=seq_len))(lengths)
    position = position.reshape(total)
    seg_blocks = segment.reshape(nseq, nb, BLOCK)
    seg_win = window(seg_blocks[..., None], fill=-1)[..., 0]
    rel_q = jnp.arange(BLOCK, dtype=jnp.int32)[:, None]
    rel_k = jnp.arange(2 * BLOCK, dtype=jnp.int32)[None, :]
    allowed = (rel_k <= rel_q + BLOCK)[None, None] & (
        seg_win[:, :, None, :] == seg_blocks[:, :, :, None]
    )
    allowed = allowed[:, None]
    valid_blk = valid.reshape(nseq, 1, nb, BLOCK, 1)

    stream = tokens.astype(jnp.float32)
    normed_one, norm_one_back = jax.vjp(normalize, stream, g1, b1)
    hidden_one = normed_one.astype(jnp.bfloat16)
    query_pre = jnp.dot(hidden_one, query_mat, preferred_element_type=jnp.float32) + bq
    key_pre = jnp.dot(hidden_one, key_mat, preferred_element_type=jnp.float32) + bk
    values = (jnp.dot(hidden_one, value_mat, preferred_element_type=jnp.float32) + bv).astype(jnp.bfloat16)

    def features_of(projected):
        return featurize(rotate(projected.reshape(total, HEADS, HD), position), features)

    query_feat, query_back = jax.vjp(features_of, query_pre)
    key_feat, key_back = jax.vjp(features_of, key_pre)
    pq = to_blocks(query_feat.astype(jnp.bfloat16).reshape(total, HEADS * FEAT), nseq, FEAT)
    pk = window(to_blocks(key_feat.astype(jnp.bfloat16).reshape(total, HEADS * FEAT), nseq, FEAT))
    vb = window(to_blocks(values, nseq, HD))

    scores = jnp.einsum("shnqf,shnkf->shnqk", pq, pk, preferred_element_type=jnp.float32)
    scores = jnp.where(allowed, scores, 0.0)
    denominator = jnp.sum(scores, axis=-1, keepdims=True)
    scores_low = scores.astype(jnp.bfloat16)
    numerator = jnp.einsum("shnqk,shnkd->shnqd", scores_low, vb, preferred_element_type=jnp.float32)
    mixed = numerator / denominator * valid_blk
    attended = from_blocks(mixed).astype(jnp.bfloat16)
    residual = stream + (jnp.dot(attended, proj_mat, preferred_element_type=jnp.float32) + bo)
    normed_two, norm_two_back = jax.vjp(normalize, residual, g2, b2)
    hidden_two = normed_two.astype(jnp.bfloat16)
    upper = jnp.dot(hidden_two, up_mat, preferred_element_type=jnp.float32) + bu
    activated, slope = gelu_parts(upper)
    act_low = activated.astype(jnp.bfloat16)
    result = residual + (jnp.dot(act_low, down_mat, preferred_element_type=jnp.float32) + bd)
    output = result.astype(jnp.bfloat16)

    upward = cotangent
    grad_out = upward.astype(jnp.float32)
    down_grad = contract_rows(act_low, upward).astype(jnp.bfloat16)
    down_grad, upward = lax.optimization_barrier((down_grad, upward))
    scattered_down = lax.psum_scatter(down_grad, "wide", scatter_dimension=0, tiled=True)
    grad_act = times_transposed(upward, down_mat)
    grad_upper = (grad_act * slope).astype(jnp.bfloat16)
    grad_hidden_two = times_transposed(grad_upper, up_mat)
    grad_residual_norm, gain_two_grad, shift_two_grad = norm_two_back(grad_hidden_two)
    grad_residual = grad_out + grad_residual_norm
    grad_proj_in = grad_residual.astype(jnp.bfloat16)
    grad_attended = times_transposed(grad_proj_in, proj_mat)
    up_grad = contract_rows(hidden_two, grad_upper).astype(jnp.bfloat16)
    proj_grad = contract_rows(attended, grad_proj_in).astype(jnp.bfloat16)
    packed_one = jnp.concatenate([up_grad, proj_grad], axis=1)
    packed_one, grad_attended = lax.optimization_barrier((packed_one, grad_attended))
    scattered_one = lax.psum_scatter(packed_one, "wide", scatter_dimension=0, tiled=True)
    down_bias_grad = column_sums(upward)
    up_bias_grad = column_sums(grad_upper)
    proj_bias_grad = column_sums(grad_proj_in)

    head_grad = to_blocks(grad_attended, nseq, HD)
    scaled = head_grad * valid_blk
    grad_num = (scaled / denominator).astype(jnp.bfloat16)
    grad_den = -jnp.sum(scaled * numerator, axis=-1, keepdims=True) / (denominator * denominator)
    grad_scores = jnp.einsum("shnqd,shnkd->shnqk", grad_num, vb, preferred_element_type=jnp.float32)
    grad_scores = (grad_scores + grad_den).astype(jnp.bfloat16)
    grad_scores = jnp.where(allowed, grad_scores, jnp.zeros((), jnp.bfloat16))
    grad_vwin = jnp.einsum("shnqk,shnqd->shnkd", scores_low, grad_num, preferred_element_type=jnp.float32)
    grad_value = from_blocks(unwindow(grad_vwin)).astype(jnp.bfloat16)
    grad_qf = jnp.einsum("shnqk,shnkf->shnqf", grad_scores, pk, preferred_element_type=jnp.float32)
    grad_kwin = jnp.einsum("shnqk,shnqf->shnkf", grad_scores, pq, preferred_element_type=jnp.float32)
    scattered_down, scattered_one, grad_qf, grad_kwin = lax.optimization_barrier(
        (scattered_down, scattered_one, grad_qf, grad_kwin)
    )
    grad_qf = from_blocks(grad_qf).reshape(total, HEADS, FEAT)
    grad_kf = from_blocks(unwindow(grad_kwin)).reshape(total, HEADS, FEAT)
    grad_key = key_back(grad_kf)[0].astype(jnp.bfloat16)
    grad_query = query_back(grad_qf)[0].astype(jnp.bfloat16)
    grad_qkv = jnp.concatenate([grad_query, grad_key, grad_value], axis=1)
    down_share = lax.psum(scattered_down, "narrow")
    share_one = lax.psum(scattered_one, "narrow")
    qkv_grad = contract_rows(hidden_one, grad_qkv)
    qkv_bias_grad = column_sums(grad_qkv)

    small_grads = (
        qkv_bias_grad[:D],
        qkv_bias_grad[D:2 * D],
        qkv_bias_grad[2 * D:],
        proj_bias_grad,
        gain_two_grad,
        shift_two_grad,
        down_bias_grad,
        up_bias_grad,
    )
    packed_two = jnp.concatenate([qkv_grad, as_columns(small_grads, D)], axis=1)
    down_share, share_one, packed_two = lax.optimization_barrier((down_share, share_one, packed_two))
    down_share = down_share.astype(jnp.float32)
    up_share = share_one[:, :ff].astype(jnp.float32)
    proj_share = share_one[:, ff:].astype(jnp.float32)
    share_two = reduce_rows(packed_two)
    small_out = []
    offset = 3 * D
    for cols in small_cols[2:]:
        small_out.append(share_two[:, offset:offset + cols].reshape(-1))
        offset += cols
    (
        query_bias_share,
        key_bias_share,
        value_bias_share,
        proj_bias_share,
        gain_two_share,
        shift_two_share,
        down_bias_share,
        up_bias_share,
    ) = small_out

    grad_hidden_one = times_transposed(grad_qkv, first[:, :3 * D])
    grad_stream_norm, gain_one_grad, shift_one_grad = norm_one_back(grad_hidden_one)
    input_grad = grad_residual + grad_stream_norm
    me = lax.axis_index("wide")
    ln1_pair = jnp.stack([gain_one_grad, shift_one_grad])
    ln1_pair = axis_sum(axis_sum(ln1_pair, "wide"), "narrow").reshape(2, wide, shard_rows)
    ln1_pair = lax.dynamic_index_in_dim(ln1_pair, me, axis=1, keepdims=False)
    gain_one_share = ln1_pair[0]
    shift_one_share = ln1_pair[1]
    return (
        output,
        input_grad,
        gain_one_share,
        shift_one_share,
        share_two[:, :D],
        query_bias_share,
        share_two[:, D:2 * D],
        key_bias_share,
        share_two[:, 2 * D:3 * D],
        value_bias_share,
        proj_share,
        proj_bias_share,
        gain_two_share,
        shift_two_share,
        up_share,
        up_bias_share,
        down_share,
        down_bias_share,
    )


def solution(mesh):
    in_specs = (
        P(("wide", "narrow"), None),
        P(("wide", "narrow"), None),
        P(("wide", "narrow"), None),
        P(),
        P("wide"),
        P("wide"),
        P("wide", None),
        P("wide"),
        P("wide", None),
        P("wide"),
        P("wide", None),
        P("wide"),
        P("wide", None),
        P("wide"),
        P("wide"),
        P("wide"),
        P("wide", None),
        P("wide"),
        P("wide", None),
        P("wide"),
    )
    out_specs = (
        P(("wide", "narrow"), None),
        P(("wide", "narrow"), None),
        P("wide"),
        P("wide"),
        P("wide", None),
        P("wide"),
        P("wide", None),
        P("wide"),
        P("wide", None),
        P("wide"),
        P("wide", None),
        P("wide"),
        P("wide"),
        P("wide"),
        P("wide", None),
        P("wide"),
        P("wide", None),
        P("wide"),
    )
    return jax.shard_map(
        on_device, mesh=mesh, in_specs=in_specs, out_specs=out_specs, check_vma=False
    )
```

```python
from functools import partial
import math

import jax
import jax.numpy as jnp
from jax import lax
from jax.sharding import PartitionSpec as P

D = 768
HEADS = 12
HD = 64
FEAT = 32
SEGS = 24
BLOCK = 128

EPSILON = 1e-05
HIGHEST = lax.Precision.HIGHEST


def pieces(lens_row, seq_len):
    seg_end = jnp.cumsum(lens_row)
    seg_start = seg_end - lens_row
    places = jnp.arange(seq_len, dtype=jnp.int32)
    segment = jnp.sum((places[:, None] >= seg_end[None, :]).astype(jnp.int32), axis=1)
    slots = jnp.arange(SEGS, dtype=jnp.int32)
    begins = jnp.sum(jnp.where(segment[:, None] == slots[None, :], seg_start[None, :], 0), axis=1)
    position = places - begins
    valid = (segment < SEGS - 1).astype(jnp.float32)
    return (position, valid, segment)


def rotate(heads_field, position):
    half = HD // 2
    rates = jnp.exp(jnp.arange(half, dtype=jnp.float32) * (-2.0 * math.log(10000.0) / HD))
    angles = position.astype(jnp.float32)[:, None] * rates[None, :]
    cosine = jnp.cos(angles)[:, None, :]
    sine = jnp.sin(angles)[:, None, :]
    first = heads_field[..., :half]
    second = heads_field[..., half:]
    return jnp.concatenate(
        [first * cosine - second * sine, second * cosine + first * sine], axis=-1
    )


def featurize(rotated, features):
    table = features.reshape(HD, HEADS, FEAT)
    scores = jnp.einsum("lhe,ehm->lhm", rotated, table, precision=HIGHEST) * 0.125
    return jax.nn.elu(scores) + 1.0


def normalize(stream, gain, shift):
    average = jnp.mean(stream, axis=-1, keepdims=True)
    centered = stream - average
    variance = jnp.mean(centered * centered, axis=-1, keepdims=True)
    return centered * lax.rsqrt(variance + EPSILON) * gain + shift


def contract_rows(left, right):
    return lax.dot_general(
        left, right, (((0,), (0,)), ((), ())), preferred_element_type=jnp.float32
    )


def times_transposed(left, right):
    return lax.dot_general(
        left, right, (((1,), (1,)), ((), ())), preferred_element_type=jnp.float32
    )


def column_sums(matrix):
    return jnp.sum(matrix.astype(jnp.float32), axis=0)


def gather_rows(shard):
    return lax.all_gather(shard, "wide", axis=0, tiled=True)


def narrow_sum(share):
    size = lax.psum(1, "narrow")
    steps = size.bit_length() - 1
    assert 1 << steps == size
    me = lax.axis_index("narrow")
    rows = share.shape[0]
    assert rows % size == 0
    acc = share.astype(jnp.float32)
    for k in range(steps):
        half = acc.shape[0] // 2
        upper = ((me >> k) & 1) == 1
        lo, hi = acc[:half], acc[half:]
        keep = jnp.where(upper, hi, lo)
        send = jnp.where(upper, lo, hi).astype(jnp.bfloat16)
        pairs = [(i, i ^ (1 << k)) for i in range(size)]
        acc = keep + lax.ppermute(send, "narrow", pairs).astype(jnp.float32)
    part = acc.astype(jnp.bfloat16)
    for k in reversed(range(steps)):
        upper = ((me >> k) & 1) == 1
        pairs = [(i, i ^ (1 << k)) for i in range(size)]
        other = lax.ppermute(part, "narrow", pairs)
        part = jnp.where(upper, jnp.concatenate([other, part]), jnp.concatenate([part, other]))
    return part.astype(jnp.float32)


def axis_sum(value, axis):
    size = lax.psum(1, axis)
    steps = size.bit_length() - 1
    assert 1 << steps == size
    for k in range(steps):
        pairs = [(i, i ^ (1 << k)) for i in range(size)]
        value = value + lax.ppermute(value, axis, pairs)
    return value


def reduce_rows(full):
    share = lax.psum_scatter(full.astype(jnp.bfloat16), "wide", scatter_dimension=0, tiled=True)
    return narrow_sum(share)


def gelu_parts(upper):
    cdf = 0.5 * (1.0 + lax.erf(upper * math.sqrt(0.5)))
    slope = cdf + upper * jnp.exp(-0.5 * upper * upper) * (1.0 / math.sqrt(2.0 * math.pi))
    return upper * cdf, slope


def to_blocks(field, nseq, width):
    seq_len = field.shape[0] // nseq
    nb = seq_len // BLOCK
    return jnp.transpose(field.reshape(nseq, nb, BLOCK, HEADS, width), (0, 3, 1, 2, 4))


def from_blocks(blocks):
    nseq, heads, nb, block, width = blocks.shape
    return jnp.transpose(blocks, (0, 2, 3, 1, 4)).reshape(nseq * nb * block, heads * width)


def window(blocks, fill=0):
    pad = [(0, 0)] * blocks.ndim
    pad[-3] = (1, 0)
    prev = jnp.pad(blocks, pad, constant_values=fill)[..., :-1, :, :]
    return jnp.concatenate([prev, blocks], axis=-2)


def unwindow(win):
    own = win[..., BLOCK:, :]
    nxt = win[..., 1:, :BLOCK, :]
    pad = [(0, 0)] * win.ndim
    pad[-3] = (0, 1)
    return own + jnp.pad(nxt, pad)


def as_columns(vectors, rows):
    return jnp.concatenate([v.reshape(rows, -1) for v in vectors], axis=1)


def on_device(
    tokens,
    cotangent,
    lengths,
    features,
    ln1_gain,
    ln1_bias,
    q_weight,
    q_bias,
    k_weight,
    k_bias,
    v_weight,
    v_bias,
    out_weight,
    out_bias,
    ln2_gain,
    ln2_bias,
    up_weight,
    up_bias,
    down_weight,
    down_bias,
):
    nseq = lengths.shape[0]
    total = tokens.shape[0]
    seq_len = total // nseq
    nb = seq_len // BLOCK
    shard_rows = ln1_gain.shape[0]
    wide = D // shard_rows

    small_shards = (ln1_gain, ln1_bias, q_bias, k_bias, v_bias, out_bias, ln2_gain, ln2_bias, down_bias, up_bias)
    small_cols = [piece.shape[0] // shard_rows for piece in small_shards]
    first = gather_rows(
        jnp.concatenate([q_weight, k_weight, v_weight, as_columns(small_shards, shard_rows)], axis=1)
    )
    query_mat = first[:, :D]
    key_mat = first[:, D:2 * D]
    value_mat = first[:, 2 * D:3 * D]
    smalls = []
    offset = 3 * D
    for cols in small_cols:
        smalls.append(first[:, offset:offset + cols].astype(jnp.float32).reshape(-1))
        offset += cols
    g1, b1, bq, bk, bv, bo, g2, b2, bd, bu = smalls
    ff = up_weight.shape[1]
    second = gather_rows(jnp.concatenate([out_weight, up_weight], axis=1))
    proj_mat = second[:, :D]
    up_mat = second[:, D:]
    down_mat = gather_rows(down_weight)

    position, valid, segment = jax.vmap(partial(pieces, seq_len=seq_len))(lengths)
    position = position.reshape(total)
    seg_blocks = segment.reshape(nseq, nb, BLOCK)
    seg_win = window(seg_blocks[..., None], fill=-1)[..., 0]
    rel_q = jnp.arange(BLOCK, dtype=jnp.int32)[:, None]
    rel_k = jnp.arange(2 * BLOCK, dtype=jnp.int32)[None, :]
    allowed = (rel_k <= rel_q + BLOCK)[None, None] & (
        seg_win[:, :, None, :] == seg_blocks[:, :, :, None]
    )
    allowed = allowed[:, None]
    valid_blk = valid.reshape(nseq, 1, nb, BLOCK, 1)

    stream = tokens.astype(jnp.float32)
    normed_one, norm_one_back = jax.vjp(normalize, stream, g1, b1)
    hidden_one = normed_one.astype(jnp.bfloat16)
    query_pre = jnp.dot(hidden_one, query_mat, preferred_element_type=jnp.float32) + bq
    key_pre = jnp.dot(hidden_one, key_mat, preferred_element_type=jnp.float32) + bk
    values = (jnp.dot(hidden_one, value_mat, preferred_element_type=jnp.float32) + bv).astype(jnp.bfloat16)

    def features_of(projected):
        return featurize(rotate(projected.reshape(total, HEADS, HD), position), features)

    query_feat, query_back = jax.vjp(features_of, query_pre)
    key_feat, key_back = jax.vjp(features_of, key_pre)
    pq = to_blocks(query_feat.astype(jnp.bfloat16).reshape(total, HEADS * FEAT), nseq, FEAT)
    pk = window(to_blocks(key_feat.astype(jnp.bfloat16).reshape(total, HEADS * FEAT), nseq, FEAT))
    vb = window(to_blocks(values, nseq, HD))

    scores = jnp.einsum("shnqf,shnkf->shnqk", pq, pk, preferred_element_type=jnp.float32)
    scores = jnp.where(allowed, scores, 0.0)
    denominator = jnp.sum(scores, axis=-1, keepdims=True)
    scores_low = scores.astype(jnp.bfloat16)
    numerator = jnp.einsum("shnqk,shnkd->shnqd", scores_low, vb, preferred_element_type=jnp.float32)
    mixed = numerator / denominator * valid_blk
    attended = from_blocks(mixed).astype(jnp.bfloat16)
    residual = stream + (jnp.dot(attended, proj_mat, preferred_element_type=jnp.float32) + bo)
    normed_two, norm_two_back = jax.vjp(normalize, residual, g2, b2)
    hidden_two = normed_two.astype(jnp.bfloat16)
    upper = jnp.dot(hidden_two, up_mat, preferred_element_type=jnp.float32) + bu
    activated, slope = gelu_parts(upper)
    act_low = activated.astype(jnp.bfloat16)
    result = residual + (jnp.dot(act_low, down_mat, preferred_element_type=jnp.float32) + bd)
    output = result.astype(jnp.bfloat16)

    upward = cotangent
    grad_out = upward.astype(jnp.float32)
    down_grad = contract_rows(act_low, upward).astype(jnp.bfloat16)
    down_grad, upward = lax.optimization_barrier((down_grad, upward))
    scattered_down = lax.psum_scatter(down_grad, "wide", scatter_dimension=0, tiled=True)
    grad_act = times_transposed(upward, down_mat)
    grad_upper = (grad_act * slope).astype(jnp.bfloat16)
    grad_hidden_two = times_transposed(grad_upper, up_mat)
    grad_residual_norm, gain_two_grad, shift_two_grad = norm_two_back(grad_hidden_two)
    grad_residual = grad_out + grad_residual_norm
    grad_proj_in = grad_residual.astype(jnp.bfloat16)
    grad_attended = times_transposed(grad_proj_in, proj_mat)
    up_grad = contract_rows(hidden_two, grad_upper).astype(jnp.bfloat16)
    proj_grad = contract_rows(attended, grad_proj_in).astype(jnp.bfloat16)
    packed_one = jnp.concatenate([up_grad, proj_grad], axis=1)
    packed_one, grad_attended = lax.optimization_barrier((packed_one, grad_attended))
    scattered_one = lax.psum_scatter(packed_one, "wide", scatter_dimension=0, tiled=True)
    down_bias_grad = column_sums(upward)
    up_bias_grad = column_sums(grad_upper)
    proj_bias_grad = column_sums(grad_proj_in)

    head_grad = to_blocks(grad_attended, nseq, HD)
    scaled = head_grad * valid_blk
    grad_num = (scaled / denominator).astype(jnp.bfloat16)
    grad_den = -jnp.sum(scaled * numerator, axis=-1, keepdims=True) / (denominator * denominator)
    grad_scores = jnp.einsum("shnqd,shnkd->shnqk", grad_num, vb, preferred_element_type=jnp.float32)
    grad_scores = (grad_scores + grad_den).astype(jnp.bfloat16)
    grad_scores = jnp.where(allowed, grad_scores, jnp.zeros((), jnp.bfloat16))
    grad_vwin = jnp.einsum("shnqk,shnqd->shnkd", scores_low, grad_num, preferred_element_type=jnp.float32)
    grad_value = from_blocks(unwindow(grad_vwin)).astype(jnp.bfloat16)
    grad_qf = jnp.einsum("shnqk,shnkf->shnqf", grad_scores, pk, preferred_element_type=jnp.float32)
    grad_kwin = jnp.einsum("shnqk,shnqf->shnkf", grad_scores, pq, preferred_element_type=jnp.float32)
    grad_qf = from_blocks(grad_qf).reshape(total, HEADS, FEAT)
    grad_kf = from_blocks(unwindow(grad_kwin)).reshape(total, HEADS, FEAT)
    grad_key = key_back(grad_kf)[0].astype(jnp.bfloat16)
    grad_query = query_back(grad_qf)[0].astype(jnp.bfloat16)
    scattered_down, scattered_one, grad_query, grad_key = lax.optimization_barrier(
        (scattered_down, scattered_one, grad_query, grad_key)
    )
    grad_qkv = jnp.concatenate([grad_query, grad_key, grad_value], axis=1)
    down_share = lax.psum(scattered_down, "narrow")
    share_one = lax.psum(scattered_one, "narrow")
    qkv_grad = contract_rows(hidden_one, grad_qkv)
    qkv_bias_grad = column_sums(grad_qkv)

    small_grads = (
        qkv_bias_grad[:D],
        qkv_bias_grad[D:2 * D],
        qkv_bias_grad[2 * D:],
        proj_bias_grad,
        gain_two_grad,
        shift_two_grad,
        down_bias_grad,
        up_bias_grad,
    )
    packed_two = jnp.concatenate([qkv_grad, as_columns(small_grads, D)], axis=1)
    down_share, share_one, packed_two = lax.optimization_barrier((down_share, share_one, packed_two))
    down_share = down_share.astype(jnp.float32)
    up_share = share_one[:, :ff].astype(jnp.float32)
    proj_share = share_one[:, ff:].astype(jnp.float32)
    share_two = reduce_rows(packed_two)
    small_out = []
    offset = 3 * D
    for cols in small_cols[2:]:
        small_out.append(share_two[:, offset:offset + cols].reshape(-1))
        offset += cols
    (
        query_bias_share,
        key_bias_share,
        value_bias_share,
        proj_bias_share,
        gain_two_share,
        shift_two_share,
        down_bias_share,
        up_bias_share,
    ) = small_out

    grad_hidden_one = times_transposed(grad_qkv, first[:, :3 * D])
    grad_stream_norm, gain_one_grad, shift_one_grad = norm_one_back(grad_hidden_one)
    input_grad = grad_residual + grad_stream_norm
    me = lax.axis_index("wide")
    ln1_pair = jnp.stack([gain_one_grad, shift_one_grad])
    ln1_pair = axis_sum(axis_sum(ln1_pair, "wide"), "narrow").reshape(2, wide, shard_rows)
    ln1_pair = lax.dynamic_index_in_dim(ln1_pair, me, axis=1, keepdims=False)
    gain_one_share = ln1_pair[0]
    shift_one_share = ln1_pair[1]
    return (
        output,
        input_grad,
        gain_one_share,
        shift_one_share,
        share_two[:, :D],
        query_bias_share,
        share_two[:, D:2 * D],
        key_bias_share,
        share_two[:, 2 * D:3 * D],
        value_bias_share,
        proj_share,
        proj_bias_share,
        gain_two_share,
        shift_two_share,
        up_share,
        up_bias_share,
        down_share,
        down_bias_share,
    )


def solution(mesh):
    in_specs = (
        P(("wide", "narrow"), None),
        P(("wide", "narrow"), None),
        P(("wide", "narrow"), None),
        P(),
        P("wide"),
        P("wide"),
        P("wide", None),
        P("wide"),
        P("wide", None),
        P("wide"),
        P("wide", None),
        P("wide"),
        P("wide", None),
        P("wide"),
        P("wide"),
        P("wide"),
        P("wide", None),
        P("wide"),
        P("wide", None),
        P("wide"),
    )
    out_specs = (
        P(("wide", "narrow"), None),
        P(("wide", "narrow"), None),
        P("wide"),
        P("wide"),
        P("wide", None),
        P("wide"),
        P("wide", None),
        P("wide"),
        P("wide", None),
        P("wide"),
        P("wide", None),
        P("wide"),
        P("wide"),
        P("wide"),
        P("wide", None),
        P("wide"),
        P("wide", None),
        P("wide"),
    )
    return jax.shard_map(
        on_device, mesh=mesh, in_specs=in_specs, out_specs=out_specs, check_vma=False
    )
```

```python
from functools import partial
import math

import jax
import jax.numpy as jnp
from jax import lax
from jax.sharding import PartitionSpec as P

D = 768
HEADS = 12
HD = 64
FEAT = 32
SEGS = 24
BLOCK = 128

EPSILON = 1e-05
HIGHEST = lax.Precision.HIGHEST


def pieces(lens_row, seq_len):
    seg_end = jnp.cumsum(lens_row)
    seg_start = seg_end - lens_row
    places = jnp.arange(seq_len, dtype=jnp.int32)
    segment = jnp.sum((places[:, None] >= seg_end[None, :]).astype(jnp.int32), axis=1)
    slots = jnp.arange(SEGS, dtype=jnp.int32)
    begins = jnp.sum(jnp.where(segment[:, None] == slots[None, :], seg_start[None, :], 0), axis=1)
    position = places - begins
    valid = (segment < SEGS - 1).astype(jnp.float32)
    return (position, valid, segment)


def rotate(heads_field, position):
    half = HD // 2
    rates = jnp.exp(jnp.arange(half, dtype=jnp.float32) * (-2.0 * math.log(10000.0) / HD))
    angles = position.astype(jnp.float32)[:, None] * rates[None, :]
    cosine = jnp.cos(angles)[:, None, :]
    sine = jnp.sin(angles)[:, None, :]
    first = heads_field[..., :half]
    second = heads_field[..., half:]
    return jnp.concatenate(
        [first * cosine - second * sine, second * cosine + first * sine], axis=-1
    )


def featurize(rotated, features):
    table = features.reshape(HD, HEADS, FEAT)
    scores = jnp.einsum("lhe,ehm->lhm", rotated, table, precision=lax.Precision.HIGH) * 0.125
    return jax.nn.elu(scores) + 1.0


def normalize(stream, gain, shift):
    average = jnp.mean(stream, axis=-1, keepdims=True)
    centered = stream - average
    variance = jnp.mean(centered * centered, axis=-1, keepdims=True)
    return centered * lax.rsqrt(variance + EPSILON) * gain + shift


def contract_rows(left, right):
    return lax.dot_general(
        left, right, (((0,), (0,)), ((), ())), preferred_element_type=jnp.float32
    )


def times_transposed(left, right):
    return lax.dot_general(
        left, right, (((1,), (1,)), ((), ())), preferred_element_type=jnp.float32
    )


def column_sums(matrix):
    return jnp.sum(matrix.astype(jnp.float32), axis=0)


def gather_rows(shard):
    return lax.all_gather(shard, "wide", axis=0, tiled=True)


def narrow_sum(share):
    size = lax.psum(1, "narrow")
    steps = size.bit_length() - 1
    assert 1 << steps == size
    me = lax.axis_index("narrow")
    rows = share.shape[0]
    assert rows % size == 0
    acc = share.astype(jnp.float32)
    for k in range(steps):
        half = acc.shape[0] // 2
        upper = ((me >> k) & 1) == 1
        lo, hi = acc[:half], acc[half:]
        keep = jnp.where(upper, hi, lo)
        send = jnp.where(upper, lo, hi).astype(jnp.bfloat16)
        pairs = [(i, i ^ (1 << k)) for i in range(size)]
        acc = keep + lax.ppermute(send, "narrow", pairs).astype(jnp.float32)
    part = acc.astype(jnp.bfloat16)
    for k in reversed(range(steps)):
        upper = ((me >> k) & 1) == 1
        pairs = [(i, i ^ (1 << k)) for i in range(size)]
        other = lax.ppermute(part, "narrow", pairs)
        part = jnp.where(upper, jnp.concatenate([other, part]), jnp.concatenate([part, other]))
    return part.astype(jnp.float32)


def axis_sum(value, axis):
    size = lax.psum(1, axis)
    steps = size.bit_length() - 1
    assert 1 << steps == size
    for k in range(steps):
        pairs = [(i, i ^ (1 << k)) for i in range(size)]
        value = value + lax.ppermute(value, axis, pairs)
    return value


def reduce_rows(full):
    share = lax.psum_scatter(full.astype(jnp.bfloat16), "wide", scatter_dimension=0, tiled=True)
    return narrow_sum(share)


def gelu_parts(upper):
    cdf = 0.5 * (1.0 + lax.erf(upper * math.sqrt(0.5)))
    slope = cdf + upper * jnp.exp(-0.5 * upper * upper) * (1.0 / math.sqrt(2.0 * math.pi))
    return upper * cdf, slope


def to_blocks(field, nseq, width):
    seq_len = field.shape[0] // nseq
    nb = seq_len // BLOCK
    return jnp.transpose(field.reshape(nseq, nb, BLOCK, HEADS, width), (0, 3, 1, 2, 4))


def from_blocks(blocks):
    nseq, heads, nb, block, width = blocks.shape
    return jnp.transpose(blocks, (0, 2, 3, 1, 4)).reshape(nseq * nb * block, heads * width)


def window(blocks, fill=0):
    pad = [(0, 0)] * blocks.ndim
    pad[-3] = (1, 0)
    prev = jnp.pad(blocks, pad, constant_values=fill)[..., :-1, :, :]
    return jnp.concatenate([prev, blocks], axis=-2)


def unwindow(win):
    own = win[..., BLOCK:, :]
    nxt = win[..., 1:, :BLOCK, :]
    pad = [(0, 0)] * win.ndim
    pad[-3] = (0, 1)
    return own + jnp.pad(nxt, pad)


def as_columns(vectors, rows):
    return jnp.concatenate([v.reshape(rows, -1) for v in vectors], axis=1)


def on_device(
    tokens,
    cotangent,
    lengths,
    features,
    ln1_gain,
    ln1_bias,
    q_weight,
    q_bias,
    k_weight,
    k_bias,
    v_weight,
    v_bias,
    out_weight,
    out_bias,
    ln2_gain,
    ln2_bias,
    up_weight,
    up_bias,
    down_weight,
    down_bias,
):
    nseq = lengths.shape[0]
    total = tokens.shape[0]
    seq_len = total // nseq
    nb = seq_len // BLOCK
    shard_rows = ln1_gain.shape[0]
    wide = D // shard_rows

    small_shards = (ln1_gain, ln1_bias, q_bias, k_bias, v_bias, out_bias, ln2_gain, ln2_bias, down_bias, up_bias)
    small_cols = [piece.shape[0] // shard_rows for piece in small_shards]
    first = gather_rows(
        jnp.concatenate([q_weight, k_weight, v_weight, as_columns(small_shards, shard_rows)], axis=1)
    )
    query_mat = first[:, :D]
    key_mat = first[:, D:2 * D]
    value_mat = first[:, 2 * D:3 * D]
    smalls = []
    offset = 3 * D
    for cols in small_cols:
        smalls.append(first[:, offset:offset + cols].astype(jnp.float32).reshape(-1))
        offset += cols
    g1, b1, bq, bk, bv, bo, g2, b2, bd, bu = smalls
    ff = up_weight.shape[1]
    second = gather_rows(jnp.concatenate([out_weight, up_weight], axis=1))
    proj_mat = second[:, :D]
    up_mat = second[:, D:]
    down_mat = gather_rows(down_weight)

    position, valid, segment = jax.vmap(partial(pieces, seq_len=seq_len))(lengths)
    position = position.reshape(total)
    seg_blocks = segment.reshape(nseq, nb, BLOCK)
    seg_win = window(seg_blocks[..., None], fill=-1)[..., 0]
    rel_q = jnp.arange(BLOCK, dtype=jnp.int32)[:, None]
    rel_k = jnp.arange(2 * BLOCK, dtype=jnp.int32)[None, :]
    allowed = (rel_k <= rel_q + BLOCK)[None, None] & (
        seg_win[:, :, None, :] == seg_blocks[:, :, :, None]
    )
    allowed = allowed[:, None]
    valid_blk = valid.reshape(nseq, 1, nb, BLOCK, 1)

    stream = tokens.astype(jnp.float32)
    normed_one, norm_one_back = jax.vjp(normalize, stream, g1, b1)
    hidden_one = normed_one.astype(jnp.bfloat16)
    query_pre = jnp.dot(hidden_one, query_mat, preferred_element_type=jnp.float32) + bq
    key_pre = jnp.dot(hidden_one, key_mat, preferred_element_type=jnp.float32) + bk
    values = (jnp.dot(hidden_one, value_mat, preferred_element_type=jnp.float32) + bv).astype(jnp.bfloat16)

    def features_of(projected):
        return featurize(rotate(projected.reshape(total, HEADS, HD), position), features)

    query_feat, query_back = jax.vjp(features_of, query_pre)
    key_feat, key_back = jax.vjp(features_of, key_pre)
    pq = to_blocks(query_feat.astype(jnp.bfloat16).reshape(total, HEADS * FEAT), nseq, FEAT)
    pk = window(to_blocks(key_feat.astype(jnp.bfloat16).reshape(total, HEADS * FEAT), nseq, FEAT))
    vb = window(to_blocks(values, nseq, HD))

    scores = jnp.einsum("shnqf,shnkf->shnqk", pq, pk, preferred_element_type=jnp.float32)
    scores = jnp.where(allowed, scores, 0.0)
    denominator = jnp.sum(scores, axis=-1, keepdims=True)
    scores_low = scores.astype(jnp.bfloat16)
    numerator = jnp.einsum("shnqk,shnkd->shnqd", scores_low, vb, preferred_element_type=jnp.float32)
    mixed = numerator / denominator * valid_blk
    attended = from_blocks(mixed).astype(jnp.bfloat16)
    residual = stream + (jnp.dot(attended, proj_mat, preferred_element_type=jnp.float32) + bo)
    normed_two, norm_two_back = jax.vjp(normalize, residual, g2, b2)
    hidden_two = normed_two.astype(jnp.bfloat16)
    upper = jnp.dot(hidden_two, up_mat, preferred_element_type=jnp.float32) + bu
    activated, slope = gelu_parts(upper)
    act_low = activated.astype(jnp.bfloat16)
    result = residual + (jnp.dot(act_low, down_mat, preferred_element_type=jnp.float32) + bd)
    output = result.astype(jnp.bfloat16)

    upward = cotangent
    grad_out = upward.astype(jnp.float32)
    down_grad = contract_rows(act_low, upward).astype(jnp.bfloat16)
    down_grad, upward = lax.optimization_barrier((down_grad, upward))
    scattered_down = lax.psum_scatter(down_grad, "wide", scatter_dimension=0, tiled=True)
    grad_act = times_transposed(upward, down_mat)
    grad_upper = (grad_act * slope).astype(jnp.bfloat16)
    grad_hidden_two = times_transposed(grad_upper, up_mat)
    grad_residual_norm, gain_two_grad, shift_two_grad = norm_two_back(grad_hidden_two)
    grad_residual = grad_out + grad_residual_norm
    grad_proj_in = grad_residual.astype(jnp.bfloat16)
    grad_attended = times_transposed(grad_proj_in, proj_mat)
    up_grad = contract_rows(hidden_two, grad_upper).astype(jnp.bfloat16)
    proj_grad = contract_rows(attended, grad_proj_in).astype(jnp.bfloat16)
    packed_one = jnp.concatenate([up_grad, proj_grad], axis=1)
    packed_one, grad_attended = lax.optimization_barrier((packed_one, grad_attended))
    scattered_one = lax.psum_scatter(packed_one, "wide", scatter_dimension=0, tiled=True)
    down_bias_grad = column_sums(upward)
    up_bias_grad = column_sums(grad_upper)
    proj_bias_grad = column_sums(grad_proj_in)

    head_grad = to_blocks(grad_attended, nseq, HD)
    scaled = head_grad * valid_blk
    grad_num = (scaled / denominator).astype(jnp.bfloat16)
    grad_den = -jnp.sum(scaled * numerator, axis=-1, keepdims=True) / (denominator * denominator)
    grad_scores = jnp.einsum("shnqd,shnkd->shnqk", grad_num, vb, preferred_element_type=jnp.float32)
    grad_scores = (grad_scores + grad_den).astype(jnp.bfloat16)
    grad_scores = jnp.where(allowed, grad_scores, jnp.zeros((), jnp.bfloat16))
    grad_vwin = jnp.einsum("shnqk,shnqd->shnkd", scores_low, grad_num, preferred_element_type=jnp.float32)
    grad_value = from_blocks(unwindow(grad_vwin)).astype(jnp.bfloat16)
    grad_qf = jnp.einsum("shnqk,shnkf->shnqf", grad_scores, pk, preferred_element_type=jnp.float32)
    grad_kwin = jnp.einsum("shnqk,shnqf->shnkf", grad_scores, pq, preferred_element_type=jnp.float32)
    grad_qf = from_blocks(grad_qf).reshape(total, HEADS, FEAT)
    grad_kf = from_blocks(unwindow(grad_kwin)).reshape(total, HEADS, FEAT)
    grad_key = key_back(grad_kf)[0].astype(jnp.bfloat16)
    grad_query = query_back(grad_qf)[0].astype(jnp.bfloat16)
    scattered_down, scattered_one, grad_query, grad_key = lax.optimization_barrier(
        (scattered_down, scattered_one, grad_query, grad_key)
    )
    grad_qkv = jnp.concatenate([grad_query, grad_key, grad_value], axis=1)
    down_share = lax.psum(scattered_down, "narrow")
    share_one = lax.psum(scattered_one, "narrow")
    qkv_grad = contract_rows(hidden_one, grad_qkv)
    qkv_bias_grad = column_sums(grad_qkv)

    small_grads = (
        qkv_bias_grad[:D],
        qkv_bias_grad[D:2 * D],
        qkv_bias_grad[2 * D:],
        proj_bias_grad,
        gain_two_grad,
        shift_two_grad,
        down_bias_grad,
        up_bias_grad,
    )
    packed_two = jnp.concatenate([qkv_grad, as_columns(small_grads, D)], axis=1)
    down_share, share_one, packed_two = lax.optimization_barrier((down_share, share_one, packed_two))
    down_share = down_share.astype(jnp.float32)
    up_share = share_one[:, :ff].astype(jnp.float32)
    proj_share = share_one[:, ff:].astype(jnp.float32)
    share_two = reduce_rows(packed_two)
    small_out = []
    offset = 3 * D
    for cols in small_cols[2:]:
        small_out.append(share_two[:, offset:offset + cols].reshape(-1))
        offset += cols
    (
        query_bias_share,
        key_bias_share,
        value_bias_share,
        proj_bias_share,
        gain_two_share,
        shift_two_share,
        down_bias_share,
        up_bias_share,
    ) = small_out

    grad_hidden_one = times_transposed(grad_qkv, first[:, :3 * D])
    grad_stream_norm, gain_one_grad, shift_one_grad = norm_one_back(grad_hidden_one)
    input_grad = grad_residual + grad_stream_norm
    me = lax.axis_index("wide")
    ln1_pair = jnp.stack([gain_one_grad, shift_one_grad])
    ln1_pair = axis_sum(axis_sum(ln1_pair, "wide"), "narrow").reshape(2, wide, shard_rows)
    ln1_pair = lax.dynamic_index_in_dim(ln1_pair, me, axis=1, keepdims=False)
    gain_one_share = ln1_pair[0]
    shift_one_share = ln1_pair[1]
    return (
        output,
        input_grad,
        gain_one_share,
        shift_one_share,
        share_two[:, :D],
        query_bias_share,
        share_two[:, D:2 * D],
        key_bias_share,
        share_two[:, 2 * D:3 * D],
        value_bias_share,
        proj_share,
        proj_bias_share,
        gain_two_share,
        shift_two_share,
        up_share,
        up_bias_share,
        down_share,
        down_bias_share,
    )


def solution(mesh):
    in_specs = (
        P(("wide", "narrow"), None),
        P(("wide", "narrow"), None),
        P(("wide", "narrow"), None),
        P(),
        P("wide"),
        P("wide"),
        P("wide", None),
        P("wide"),
        P("wide", None),
        P("wide"),
        P("wide", None),
        P("wide"),
        P("wide", None),
        P("wide"),
        P("wide"),
        P("wide"),
        P("wide", None),
        P("wide"),
        P("wide", None),
        P("wide"),
    )
    out_specs = (
        P(("wide", "narrow"), None),
        P(("wide", "narrow"), None),
        P("wide"),
        P("wide"),
        P("wide", None),
        P("wide"),
        P("wide", None),
        P("wide"),
        P("wide", None),
        P("wide"),
        P("wide", None),
        P("wide"),
        P("wide"),
        P("wide"),
        P("wide", None),
        P("wide"),
        P("wide", None),
        P("wide"),
    )
    return jax.shard_map(
        on_device, mesh=mesh, in_specs=in_specs, out_specs=out_specs, check_vma=False
    )
```

```python
from functools import partial
import math

import jax
import jax.numpy as jnp
from jax import lax
from jax.sharding import PartitionSpec as P

D = 768
HEADS = 12
HD = 64
FEAT = 32
SEGS = 24
BLOCK = 128

EPSILON = 1e-05
HIGHEST = lax.Precision.HIGHEST


def pieces(lens_row, seq_len):
    seg_end = jnp.cumsum(lens_row)
    seg_start = seg_end - lens_row
    places = jnp.arange(seq_len, dtype=jnp.int32)
    segment = jnp.sum((places[:, None] >= seg_end[None, :]).astype(jnp.int32), axis=1)
    slots = jnp.arange(SEGS, dtype=jnp.int32)
    begins = jnp.sum(jnp.where(segment[:, None] == slots[None, :], seg_start[None, :], 0), axis=1)
    position = places - begins
    valid = (segment < SEGS - 1).astype(jnp.float32)
    return (position, valid, segment)


def rotate(heads_field, position):
    half = HD // 2
    rates = jnp.exp(jnp.arange(half, dtype=jnp.float32) * (-2.0 * math.log(10000.0) / HD))
    angles = position.astype(jnp.float32)[:, None] * rates[None, :]
    cosine = jnp.cos(angles)[:, None, :]
    sine = jnp.sin(angles)[:, None, :]
    first = heads_field[..., :half]
    second = heads_field[..., half:]
    return jnp.concatenate(
        [first * cosine - second * sine, second * cosine + first * sine], axis=-1
    )


def featurize(rotated, features):
    table = features.reshape(HD, HEADS, FEAT)
    scores = jnp.einsum("lhe,ehm->lhm", rotated, table, precision=lax.Precision.HIGH) * 0.125
    return jax.nn.elu(scores) + 1.0


def normalize(stream, gain, shift):
    average = jnp.mean(stream, axis=-1, keepdims=True)
    centered = stream - average
    variance = jnp.mean(centered * centered, axis=-1, keepdims=True)
    return centered * lax.rsqrt(variance + EPSILON) * gain + shift


def contract_rows(left, right):
    return lax.dot_general(
        left, right, (((0,), (0,)), ((), ())), preferred_element_type=jnp.float32
    )


def times_transposed(left, right):
    return lax.dot_general(
        left, right, (((1,), (1,)), ((), ())), preferred_element_type=jnp.float32
    )


def column_sums(matrix):
    return jnp.sum(matrix.astype(jnp.float32), axis=0)


def gather_rows(shard):
    return lax.all_gather(shard, "wide", axis=0, tiled=True)


def narrow_sum(share):
    size = lax.psum(1, "narrow")
    steps = size.bit_length() - 1
    assert 1 << steps == size
    me = lax.axis_index("narrow")
    rows = share.shape[0]
    assert rows % size == 0
    acc = share.astype(jnp.float32)
    for k in range(steps):
        half = acc.shape[0] // 2
        upper = ((me >> k) & 1) == 1
        lo, hi = acc[:half], acc[half:]
        keep = jnp.where(upper, hi, lo)
        send = jnp.where(upper, lo, hi).astype(jnp.bfloat16)
        pairs = [(i, i ^ (1 << k)) for i in range(size)]
        acc = keep + lax.ppermute(send, "narrow", pairs).astype(jnp.float32)
    part = acc.astype(jnp.bfloat16)
    for k in reversed(range(steps)):
        upper = ((me >> k) & 1) == 1
        pairs = [(i, i ^ (1 << k)) for i in range(size)]
        other = lax.ppermute(part, "narrow", pairs)
        part = jnp.where(upper, jnp.concatenate([other, part]), jnp.concatenate([part, other]))
    return part.astype(jnp.float32)


def axis_sum(value, axis):
    size = lax.psum(1, axis)
    steps = size.bit_length() - 1
    assert 1 << steps == size
    for k in range(steps):
        pairs = [(i, i ^ (1 << k)) for i in range(size)]
        value = value + lax.ppermute(value, axis, pairs)
    return value


def reduce_rows(full):
    share = lax.psum_scatter(full.astype(jnp.bfloat16), "wide", scatter_dimension=0, tiled=True)
    return narrow_sum(share)


def gelu_parts(upper):
    cdf = 0.5 * (1.0 + lax.erf(upper * math.sqrt(0.5)))
    slope = cdf + upper * jnp.exp(-0.5 * upper * upper) * (1.0 / math.sqrt(2.0 * math.pi))
    return upper * cdf, slope


def to_blocks(field, nseq, width):
    seq_len = field.shape[0] // nseq
    nb = seq_len // BLOCK
    return jnp.transpose(field.reshape(nseq, nb, BLOCK, HEADS, width), (0, 3, 1, 2, 4))


def from_blocks(blocks):
    nseq, heads, nb, block, width = blocks.shape
    return jnp.transpose(blocks, (0, 2, 3, 1, 4)).reshape(nseq * nb * block, heads * width)


def window(blocks, fill=0):
    pad = [(0, 0)] * blocks.ndim
    pad[-3] = (1, 0)
    prev = jnp.pad(blocks, pad, constant_values=fill)[..., :-1, :, :]
    return jnp.concatenate([prev, blocks], axis=-2)


def unwindow(win):
    own = win[..., BLOCK:, :]
    nxt = win[..., 1:, :BLOCK, :]
    pad = [(0, 0)] * win.ndim
    pad[-3] = (0, 1)
    return own + jnp.pad(nxt, pad)


def as_columns(vectors, rows):
    return jnp.concatenate([v.reshape(rows, -1) for v in vectors], axis=1)


def on_device(
    tokens,
    cotangent,
    lengths,
    features,
    ln1_gain,
    ln1_bias,
    q_weight,
    q_bias,
    k_weight,
    k_bias,
    v_weight,
    v_bias,
    out_weight,
    out_bias,
    ln2_gain,
    ln2_bias,
    up_weight,
    up_bias,
    down_weight,
    down_bias,
):
    nseq = lengths.shape[0]
    total = tokens.shape[0]
    seq_len = total // nseq
    nb = seq_len // BLOCK
    shard_rows = ln1_gain.shape[0]
    wide = D // shard_rows

    small_shards = (ln1_gain, ln1_bias, q_bias, k_bias, v_bias, out_bias, ln2_gain, ln2_bias, down_bias, up_bias)
    small_cols = [piece.shape[0] // shard_rows for piece in small_shards]
    first = gather_rows(
        jnp.concatenate([q_weight, k_weight, v_weight, as_columns(small_shards, shard_rows)], axis=1)
    )
    query_mat = first[:, :D]
    key_mat = first[:, D:2 * D]
    value_mat = first[:, 2 * D:3 * D]
    smalls = []
    offset = 3 * D
    for cols in small_cols:
        smalls.append(first[:, offset:offset + cols].astype(jnp.float32).reshape(-1))
        offset += cols
    g1, b1, bq, bk, bv, bo, g2, b2, bd, bu = smalls
    ff = up_weight.shape[1]
    second = gather_rows(jnp.concatenate([out_weight, up_weight], axis=1))
    proj_mat = second[:, :D]
    up_mat = second[:, D:]
    down_mat = gather_rows(down_weight)

    position, valid, segment = jax.vmap(partial(pieces, seq_len=seq_len))(lengths)
    position = position.reshape(total)
    seg_blocks = segment.reshape(nseq, nb, BLOCK)
    seg_win = window(seg_blocks[..., None], fill=-1)[..., 0]
    rel_q = jnp.arange(BLOCK, dtype=jnp.int32)[:, None]
    rel_k = jnp.arange(2 * BLOCK, dtype=jnp.int32)[None, :]
    allowed = (rel_k <= rel_q + BLOCK)[None, None] & (
        seg_win[:, :, None, :] == seg_blocks[:, :, :, None]
    )
    allowed = allowed[:, None]
    valid_blk = valid.reshape(nseq, 1, nb, BLOCK, 1)

    stream = tokens.astype(jnp.float32)
    normed_one, norm_one_back = jax.vjp(normalize, stream, g1, b1)
    hidden_one = normed_one.astype(jnp.bfloat16)
    qkv = jnp.dot(hidden_one, first[:, :3 * D], preferred_element_type=jnp.float32)
    query_pre = qkv[:, :D] + bq
    key_pre = qkv[:, D:2 * D] + bk
    values = (qkv[:, 2 * D:] + bv).astype(jnp.bfloat16)

    def features_of(projected):
        return featurize(rotate(projected.reshape(total, HEADS, HD), position), features)

    query_feat, query_back = jax.vjp(features_of, query_pre)
    key_feat, key_back = jax.vjp(features_of, key_pre)
    pq = to_blocks(query_feat.astype(jnp.bfloat16).reshape(total, HEADS * FEAT), nseq, FEAT)
    pk = window(to_blocks(key_feat.astype(jnp.bfloat16).reshape(total, HEADS * FEAT), nseq, FEAT))
    vb = window(to_blocks(values, nseq, HD))

    scores = jnp.einsum("shnqf,shnkf->shnqk", pq, pk, preferred_element_type=jnp.float32)
    scores = jnp.where(allowed, scores, 0.0)
    denominator = jnp.sum(scores, axis=-1, keepdims=True)
    scores_low = scores.astype(jnp.bfloat16)
    numerator = jnp.einsum("shnqk,shnkd->shnqd", scores_low, vb, preferred_element_type=jnp.float32)
    mixed = numerator / denominator * valid_blk
    attended = from_blocks(mixed).astype(jnp.bfloat16)
    residual = stream + (jnp.dot(attended, proj_mat, preferred_element_type=jnp.float32) + bo)
    normed_two, norm_two_back = jax.vjp(normalize, residual, g2, b2)
    hidden_two = normed_two.astype(jnp.bfloat16)
    upper = jnp.dot(hidden_two, up_mat, preferred_element_type=jnp.float32) + bu
    activated, slope = gelu_parts(upper)
    act_low = activated.astype(jnp.bfloat16)
    result = residual + (jnp.dot(act_low, down_mat, preferred_element_type=jnp.float32) + bd)
    output = result.astype(jnp.bfloat16)

    upward = cotangent
    grad_out = upward.astype(jnp.float32)
    down_grad = contract_rows(act_low, upward).astype(jnp.bfloat16)
    down_grad, upward = lax.optimization_barrier((down_grad, upward))
    scattered_down = lax.psum_scatter(down_grad, "wide", scatter_dimension=0, tiled=True)
    grad_act = times_transposed(upward, down_mat)
    grad_upper = (grad_act * slope).astype(jnp.bfloat16)
    grad_hidden_two = times_transposed(grad_upper, up_mat)
    grad_residual_norm, gain_two_grad, shift_two_grad = norm_two_back(grad_hidden_two)
    grad_residual = grad_out + grad_residual_norm
    grad_proj_in = grad_residual.astype(jnp.bfloat16)
    grad_attended = times_transposed(grad_proj_in, proj_mat)
    up_grad = contract_rows(hidden_two, grad_upper).astype(jnp.bfloat16)
    proj_grad = contract_rows(attended, grad_proj_in).astype(jnp.bfloat16)
    packed_one = jnp.concatenate([up_grad, proj_grad], axis=1)
    packed_one, grad_attended = lax.optimization_barrier((packed_one, grad_attended))
    scattered_one = lax.psum_scatter(packed_one, "wide", scatter_dimension=0, tiled=True)
    down_bias_grad = column_sums(upward)
    up_bias_grad = column_sums(grad_upper)
    proj_bias_grad = column_sums(grad_proj_in)

    head_grad = to_blocks(grad_attended, nseq, HD)
    scaled = head_grad * valid_blk
    grad_num = (scaled / denominator).astype(jnp.bfloat16)
    grad_den = -jnp.sum(scaled * numerator, axis=-1, keepdims=True) / (denominator * denominator)
    grad_scores = jnp.einsum("shnqd,shnkd->shnqk", grad_num, vb, preferred_element_type=jnp.float32)
    grad_scores = (grad_scores + grad_den).astype(jnp.bfloat16)
    grad_scores = jnp.where(allowed, grad_scores, jnp.zeros((), jnp.bfloat16))
    grad_vwin = jnp.einsum("shnqk,shnqd->shnkd", scores_low, grad_num, preferred_element_type=jnp.float32)
    grad_value = from_blocks(unwindow(grad_vwin)).astype(jnp.bfloat16)
    grad_qf = jnp.einsum("shnqk,shnkf->shnqf", grad_scores, pk, preferred_element_type=jnp.float32)
    grad_kwin = jnp.einsum("shnqk,shnqf->shnkf", grad_scores, pq, preferred_element_type=jnp.float32)
    grad_qf = from_blocks(grad_qf).reshape(total, HEADS, FEAT)
    grad_kf = from_blocks(unwindow(grad_kwin)).reshape(total, HEADS, FEAT)
    grad_key = key_back(grad_kf)[0].astype(jnp.bfloat16)
    grad_query = query_back(grad_qf)[0].astype(jnp.bfloat16)
    scattered_down, scattered_one, grad_query, grad_key = lax.optimization_barrier(
        (scattered_down, scattered_one, grad_query, grad_key)
    )
    grad_qkv = jnp.concatenate([grad_query, grad_key, grad_value], axis=1)
    down_share = lax.psum(scattered_down, "narrow")
    share_one = lax.psum(scattered_one, "narrow")
    qkv_grad = contract_rows(hidden_one, grad_qkv)
    qkv_bias_grad = column_sums(grad_qkv)

    small_grads = (
        qkv_bias_grad[:D],
        qkv_bias_grad[D:2 * D],
        qkv_bias_grad[2 * D:],
        proj_bias_grad,
        gain_two_grad,
        shift_two_grad,
        down_bias_grad,
        up_bias_grad,
    )
    packed_two = jnp.concatenate([qkv_grad, as_columns(small_grads, D)], axis=1)
    down_share, share_one, packed_two = lax.optimization_barrier((down_share, share_one, packed_two))
    down_share = down_share.astype(jnp.float32)
    up_share = share_one[:, :ff].astype(jnp.float32)
    proj_share = share_one[:, ff:].astype(jnp.float32)
    share_two = reduce_rows(packed_two)
    small_out = []
    offset = 3 * D
    for cols in small_cols[2:]:
        small_out.append(share_two[:, offset:offset + cols].reshape(-1))
        offset += cols
    (
        query_bias_share,
        key_bias_share,
        value_bias_share,
        proj_bias_share,
        gain_two_share,
        shift_two_share,
        down_bias_share,
        up_bias_share,
    ) = small_out

    grad_hidden_one = times_transposed(grad_qkv, first[:, :3 * D])
    grad_stream_norm, gain_one_grad, shift_one_grad = norm_one_back(grad_hidden_one)
    input_grad = grad_residual + grad_stream_norm
    me = lax.axis_index("wide")
    ln1_pair = jnp.stack([gain_one_grad, shift_one_grad])
    ln1_pair = axis_sum(axis_sum(ln1_pair, "wide"), "narrow").reshape(2, wide, shard_rows)
    ln1_pair = lax.dynamic_index_in_dim(ln1_pair, me, axis=1, keepdims=False)
    gain_one_share = ln1_pair[0]
    shift_one_share = ln1_pair[1]
    return (
        output,
        input_grad,
        gain_one_share,
        shift_one_share,
        share_two[:, :D],
        query_bias_share,
        share_two[:, D:2 * D],
        key_bias_share,
        share_two[:, 2 * D:3 * D],
        value_bias_share,
        proj_share,
        proj_bias_share,
        gain_two_share,
        shift_two_share,
        up_share,
        up_bias_share,
        down_share,
        down_bias_share,
    )


def solution(mesh):
    in_specs = (
        P(("wide", "narrow"), None),
        P(("wide", "narrow"), None),
        P(("wide", "narrow"), None),
        P(),
        P("wide"),
        P("wide"),
        P("wide", None),
        P("wide"),
        P("wide", None),
        P("wide"),
        P("wide", None),
        P("wide"),
        P("wide", None),
        P("wide"),
        P("wide"),
        P("wide"),
        P("wide", None),
        P("wide"),
        P("wide", None),
        P("wide"),
    )
    out_specs = (
        P(("wide", "narrow"), None),
        P(("wide", "narrow"), None),
        P("wide"),
        P("wide"),
        P("wide", None),
        P("wide"),
        P("wide", None),
        P("wide"),
        P("wide", None),
        P("wide"),
        P("wide", None),
        P("wide"),
        P("wide"),
        P("wide"),
        P("wide", None),
        P("wide"),
        P("wide", None),
        P("wide"),
    )
    return jax.shard_map(
        on_device, mesh=mesh, in_specs=in_specs, out_specs=out_specs, check_vma=False
    )
```

```python
from functools import partial
import math

import jax
import jax.numpy as jnp
from jax import lax
from jax.sharding import PartitionSpec as P

D = 768
HEADS = 12
HD = 64
FEAT = 32
SEGS = 24
BLOCK = 128

EPSILON = 1e-05
HIGHEST = lax.Precision.HIGHEST


def pieces(lens_row, seq_len):
    seg_end = jnp.cumsum(lens_row)
    seg_start = seg_end - lens_row
    places = jnp.arange(seq_len, dtype=jnp.int32)
    segment = jnp.sum((places[:, None] >= seg_end[None, :]).astype(jnp.int32), axis=1)
    slots = jnp.arange(SEGS, dtype=jnp.int32)
    begins = jnp.sum(jnp.where(segment[:, None] == slots[None, :], seg_start[None, :], 0), axis=1)
    position = places - begins
    valid = (segment < SEGS - 1).astype(jnp.float32)
    return (position, valid, segment)


def rotate(heads_field, position):
    half = HD // 2
    rates = jnp.exp(jnp.arange(half, dtype=jnp.float32) * (-2.0 * math.log(10000.0) / HD))
    angles = position.astype(jnp.float32)[:, None] * rates[None, :]
    cosine = jnp.cos(angles)[:, None, :]
    sine = jnp.sin(angles)[:, None, :]
    first = heads_field[..., :half]
    second = heads_field[..., half:]
    return jnp.concatenate(
        [first * cosine - second * sine, second * cosine + first * sine], axis=-1
    )


def featurize(rotated, features):
    table = features.reshape(HD, HEADS, FEAT)
    scores = jnp.einsum("lhe,ehm->lhm", rotated, table, preferred_element_type=jnp.float32) * 0.125
    return jax.nn.elu(scores) + 1.0


def normalize(stream, gain, shift):
    average = jnp.mean(stream, axis=-1, keepdims=True)
    centered = stream - average
    variance = jnp.mean(centered * centered, axis=-1, keepdims=True)
    return centered * lax.rsqrt(variance + EPSILON) * gain + shift


def contract_rows(left, right):
    return lax.dot_general(
        left, right, (((0,), (0,)), ((), ())), preferred_element_type=jnp.float32
    )


def times_transposed(left, right):
    return lax.dot_general(
        left, right, (((1,), (1,)), ((), ())), preferred_element_type=jnp.float32
    )


def column_sums(matrix):
    return jnp.sum(matrix.astype(jnp.float32), axis=0)


def gather_rows(shard):
    return lax.all_gather(shard, "wide", axis=0, tiled=True)


def narrow_sum(share):
    size = lax.psum(1, "narrow")
    steps = size.bit_length() - 1
    assert 1 << steps == size
    me = lax.axis_index("narrow")
    rows = share.shape[0]
    assert rows % size == 0
    acc = share.astype(jnp.float32)
    for k in range(steps):
        half = acc.shape[0] // 2
        upper = ((me >> k) & 1) == 1
        lo, hi = acc[:half], acc[half:]
        keep = jnp.where(upper, hi, lo)
        send = jnp.where(upper, lo, hi).astype(jnp.bfloat16)
        pairs = [(i, i ^ (1 << k)) for i in range(size)]
        acc = keep + lax.ppermute(send, "narrow", pairs).astype(jnp.float32)
    part = acc.astype(jnp.bfloat16)
    for k in reversed(range(steps)):
        upper = ((me >> k) & 1) == 1
        pairs = [(i, i ^ (1 << k)) for i in range(size)]
        other = lax.ppermute(part, "narrow", pairs)
        part = jnp.where(upper, jnp.concatenate([other, part]), jnp.concatenate([part, other]))
    return part.astype(jnp.float32)


def axis_sum(value, axis):
    size = lax.psum(1, axis)
    steps = size.bit_length() - 1
    assert 1 << steps == size
    for k in range(steps):
        pairs = [(i, i ^ (1 << k)) for i in range(size)]
        value = value + lax.ppermute(value, axis, pairs)
    return value


def reduce_rows(full):
    share = lax.psum_scatter(full.astype(jnp.bfloat16), "wide", scatter_dimension=0, tiled=True)
    return narrow_sum(share)


def gelu_parts(upper):
    cdf = 0.5 * (1.0 + lax.erf(upper * math.sqrt(0.5)))
    slope = cdf + upper * jnp.exp(-0.5 * upper * upper) * (1.0 / math.sqrt(2.0 * math.pi))
    return upper * cdf, slope


def to_blocks(field, nseq, width):
    seq_len = field.shape[0] // nseq
    nb = seq_len // BLOCK
    return jnp.transpose(field.reshape(nseq, nb, BLOCK, HEADS, width), (0, 3, 1, 2, 4))


def from_blocks(blocks):
    nseq, heads, nb, block, width = blocks.shape
    return jnp.transpose(blocks, (0, 2, 3, 1, 4)).reshape(nseq * nb * block, heads * width)


def window(blocks, fill=0):
    pad = [(0, 0)] * blocks.ndim
    pad[-3] = (1, 0)
    prev = jnp.pad(blocks, pad, constant_values=fill)[..., :-1, :, :]
    return jnp.concatenate([prev, blocks], axis=-2)


def unwindow(win):
    own = win[..., BLOCK:, :]
    nxt = win[..., 1:, :BLOCK, :]
    pad = [(0, 0)] * win.ndim
    pad[-3] = (0, 1)
    return own + jnp.pad(nxt, pad)


def as_columns(vectors, rows):
    return jnp.concatenate([v.reshape(rows, -1) for v in vectors], axis=1)


def on_device(
    tokens,
    cotangent,
    lengths,
    features,
    ln1_gain,
    ln1_bias,
    q_weight,
    q_bias,
    k_weight,
    k_bias,
    v_weight,
    v_bias,
    out_weight,
    out_bias,
    ln2_gain,
    ln2_bias,
    up_weight,
    up_bias,
    down_weight,
    down_bias,
):
    nseq = lengths.shape[0]
    total = tokens.shape[0]
    seq_len = total // nseq
    nb = seq_len // BLOCK
    shard_rows = ln1_gain.shape[0]
    wide = D // shard_rows

    small_shards = (ln1_gain, ln1_bias, q_bias, k_bias, v_bias, out_bias, ln2_gain, ln2_bias, down_bias, up_bias)
    small_cols = [piece.shape[0] // shard_rows for piece in small_shards]
    first = gather_rows(
        jnp.concatenate([q_weight, k_weight, v_weight, as_columns(small_shards, shard_rows)], axis=1)
    )
    query_mat = first[:, :D]
    key_mat = first[:, D:2 * D]
    value_mat = first[:, 2 * D:3 * D]
    smalls = []
    offset = 3 * D
    for cols in small_cols:
        smalls.append(first[:, offset:offset + cols].astype(jnp.float32).reshape(-1))
        offset += cols
    g1, b1, bq, bk, bv, bo, g2, b2, bd, bu = smalls
    ff = up_weight.shape[1]
    second = gather_rows(jnp.concatenate([out_weight, up_weight], axis=1))
    proj_mat = second[:, :D]
    up_mat = second[:, D:]
    down_mat = gather_rows(down_weight)

    position, valid, segment = jax.vmap(partial(pieces, seq_len=seq_len))(lengths)
    position = position.reshape(total)
    seg_blocks = segment.reshape(nseq, nb, BLOCK)
    seg_win = window(seg_blocks[..., None], fill=-1)[..., 0]
    rel_q = jnp.arange(BLOCK, dtype=jnp.int32)[:, None]
    rel_k = jnp.arange(2 * BLOCK, dtype=jnp.int32)[None, :]
    allowed = (rel_k <= rel_q + BLOCK)[None, None] & (
        seg_win[:, :, None, :] == seg_blocks[:, :, :, None]
    )
    allowed = allowed[:, None]
    valid_blk = valid.reshape(nseq, 1, nb, BLOCK, 1)

    stream = tokens.astype(jnp.float32)
    normed_one, norm_one_back = jax.vjp(normalize, stream, g1, b1)
    hidden_one = normed_one.astype(jnp.bfloat16)
    query_pre = jnp.dot(hidden_one, query_mat, preferred_element_type=jnp.float32) + bq
    key_pre = jnp.dot(hidden_one, key_mat, preferred_element_type=jnp.float32) + bk
    values = (jnp.dot(hidden_one, value_mat, preferred_element_type=jnp.float32) + bv).astype(jnp.bfloat16)

    def features_of(projected):
        return featurize(rotate(projected.reshape(total, HEADS, HD), position), features)

    query_feat, query_back = jax.vjp(features_of, query_pre)
    key_feat, key_back = jax.vjp(features_of, key_pre)
    pq = to_blocks(query_feat.astype(jnp.bfloat16).reshape(total, HEADS * FEAT), nseq, FEAT)
    pk = window(to_blocks(key_feat.astype(jnp.bfloat16).reshape(total, HEADS * FEAT), nseq, FEAT))
    vb = window(to_blocks(values, nseq, HD))

    scores = jnp.einsum("shnqf,shnkf->shnqk", pq, pk, preferred_element_type=jnp.float32)
    scores = jnp.where(allowed, scores, 0.0)
    denominator = jnp.sum(scores, axis=-1, keepdims=True)
    scores_low = scores.astype(jnp.bfloat16)
    numerator = jnp.einsum("shnqk,shnkd->shnqd", scores_low, vb, preferred_element_type=jnp.float32)
    mixed = numerator / denominator * valid_blk
    attended = from_blocks(mixed).astype(jnp.bfloat16)
    residual = stream + (jnp.dot(attended, proj_mat, preferred_element_type=jnp.float32) + bo)
    normed_two, norm_two_back = jax.vjp(normalize, residual, g2, b2)
    hidden_two = normed_two.astype(jnp.bfloat16)
    upper = jnp.dot(hidden_two, up_mat, preferred_element_type=jnp.float32) + bu
    activated, slope = gelu_parts(upper)
    act_low = activated.astype(jnp.bfloat16)
    result = residual + (jnp.dot(act_low, down_mat, preferred_element_type=jnp.float32) + bd)
    output = result.astype(jnp.bfloat16)

    upward = cotangent
    grad_out = upward.astype(jnp.float32)
    down_grad = contract_rows(act_low, upward).astype(jnp.bfloat16)
    down_grad, upward = lax.optimization_barrier((down_grad, upward))
    scattered_down = lax.psum_scatter(down_grad, "wide", scatter_dimension=0, tiled=True)
    grad_act = times_transposed(upward, down_mat)
    grad_upper = (grad_act * slope).astype(jnp.bfloat16)
    grad_hidden_two = times_transposed(grad_upper, up_mat)
    grad_residual_norm, gain_two_grad, shift_two_grad = norm_two_back(grad_hidden_two)
    grad_residual = grad_out + grad_residual_norm
    grad_proj_in = grad_residual.astype(jnp.bfloat16)
    grad_attended = times_transposed(grad_proj_in, proj_mat)
    up_grad = contract_rows(hidden_two, grad_upper).astype(jnp.bfloat16)
    proj_grad = contract_rows(attended, grad_proj_in).astype(jnp.bfloat16)
    packed_one = jnp.concatenate([up_grad, proj_grad], axis=1)
    packed_one, grad_attended = lax.optimization_barrier((packed_one, grad_attended))
    scattered_one = lax.psum_scatter(packed_one, "wide", scatter_dimension=0, tiled=True)
    down_bias_grad = column_sums(upward)
    up_bias_grad = column_sums(grad_upper)
    proj_bias_grad = column_sums(grad_proj_in)

    head_grad = to_blocks(grad_attended, nseq, HD)
    scaled = head_grad * valid_blk
    grad_num = (scaled / denominator).astype(jnp.bfloat16)
    grad_den = -jnp.sum(scaled * numerator, axis=-1, keepdims=True) / (denominator * denominator)
    grad_scores = jnp.einsum("shnqd,shnkd->shnqk", grad_num, vb, preferred_element_type=jnp.float32)
    grad_scores = (grad_scores + grad_den).astype(jnp.bfloat16)
    grad_scores = jnp.where(allowed, grad_scores, jnp.zeros((), jnp.bfloat16))
    grad_vwin = jnp.einsum("shnqk,shnqd->shnkd", scores_low, grad_num, preferred_element_type=jnp.float32)
    grad_value = from_blocks(unwindow(grad_vwin)).astype(jnp.bfloat16)
    grad_qf = jnp.einsum("shnqk,shnkf->shnqf", grad_scores, pk, preferred_element_type=jnp.float32)
    grad_kwin = jnp.einsum("shnqk,shnqf->shnkf", grad_scores, pq, preferred_element_type=jnp.float32)
    grad_qf = from_blocks(grad_qf).reshape(total, HEADS, FEAT)
    grad_kf = from_blocks(unwindow(grad_kwin)).reshape(total, HEADS, FEAT)
    grad_key = key_back(grad_kf)[0].astype(jnp.bfloat16)
    grad_query = query_back(grad_qf)[0].astype(jnp.bfloat16)
    scattered_down, scattered_one, grad_query, grad_key = lax.optimization_barrier(
        (scattered_down, scattered_one, grad_query, grad_key)
    )
    grad_qkv = jnp.concatenate([grad_query, grad_key, grad_value], axis=1)
    down_share = lax.psum(scattered_down, "narrow")
    share_one = lax.psum(scattered_one, "narrow")
    qkv_grad = contract_rows(hidden_one, grad_qkv)
    qkv_bias_grad = column_sums(grad_qkv)

    small_grads = (
        qkv_bias_grad[:D],
        qkv_bias_grad[D:2 * D],
        qkv_bias_grad[2 * D:],
        proj_bias_grad,
        gain_two_grad,
        shift_two_grad,
        down_bias_grad,
        up_bias_grad,
    )
    packed_two = jnp.concatenate([qkv_grad, as_columns(small_grads, D)], axis=1)
    down_share, share_one, packed_two = lax.optimization_barrier((down_share, share_one, packed_two))
    down_share = down_share.astype(jnp.float32)
    up_share = share_one[:, :ff].astype(jnp.float32)
    proj_share = share_one[:, ff:].astype(jnp.float32)
    share_two = reduce_rows(packed_two)
    small_out = []
    offset = 3 * D
    for cols in small_cols[2:]:
        small_out.append(share_two[:, offset:offset + cols].reshape(-1))
        offset += cols
    (
        query_bias_share,
        key_bias_share,
        value_bias_share,
        proj_bias_share,
        gain_two_share,
        shift_two_share,
        down_bias_share,
        up_bias_share,
    ) = small_out

    grad_hidden_one = times_transposed(grad_qkv, first[:, :3 * D])
    grad_stream_norm, gain_one_grad, shift_one_grad = norm_one_back(grad_hidden_one)
    input_grad = grad_residual + grad_stream_norm
    me = lax.axis_index("wide")
    ln1_pair = jnp.stack([gain_one_grad, shift_one_grad])
    ln1_pair = axis_sum(axis_sum(ln1_pair, "wide"), "narrow").reshape(2, wide, shard_rows)
    ln1_pair = lax.dynamic_index_in_dim(ln1_pair, me, axis=1, keepdims=False)
    gain_one_share = ln1_pair[0]
    shift_one_share = ln1_pair[1]
    return (
        output,
        input_grad,
        gain_one_share,
        shift_one_share,
        share_two[:, :D],
        query_bias_share,
        share_two[:, D:2 * D],
        key_bias_share,
        share_two[:, 2 * D:3 * D],
        value_bias_share,
        proj_share,
        proj_bias_share,
        gain_two_share,
        shift_two_share,
        up_share,
        up_bias_share,
        down_share,
        down_bias_share,
    )


def solution(mesh):
    in_specs = (
        P(("wide", "narrow"), None),
        P(("wide", "narrow"), None),
        P(("wide", "narrow"), None),
        P(),
        P("wide"),
        P("wide"),
        P("wide", None),
        P("wide"),
        P("wide", None),
        P("wide"),
        P("wide", None),
        P("wide"),
        P("wide", None),
        P("wide"),
        P("wide"),
        P("wide"),
        P("wide", None),
        P("wide"),
        P("wide", None),
        P("wide"),
    )
    out_specs = (
        P(("wide", "narrow"), None),
        P(("wide", "narrow"), None),
        P("wide"),
        P("wide"),
        P("wide", None),
        P("wide"),
        P("wide", None),
        P("wide"),
        P("wide", None),
        P("wide"),
        P("wide", None),
        P("wide"),
        P("wide"),
        P("wide"),
        P("wide", None),
        P("wide"),
        P("wide", None),
        P("wide"),
    )
    return jax.shard_map(
        on_device, mesh=mesh, in_specs=in_specs, out_specs=out_specs, check_vma=False
    )
```

```python
from functools import partial
import math

import jax
import jax.numpy as jnp
from jax import lax
from jax.sharding import PartitionSpec as P

D = 768
HEADS = 12
HD = 64
FEAT = 32
SEGS = 24
BLOCK = 128

EPSILON = 1e-05
HIGHEST = lax.Precision.HIGHEST


def pieces(lens_row, seq_len):
    seg_end = jnp.cumsum(lens_row)
    seg_start = seg_end - lens_row
    places = jnp.arange(seq_len, dtype=jnp.int32)
    segment = jnp.sum((places[:, None] >= seg_end[None, :]).astype(jnp.int32), axis=1)
    slots = jnp.arange(SEGS, dtype=jnp.int32)
    begins = jnp.sum(jnp.where(segment[:, None] == slots[None, :], seg_start[None, :], 0), axis=1)
    position = places - begins
    valid = (segment < SEGS - 1).astype(jnp.float32)
    return (position, valid, segment)


def rotate(heads_field, position):
    half = HD // 2
    rates = jnp.exp(jnp.arange(half, dtype=jnp.float32) * (-2.0 * math.log(10000.0) / HD))
    angles = position.astype(jnp.float32)[:, None] * rates[None, :]
    cosine = jnp.cos(angles)[:, None, :]
    sine = jnp.sin(angles)[:, None, :]
    first = heads_field[..., :half]
    second = heads_field[..., half:]
    return jnp.concatenate(
        [first * cosine - second * sine, second * cosine + first * sine], axis=-1
    )


def featurize(rotated, features):
    table = features.reshape(HD, HEADS, FEAT)
    scores = jnp.einsum("lhe,ehm->lhm", rotated, table, precision=lax.Precision.HIGH) * 0.125
    return jax.nn.elu(scores) + 1.0


def normalize(stream, gain, shift):
    average = jnp.mean(stream, axis=-1, keepdims=True)
    centered = stream - average
    variance = jnp.mean(centered * centered, axis=-1, keepdims=True)
    return centered * lax.rsqrt(variance + EPSILON) * gain + shift


def contract_rows(left, right):
    return lax.dot_general(
        left, right, (((0,), (0,)), ((), ())), preferred_element_type=jnp.float32
    )


def times_transposed(left, right):
    return lax.dot_general(
        left, right, (((1,), (1,)), ((), ())), preferred_element_type=jnp.float32
    )


def column_sums(matrix):
    return jnp.sum(matrix.astype(jnp.float32), axis=0)


def gather_rows(shard):
    return lax.all_gather(shard, "wide", axis=0, tiled=True)


def narrow_sum(share):
    size = lax.psum(1, "narrow")
    steps = size.bit_length() - 1
    assert 1 << steps == size
    me = lax.axis_index("narrow")
    rows = share.shape[0]
    assert rows % size == 0
    acc = share.astype(jnp.float32)
    for k in range(steps):
        half = acc.shape[0] // 2
        upper = ((me >> k) & 1) == 1
        lo, hi = acc[:half], acc[half:]
        keep = jnp.where(upper, hi, lo)
        send = jnp.where(upper, lo, hi).astype(jnp.bfloat16)
        pairs = [(i, i ^ (1 << k)) for i in range(size)]
        acc = keep + lax.ppermute(send, "narrow", pairs).astype(jnp.float32)
    part = acc.astype(jnp.bfloat16)
    for k in reversed(range(steps)):
        upper = ((me >> k) & 1) == 1
        pairs = [(i, i ^ (1 << k)) for i in range(size)]
        other = lax.ppermute(part, "narrow", pairs)
        part = jnp.where(upper, jnp.concatenate([other, part]), jnp.concatenate([part, other]))
    return part.astype(jnp.float32)


def axis_sum(value, axis):
    size = lax.psum(1, axis)
    steps = size.bit_length() - 1
    assert 1 << steps == size
    for k in range(steps):
        pairs = [(i, i ^ (1 << k)) for i in range(size)]
        value = value + lax.ppermute(value, axis, pairs)
    return value


def reduce_rows(full):
    share = lax.psum_scatter(full.astype(jnp.bfloat16), "wide", scatter_dimension=0, tiled=True)
    return narrow_sum(share)


def gelu_parts(upper):
    cdf = 0.5 * (1.0 + lax.erf(upper * math.sqrt(0.5)))
    slope = cdf + upper * jnp.exp(-0.5 * upper * upper) * (1.0 / math.sqrt(2.0 * math.pi))
    return upper * cdf, slope


def to_blocks(field, nseq, width):
    seq_len = field.shape[0] // nseq
    nb = seq_len // BLOCK
    return jnp.transpose(field.reshape(nseq, nb, BLOCK, HEADS, width), (0, 3, 1, 2, 4))


def from_blocks(blocks):
    nseq, heads, nb, block, width = blocks.shape
    return jnp.transpose(blocks, (0, 2, 3, 1, 4)).reshape(nseq * nb * block, heads * width)


def window(blocks, fill=0):
    pad = [(0, 0)] * blocks.ndim
    pad[-3] = (1, 0)
    prev = jnp.pad(blocks, pad, constant_values=fill)[..., :-1, :, :]
    return jnp.concatenate([prev, blocks], axis=-2)


def unwindow(win):
    own = win[..., BLOCK:, :]
    nxt = win[..., 1:, :BLOCK, :]
    pad = [(0, 0)] * win.ndim
    pad[-3] = (0, 1)
    return own + jnp.pad(nxt, pad)


def as_columns(vectors, rows):
    return jnp.concatenate([v.reshape(rows, -1) for v in vectors], axis=1)


def on_device(
    tokens,
    cotangent,
    lengths,
    features,
    ln1_gain,
    ln1_bias,
    q_weight,
    q_bias,
    k_weight,
    k_bias,
    v_weight,
    v_bias,
    out_weight,
    out_bias,
    ln2_gain,
    ln2_bias,
    up_weight,
    up_bias,
    down_weight,
    down_bias,
):
    nseq = lengths.shape[0]
    total = tokens.shape[0]
    seq_len = total // nseq
    nb = seq_len // BLOCK
    shard_rows = ln1_gain.shape[0]
    wide = D // shard_rows

    small_shards = (ln1_gain, ln1_bias, q_bias, k_bias, v_bias, out_bias, ln2_gain, ln2_bias, down_bias, up_bias)
    small_cols = [piece.shape[0] // shard_rows for piece in small_shards]
    first = gather_rows(
        jnp.concatenate([q_weight, k_weight, v_weight, as_columns(small_shards, shard_rows)], axis=1)
    )
    query_mat = first[:, :D]
    key_mat = first[:, D:2 * D]
    value_mat = first[:, 2 * D:3 * D]
    smalls = []
    offset = 3 * D
    for cols in small_cols:
        smalls.append(first[:, offset:offset + cols].astype(jnp.float32).reshape(-1))
        offset += cols
    g1, b1, bq, bk, bv, bo, g2, b2, bd, bu = smalls
    ff = up_weight.shape[1]
    second = gather_rows(jnp.concatenate([out_weight, up_weight], axis=1))
    proj_mat = second[:, :D]
    up_mat = second[:, D:]
    down_mat = gather_rows(down_weight)

    position, valid, segment = jax.vmap(partial(pieces, seq_len=seq_len))(lengths)
    position = position.reshape(total)
    seg_blocks = segment.reshape(nseq, nb, BLOCK)
    seg_win = window(seg_blocks[..., None], fill=-1)[..., 0]
    rel_q = jnp.arange(BLOCK, dtype=jnp.int32)[:, None]
    rel_k = jnp.arange(2 * BLOCK, dtype=jnp.int32)[None, :]
    allowed = (rel_k <= rel_q + BLOCK)[None, None] & (
        seg_win[:, :, None, :] == seg_blocks[:, :, :, None]
    )
    allowed = allowed[:, None]
    valid_blk = valid.reshape(nseq, 1, nb, BLOCK, 1)

    stream = tokens.astype(jnp.float32)
    standard_one, standard_back = jax.vjp(partial(normalize, gain=1.0, shift=0.0), stream)
    standard_one = lax.optimization_barrier(standard_one)
    hidden_one = (standard_one * g1 + b1).astype(jnp.bfloat16)
    query_pre = jnp.dot(hidden_one, query_mat, preferred_element_type=jnp.float32) + bq
    key_pre = jnp.dot(hidden_one, key_mat, preferred_element_type=jnp.float32) + bk
    values = (jnp.dot(hidden_one, value_mat, preferred_element_type=jnp.float32) + bv).astype(jnp.bfloat16)

    def features_of(projected):
        return featurize(rotate(projected.reshape(total, HEADS, HD), position), features)

    query_feat, query_back = jax.vjp(features_of, query_pre)
    key_feat, key_back = jax.vjp(features_of, key_pre)
    pq = to_blocks(query_feat.astype(jnp.bfloat16).reshape(total, HEADS * FEAT), nseq, FEAT)
    pk = window(to_blocks(key_feat.astype(jnp.bfloat16).reshape(total, HEADS * FEAT), nseq, FEAT))
    vb = window(to_blocks(values, nseq, HD))

    scores = jnp.einsum("shnqf,shnkf->shnqk", pq, pk, preferred_element_type=jnp.float32)
    scores = jnp.where(allowed, scores, 0.0)
    denominator = jnp.sum(scores, axis=-1, keepdims=True)
    scores_low = scores.astype(jnp.bfloat16)
    numerator = jnp.einsum("shnqk,shnkd->shnqd", scores_low, vb, preferred_element_type=jnp.float32)
    mixed = numerator / denominator * valid_blk
    attended = from_blocks(mixed).astype(jnp.bfloat16)
    residual = stream + (jnp.dot(attended, proj_mat, preferred_element_type=jnp.float32) + bo)
    normed_two, norm_two_back = jax.vjp(normalize, residual, g2, b2)
    hidden_two = normed_two.astype(jnp.bfloat16)
    upper = jnp.dot(hidden_two, up_mat, preferred_element_type=jnp.float32) + bu
    activated, slope = gelu_parts(upper)
    act_low = activated.astype(jnp.bfloat16)
    result = residual + (jnp.dot(act_low, down_mat, preferred_element_type=jnp.float32) + bd)
    output = result.astype(jnp.bfloat16)

    upward = cotangent
    grad_out = upward.astype(jnp.float32)
    down_grad = contract_rows(act_low, upward).astype(jnp.bfloat16)
    down_grad, upward = lax.optimization_barrier((down_grad, upward))
    scattered_down = lax.psum_scatter(down_grad, "wide", scatter_dimension=0, tiled=True)
    grad_act = times_transposed(upward, down_mat)
    grad_upper = (grad_act * slope).astype(jnp.bfloat16)
    grad_hidden_two = times_transposed(grad_upper, up_mat)
    grad_residual_norm, gain_two_grad, shift_two_grad = norm_two_back(grad_hidden_two)
    grad_residual = grad_out + grad_residual_norm
    grad_proj_in = grad_residual.astype(jnp.bfloat16)
    grad_attended = times_transposed(grad_proj_in, proj_mat)
    up_grad = contract_rows(hidden_two, grad_upper).astype(jnp.bfloat16)
    proj_grad = contract_rows(attended, grad_proj_in).astype(jnp.bfloat16)
    packed_one = jnp.concatenate([up_grad, proj_grad], axis=1)
    packed_one, grad_attended = lax.optimization_barrier((packed_one, grad_attended))
    scattered_one = lax.psum_scatter(packed_one, "wide", scatter_dimension=0, tiled=True)
    down_bias_grad = column_sums(upward)
    up_bias_grad = column_sums(grad_upper)
    proj_bias_grad = column_sums(grad_proj_in)

    head_grad = to_blocks(grad_attended, nseq, HD)
    scaled = head_grad * valid_blk
    grad_num = (scaled / denominator).astype(jnp.bfloat16)
    grad_den = -jnp.sum(scaled * numerator, axis=-1, keepdims=True) / (denominator * denominator)
    grad_scores = jnp.einsum("shnqd,shnkd->shnqk", grad_num, vb, preferred_element_type=jnp.float32)
    grad_scores = (grad_scores + grad_den).astype(jnp.bfloat16)
    grad_scores = jnp.where(allowed, grad_scores, jnp.zeros((), jnp.bfloat16))
    grad_vwin = jnp.einsum("shnqk,shnqd->shnkd", scores_low, grad_num, preferred_element_type=jnp.float32)
    grad_value = from_blocks(unwindow(grad_vwin)).astype(jnp.bfloat16)
    grad_qf = jnp.einsum("shnqk,shnkf->shnqf", grad_scores, pk, preferred_element_type=jnp.float32)
    grad_kwin = jnp.einsum("shnqk,shnqf->shnkf", grad_scores, pq, preferred_element_type=jnp.float32)
    grad_qf = from_blocks(grad_qf).reshape(total, HEADS, FEAT)
    grad_kf = from_blocks(unwindow(grad_kwin)).reshape(total, HEADS, FEAT)
    grad_key = key_back(grad_kf)[0].astype(jnp.bfloat16)
    grad_query = query_back(grad_qf)[0].astype(jnp.bfloat16)
    scattered_down, scattered_one, grad_query, grad_key = lax.optimization_barrier(
        (scattered_down, scattered_one, grad_query, grad_key)
    )
    grad_qkv = jnp.concatenate([grad_query, grad_key, grad_value], axis=1)
    down_share = lax.psum(scattered_down, "narrow")
    share_one = lax.psum(scattered_one, "narrow")
    qkv_grad = contract_rows(hidden_one, grad_qkv)
    qkv_bias_grad = column_sums(grad_qkv)

    small_grads = (
        qkv_bias_grad[:D],
        qkv_bias_grad[D:2 * D],
        qkv_bias_grad[2 * D:],
        proj_bias_grad,
        gain_two_grad,
        shift_two_grad,
        down_bias_grad,
        up_bias_grad,
    )
    packed_two = jnp.concatenate([qkv_grad, as_columns(small_grads, D)], axis=1)
    down_share, share_one, packed_two = lax.optimization_barrier((down_share, share_one, packed_two))
    down_share = down_share.astype(jnp.float32)
    up_share = share_one[:, :ff].astype(jnp.float32)
    proj_share = share_one[:, ff:].astype(jnp.float32)
    share_two = reduce_rows(packed_two)
    small_out = []
    offset = 3 * D
    for cols in small_cols[2:]:
        small_out.append(share_two[:, offset:offset + cols].reshape(-1))
        offset += cols
    (
        query_bias_share,
        key_bias_share,
        value_bias_share,
        proj_bias_share,
        gain_two_share,
        shift_two_share,
        down_bias_share,
        up_bias_share,
    ) = small_out

    grad_hidden_one = times_transposed(grad_qkv, first[:, :3 * D])
    gain_one_grad = jnp.sum(grad_hidden_one * standard_one, axis=0)
    shift_one_grad = jnp.sum(grad_hidden_one, axis=0)
    (grad_stream_norm,) = standard_back(grad_hidden_one * g1)
    input_grad = grad_residual + grad_stream_norm
    me = lax.axis_index("wide")
    ln1_pair = jnp.stack([gain_one_grad, shift_one_grad])
    ln1_pair = axis_sum(axis_sum(ln1_pair, "wide"), "narrow").reshape(2, wide, shard_rows)
    ln1_pair = lax.dynamic_index_in_dim(ln1_pair, me, axis=1, keepdims=False)
    gain_one_share = ln1_pair[0]
    shift_one_share = ln1_pair[1]
    return (
        output,
        input_grad,
        gain_one_share,
        shift_one_share,
        share_two[:, :D],
        query_bias_share,
        share_two[:, D:2 * D],
        key_bias_share,
        share_two[:, 2 * D:3 * D],
        value_bias_share,
        proj_share,
        proj_bias_share,
        gain_two_share,
        shift_two_share,
        up_share,
        up_bias_share,
        down_share,
        down_bias_share,
    )


def solution(mesh):
    in_specs = (
        P(("wide", "narrow"), None),
        P(("wide", "narrow"), None),
        P(("wide", "narrow"), None),
        P(),
        P("wide"),
        P("wide"),
        P("wide", None),
        P("wide"),
        P("wide", None),
        P("wide"),
        P("wide", None),
        P("wide"),
        P("wide", None),
        P("wide"),
        P("wide"),
        P("wide"),
        P("wide", None),
        P("wide"),
        P("wide", None),
        P("wide"),
    )
    out_specs = (
        P(("wide", "narrow"), None),
        P(("wide", "narrow"), None),
        P("wide"),
        P("wide"),
        P("wide", None),
        P("wide"),
        P("wide", None),
        P("wide"),
        P("wide", None),
        P("wide"),
        P("wide", None),
        P("wide"),
        P("wide"),
        P("wide"),
        P("wide", None),
        P("wide"),
        P("wide", None),
        P("wide"),
    )
    return jax.shard_map(
        on_device, mesh=mesh, in_specs=in_specs, out_specs=out_specs, check_vma=False
    )
```

```python
from functools import partial
import math

import jax
import jax.numpy as jnp
from jax import lax
from jax.sharding import PartitionSpec as P

D = 768
HEADS = 12
HD = 64
FEAT = 32
SEGS = 24
BLOCK = 128

EPSILON = 1e-05
HIGHEST = lax.Precision.HIGHEST


def pieces(lens_row, seq_len):
    seg_end = jnp.cumsum(lens_row)
    seg_start = seg_end - lens_row
    places = jnp.arange(seq_len, dtype=jnp.int32)
    segment = jnp.sum((places[:, None] >= seg_end[None, :]).astype(jnp.int32), axis=1)
    slots = jnp.arange(SEGS, dtype=jnp.int32)
    begins = jnp.sum(jnp.where(segment[:, None] == slots[None, :], seg_start[None, :], 0), axis=1)
    position = places - begins
    valid = (segment < SEGS - 1).astype(jnp.float32)
    return (position, valid, segment)


def rotate(heads_field, position):
    half = HD // 2
    rates = jnp.exp(jnp.arange(half, dtype=jnp.float32) * (-2.0 * math.log(10000.0) / HD))
    angles = position.astype(jnp.float32)[:, None] * rates[None, :]
    cosine = jnp.cos(angles)[:, None, :]
    sine = jnp.sin(angles)[:, None, :]
    first = heads_field[..., :half]
    second = heads_field[..., half:]
    return jnp.concatenate(
        [first * cosine - second * sine, second * cosine + first * sine], axis=-1
    )


def featurize(rotated, features):
    table = features.reshape(HD, HEADS, FEAT)
    scores = jnp.einsum("lhe,ehm->lhm", rotated, table, precision=lax.Precision.HIGH) * 0.125
    return jax.nn.elu(scores) + 1.0


def normalize(stream, gain, shift):
    average = jnp.mean(stream, axis=-1, keepdims=True)
    centered = stream - average
    variance = jnp.mean(centered * centered, axis=-1, keepdims=True)
    return centered * lax.rsqrt(variance + EPSILON) * gain + shift


def contract_rows(left, right):
    return lax.dot_general(
        left, right, (((0,), (0,)), ((), ())), preferred_element_type=jnp.float32
    )


def times_transposed(left, right):
    return lax.dot_general(
        left, right, (((1,), (1,)), ((), ())), preferred_element_type=jnp.float32
    )


def column_sums(matrix):
    return jnp.sum(matrix.astype(jnp.float32), axis=0)


def gather_rows(shard):
    return lax.all_gather(shard, "wide", axis=0, tiled=True)


def narrow_sum(share):
    size = lax.psum(1, "narrow")
    steps = size.bit_length() - 1
    assert 1 << steps == size
    me = lax.axis_index("narrow")
    rows = share.shape[0]
    assert rows % size == 0
    acc = share.astype(jnp.float32)
    for k in range(steps):
        half = acc.shape[0] // 2
        upper = ((me >> k) & 1) == 1
        lo, hi = acc[:half], acc[half:]
        keep = jnp.where(upper, hi, lo)
        send = jnp.where(upper, lo, hi).astype(jnp.bfloat16)
        pairs = [(i, i ^ (1 << k)) for i in range(size)]
        acc = keep + lax.ppermute(send, "narrow", pairs).astype(jnp.float32)
    part = acc.astype(jnp.bfloat16)
    for k in reversed(range(steps)):
        upper = ((me >> k) & 1) == 1
        pairs = [(i, i ^ (1 << k)) for i in range(size)]
        other = lax.ppermute(part, "narrow", pairs)
        part = jnp.where(upper, jnp.concatenate([other, part]), jnp.concatenate([part, other]))
    return part.astype(jnp.float32)


def axis_sum(value, axis):
    size = lax.psum(1, axis)
    steps = size.bit_length() - 1
    assert 1 << steps == size
    for k in range(steps):
        pairs = [(i, i ^ (1 << k)) for i in range(size)]
        value = value + lax.ppermute(value, axis, pairs)
    return value


def reduce_rows(full):
    share = lax.psum_scatter(full.astype(jnp.bfloat16), "wide", scatter_dimension=0, tiled=True)
    return narrow_sum(share)


def gelu_parts(upper):
    cdf = 0.5 * (1.0 + lax.erf(upper * math.sqrt(0.5)))
    slope = cdf + upper * jnp.exp(-0.5 * upper * upper) * (1.0 / math.sqrt(2.0 * math.pi))
    return upper * cdf, slope


def to_blocks(field, nseq, width):
    seq_len = field.shape[0] // nseq
    nb = seq_len // BLOCK
    return jnp.transpose(field.reshape(nseq, nb, BLOCK, HEADS, width), (0, 3, 1, 2, 4))


def from_blocks(blocks):
    nseq, heads, nb, block, width = blocks.shape
    return jnp.transpose(blocks, (0, 2, 3, 1, 4)).reshape(nseq * nb * block, heads * width)


def window(blocks, fill=0):
    pad = [(0, 0)] * blocks.ndim
    pad[-3] = (1, 0)
    prev = jnp.pad(blocks, pad, constant_values=fill)[..., :-1, :, :]
    return jnp.concatenate([prev, blocks], axis=-2)


def unwindow(win):
    own = win[..., BLOCK:, :]
    nxt = win[..., 1:, :BLOCK, :]
    pad = [(0, 0)] * win.ndim
    pad[-3] = (0, 1)
    return own + jnp.pad(nxt, pad)


def as_columns(vectors, rows):
    return jnp.concatenate([v.reshape(rows, -1) for v in vectors], axis=1)


def on_device(
    tokens,
    cotangent,
    lengths,
    features,
    ln1_gain,
    ln1_bias,
    q_weight,
    q_bias,
    k_weight,
    k_bias,
    v_weight,
    v_bias,
    out_weight,
    out_bias,
    ln2_gain,
    ln2_bias,
    up_weight,
    up_bias,
    down_weight,
    down_bias,
):
    nseq = lengths.shape[0]
    total = tokens.shape[0]
    seq_len = total // nseq
    nb = seq_len // BLOCK
    shard_rows = ln1_gain.shape[0]
    wide = D // shard_rows

    small_shards = (ln1_gain, ln1_bias, q_bias, k_bias, v_bias, out_bias, ln2_gain, ln2_bias, down_bias, up_bias)
    small_cols = [piece.shape[0] // shard_rows for piece in small_shards]
    first = gather_rows(
        jnp.concatenate([q_weight, k_weight, v_weight, as_columns(small_shards, shard_rows)], axis=1)
    )
    query_mat = first[:, :D]
    key_mat = first[:, D:2 * D]
    value_mat = first[:, 2 * D:3 * D]
    smalls = []
    offset = 3 * D
    for cols in small_cols:
        smalls.append(first[:, offset:offset + cols].astype(jnp.float32).reshape(-1))
        offset += cols
    g1, b1, bq, bk, bv, bo, g2, b2, bd, bu = smalls
    ff = up_weight.shape[1]
    second = gather_rows(jnp.concatenate([out_weight, up_weight], axis=1))
    proj_mat = second[:, :D]
    up_mat = second[:, D:]
    down_mat = gather_rows(down_weight)

    position, valid, segment = jax.vmap(partial(pieces, seq_len=seq_len))(lengths)
    position = position.reshape(total)
    seg_blocks = segment.reshape(nseq, nb, BLOCK)
    seg_win = window(seg_blocks[..., None], fill=-1)[..., 0]
    rel_q = jnp.arange(BLOCK, dtype=jnp.int32)[:, None]
    rel_k = jnp.arange(2 * BLOCK, dtype=jnp.int32)[None, :]
    allowed = (rel_k <= rel_q + BLOCK)[None, None] & (
        seg_win[:, :, None, :] == seg_blocks[:, :, :, None]
    )
    allowed = allowed[:, None]
    valid_blk = valid.reshape(nseq, 1, nb, BLOCK, 1)

    stream = tokens.astype(jnp.float32)
    standard_one, standard_back = jax.vjp(partial(normalize, gain=1.0, shift=0.0), stream)
    standard_one = lax.optimization_barrier(standard_one)
    hidden_one = (standard_one * g1 + b1).astype(jnp.bfloat16)
    query_pre = jnp.dot(hidden_one, query_mat, preferred_element_type=jnp.float32) + bq
    key_pre = jnp.dot(hidden_one, key_mat, preferred_element_type=jnp.float32) + bk
    values = (jnp.dot(hidden_one, value_mat, preferred_element_type=jnp.float32) + bv).astype(jnp.bfloat16)

    def features_of(projected):
        return featurize(rotate(projected.reshape(total, HEADS, HD), position), features)

    query_feat, query_back = jax.vjp(features_of, query_pre)
    key_feat, key_back = jax.vjp(features_of, key_pre)
    pq = to_blocks(query_feat.astype(jnp.bfloat16).reshape(total, HEADS * FEAT), nseq, FEAT)
    pk = window(to_blocks(key_feat.astype(jnp.bfloat16).reshape(total, HEADS * FEAT), nseq, FEAT))
    vb = window(to_blocks(values, nseq, HD))

    scores = jnp.einsum("shnqf,shnkf->shnqk", pq, pk, preferred_element_type=jnp.float32)
    scores = jnp.where(allowed, scores, 0.0)
    denominator = jnp.sum(scores, axis=-1, keepdims=True)
    scores_low = scores.astype(jnp.bfloat16)
    numerator = jnp.einsum("shnqk,shnkd->shnqd", scores_low, vb, preferred_element_type=jnp.float32)
    mixed = numerator / denominator * valid_blk
    attended = from_blocks(mixed).astype(jnp.bfloat16)
    residual = stream + (jnp.dot(attended, proj_mat, preferred_element_type=jnp.float32) + bo)
    normed_two, norm_two_back = jax.vjp(normalize, residual, g2, b2)
    hidden_two = normed_two.astype(jnp.bfloat16)
    upper = jnp.dot(hidden_two, up_mat, preferred_element_type=jnp.float32) + bu
    activated, slope = gelu_parts(upper)
    act_low = activated.astype(jnp.bfloat16)
    result = residual + (jnp.dot(act_low, down_mat, preferred_element_type=jnp.float32) + bd)
    output = result.astype(jnp.bfloat16)

    upward = cotangent
    grad_out = upward.astype(jnp.float32)
    down_grad = contract_rows(act_low, upward).astype(jnp.bfloat16)
    down_grad, upward = lax.optimization_barrier((down_grad, upward))
    scattered_down = lax.psum_scatter(down_grad, "wide", scatter_dimension=0, tiled=True)
    grad_act = times_transposed(upward, down_mat)
    grad_upper = (grad_act * slope).astype(jnp.bfloat16)
    grad_hidden_two = times_transposed(grad_upper, up_mat)
    grad_residual_norm, gain_two_grad, shift_two_grad = norm_two_back(grad_hidden_two)
    grad_residual = grad_out + grad_residual_norm
    grad_proj_in = grad_residual.astype(jnp.bfloat16)
    grad_attended = times_transposed(grad_proj_in, proj_mat)
    up_grad = contract_rows(hidden_two, grad_upper).astype(jnp.bfloat16)
    proj_grad = contract_rows(attended, grad_proj_in).astype(jnp.bfloat16)
    packed_one = jnp.concatenate([up_grad, proj_grad], axis=1)
    packed_one, grad_attended = lax.optimization_barrier((packed_one, grad_attended))
    scattered_one = lax.psum_scatter(packed_one, "wide", scatter_dimension=0, tiled=True)
    down_bias_grad = column_sums(upward)
    up_bias_grad = column_sums(grad_upper)
    proj_bias_grad = column_sums(grad_proj_in)

    head_grad = to_blocks(grad_attended, nseq, HD)
    scaled = head_grad * valid_blk
    grad_num = (scaled / denominator).astype(jnp.bfloat16)
    grad_den = -jnp.sum(scaled * numerator, axis=-1, keepdims=True) / (denominator * denominator)
    grad_scores = jnp.einsum("shnqd,shnkd->shnqk", grad_num, vb, preferred_element_type=jnp.float32)
    grad_scores = (grad_scores + grad_den).astype(jnp.bfloat16)
    grad_scores = jnp.where(allowed, grad_scores, jnp.zeros((), jnp.bfloat16))
    grad_vwin = jnp.einsum("shnqk,shnqd->shnkd", scores_low, grad_num, preferred_element_type=jnp.float32)
    grad_value = from_blocks(unwindow(grad_vwin)).astype(jnp.bfloat16)
    grad_qf = jnp.einsum("shnqk,shnkf->shnqf", grad_scores, pk, preferred_element_type=jnp.float32)
    grad_kwin = jnp.einsum("shnqk,shnqf->shnkf", grad_scores, pq, preferred_element_type=jnp.float32)
    grad_qf = from_blocks(grad_qf).reshape(total, HEADS, FEAT)
    grad_kf = from_blocks(unwindow(grad_kwin)).reshape(total, HEADS, FEAT)
    grad_key = key_back(grad_kf)[0].astype(jnp.bfloat16)
    grad_query = query_back(grad_qf)[0].astype(jnp.bfloat16)
    scattered_down, scattered_one, grad_query, grad_key = lax.optimization_barrier(
        (scattered_down, scattered_one, grad_query, grad_key)
    )
    grad_qkv = jnp.concatenate([grad_query, grad_key, grad_value], axis=1)
    down_share = lax.psum(scattered_down, "narrow")
    share_one = lax.psum(scattered_one, "narrow")
    qkv_grad = contract_rows(hidden_one, grad_qkv)
    qkv_bias_grad = column_sums(grad_qkv)

    down_share, share_one, qkv_grad = lax.optimization_barrier((down_share, share_one, qkv_grad))
    down_share = down_share.astype(jnp.float32)
    up_share = share_one[:, :ff].astype(jnp.float32)
    proj_share = share_one[:, ff:].astype(jnp.float32)
    share_two = reduce_rows(qkv_grad)

    grad_hidden_one = times_transposed(grad_qkv, first[:, :3 * D])
    gain_one_grad = jnp.sum(grad_hidden_one * standard_one, axis=0)
    shift_one_grad = jnp.sum(grad_hidden_one, axis=0)
    (grad_stream_norm,) = standard_back(grad_hidden_one * g1)
    input_grad = grad_residual + grad_stream_norm
    small_grads = (
        gain_one_grad,
        shift_one_grad,
        qkv_bias_grad[:D],
        qkv_bias_grad[D:2 * D],
        qkv_bias_grad[2 * D:],
        proj_bias_grad,
        gain_two_grad,
        shift_two_grad,
        down_bias_grad,
        up_bias_grad,
    )
    me = lax.axis_index("wide")
    summed = axis_sum(axis_sum(jnp.concatenate(small_grads), "wide"), "narrow")
    small_out = []
    offset = 0
    for piece in small_grads:
        size = piece.shape[0]
        rows = summed[offset:offset + size].reshape(wide, size // wide)
        small_out.append(lax.dynamic_index_in_dim(rows, me, axis=0, keepdims=False))
        offset += size
    (
        gain_one_share,
        shift_one_share,
        query_bias_share,
        key_bias_share,
        value_bias_share,
        proj_bias_share,
        gain_two_share,
        shift_two_share,
        down_bias_share,
        up_bias_share,
    ) = small_out
    return (
        output,
        input_grad,
        gain_one_share,
        shift_one_share,
        share_two[:, :D],
        query_bias_share,
        share_two[:, D:2 * D],
        key_bias_share,
        share_two[:, 2 * D:3 * D],
        value_bias_share,
        proj_share,
        proj_bias_share,
        gain_two_share,
        shift_two_share,
        up_share,
        up_bias_share,
        down_share,
        down_bias_share,
    )


def solution(mesh):
    in_specs = (
        P(("wide", "narrow"), None),
        P(("wide", "narrow"), None),
        P(("wide", "narrow"), None),
        P(),
        P("wide"),
        P("wide"),
        P("wide", None),
        P("wide"),
        P("wide", None),
        P("wide"),
        P("wide", None),
        P("wide"),
        P("wide", None),
        P("wide"),
        P("wide"),
        P("wide"),
        P("wide", None),
        P("wide"),
        P("wide", None),
        P("wide"),
    )
    out_specs = (
        P(("wide", "narrow"), None),
        P(("wide", "narrow"), None),
        P("wide"),
        P("wide"),
        P("wide", None),
        P("wide"),
        P("wide", None),
        P("wide"),
        P("wide", None),
        P("wide"),
        P("wide", None),
        P("wide"),
        P("wide"),
        P("wide"),
        P("wide", None),
        P("wide"),
        P("wide", None),
        P("wide"),
    )
    return jax.shard_map(
        on_device, mesh=mesh, in_specs=in_specs, out_specs=out_specs, check_vma=False
    )
```
